512 devices in a mesh: gx: 8 (over x, core), gy: 8 (over y), gz: 8 (over z).
Axes of the slice: x: 4, y: 8, z: 8, core: 2. Of those that a mesh axis runs over, the one named last changes fastest.
Arguments:
- warped_image: float32 [512, 512, 1024], P('gx', 'gy', 'gz'), may hold values from -6 to 6
- fixed_image: float32 [512, 512, 1024], P('gx', 'gy', 'gz'), may hold values from -6 to 6
- fine_control: float32 [3, 64, 64, 128], P(None, 'gx', 'gy', 'gz'), may hold values from -6 to 6
- coarse_control: float32 [3, 16, 16, 32], replicated, may hold values from -6 to 6
Outputs:
- fine_gradient: float32 [3, 64, 64, 128], P(None, 'gx', 'gy', 'gz')
- coarse_gradient: float32 [3, 16, 16, 32], replicated
The draws below stay inside these ranges and needn't reach their ends.
All inputs are finite; a program needn't handle non-finite values.
Results may differ from the reference program's by a relative error of at most 0.0003.
Values sent between devices are 32-bit elements; how exact they have to be, the bound alone decides.
A program may use at most 64 MiB of HBM per device.

```python
import jax
import jax.numpy as jnp
from jax import lax

SPF = 8
SPC = 32
NX = 512
NY = 512
NZ = 1024
FX = 64
FY = 64
FZ = 128
KX = 16
KY = 16
KZ = 32


def levels(key, shape, shards, low, largest):
    def one(position, shards_of):
        draws = jax.random.uniform(jax.random.fold_in(jax.random.fold_in(key, 6), position), (shards_of,), jnp.float32, low / len(shards), largest / len(shards))
        return jnp.repeat(jnp.exp(draws), shape[position] // shards_of).reshape((-1,) + (1,) * (len(shape) - position - 1))

    gain = one(*shards[0])
    for cut in shards[1:]:
        gain = gain * one(*cut)
    return gain


def scatter_about(rng, extent, deviation, most, cuts=(), kind=jnp.bfloat16):
    entries = deviation * jax.random.normal(rng, extent, jnp.float32)
    if cuts:
        entries = entries * levels(rng, extent, cuts, -0.22, 0.18)
    return jnp.clip(entries, -most, most).astype(kind)


def setup_inputs(seed: int = 0) -> dict:
    arg_keys = jax.random.split(jax.random.key(seed), 5)
    return {
        "warped_image": scatter_about(arg_keys[0], (NX, NY, NZ), 1.0, 6.0, ((0, 8), (1, 8), (2, 8)), jnp.float32),
        "fixed_image": scatter_about(arg_keys[1], (NX, NY, NZ), 1.0, 6.0, ((0, 8), (1, 8), (2, 8)), jnp.float32),
        "fine_control": scatter_about(arg_keys[2], (3, FX, FY, FZ), 1.0, 6.0, ((1, 8), (2, 8), (3, 8)), jnp.float32),
        "coarse_control": scatter_about(arg_keys[3], (3, KX, KY, KZ), 1.0, 6.0, (), jnp.float32),
    }


bend_factor = 0.01
highest = lax.Precision.HIGHEST


def spline(values):
    magnitude = jnp.abs(values)
    inner = 2.0 / 3.0 - magnitude * magnitude + 0.5 * magnitude * magnitude * magnitude
    remain = 2.0 - magnitude
    outer = remain * remain * remain / 6.0
    return jnp.where(magnitude < 1.0, inner, jnp.where(magnitude < 2.0, outer, 0.0 * magnitude))


def basis_matrix(voxels, points, spacing, voxel_start, point_start):
    voxel = (jnp.arange(voxels, dtype=jnp.int32) + voxel_start).astype(jnp.float32) + 0.5
    centre = (jnp.arange(points, dtype=jnp.int32) + point_start).astype(jnp.float32) * spacing + 0.5 * spacing
    return spline((voxel[:, None] - centre[None, :]) / spacing)


def slope(padded, axis):
    rank = padded.ndim
    count = padded.shape[axis] - 4

    def shifted(offset):
        piece = lax.slice_in_dim(padded, offset, offset + count, axis=axis)
        for other in range(rank - 3, rank):
            if other != axis:
                piece = lax.slice_in_dim(piece, 2, piece.shape[other] - 2, axis=other)
        return piece

    return (shifted(0) - 8.0 * shifted(1) + 8.0 * shifted(3) - shifted(4)) / 12.0


def stencil(padded):
    centre = padded[:, 1:-1, 1:-1, 1:-1]
    total = padded[:, 2:, 1:-1, 1:-1] + padded[:, :-2, 1:-1, 1:-1]
    total = total + padded[:, 1:-1, 2:, 1:-1] + padded[:, 1:-1, :-2, 1:-1]
    total = total + padded[:, 1:-1, 1:-1, 2:] + padded[:, 1:-1, 1:-1, :-2]
    return total - 6.0 * centre


def laplace(field):
    return stencil(jnp.pad(field, ((0, 0), (1, 1), (1, 1), (1, 1))))


def project_blocks(force, along_x, along_y, along_z):
    section = jnp.einsum("axyz,zr->axyr", force, along_z, precision=highest)
    section = jnp.einsum("axyr,yq->axqr", section, along_y, precision=highest)
    return jnp.einsum("axqr,xp->apqr", section, along_x, precision=highest)


def reference(warped_image, fixed_image, fine_control, coarse_control):
    summed = jnp.pad(warped_image + fixed_image, 2)
    difference = warped_image - fixed_image
    fine_x = basis_matrix(NX, FX, SPF, 0, 0)
    fine_y = basis_matrix(NY, FY, SPF, 0, 0)
    fine_z = basis_matrix(NZ, FZ, SPF, 0, 0)
    coarse_x = basis_matrix(NX, KX, SPC, 0, 0)
    coarse_y = basis_matrix(NY, KY, SPC, 0, 0)
    coarse_z = basis_matrix(NZ, KZ, SPC, 0, 0)
    block_rows = 16

    def block(carry, start):
        fine_sum, coarse_sum = carry
        slab = lax.dynamic_slice_in_dim(summed, start, block_rows + 4, 0)
        slopes = jnp.stack([slope(slab, 0), slope(slab, 1), slope(slab, 2)]) * 0.5
        local = lax.dynamic_slice_in_dim(difference, start, block_rows, 0)
        force = slopes * local[None]
        fine_rows = lax.dynamic_slice_in_dim(fine_x, start, block_rows, 0)
        coarse_rows = lax.dynamic_slice_in_dim(coarse_x, start, block_rows, 0)
        fine_sum = fine_sum + project_blocks(force, fine_rows, fine_y, fine_z)
        coarse_sum = coarse_sum + project_blocks(force, coarse_rows, coarse_y, coarse_z)
        return (fine_sum, coarse_sum), None

    starts = jnp.arange(NX // block_rows, dtype=jnp.int32) * block_rows
    initial = (jnp.zeros((3, FX, FY, FZ), jnp.float32), jnp.zeros((3, KX, KY, KZ), jnp.float32))
    (fine_sum, coarse_sum), _ = lax.scan(block, initial, starts)
    fine_gradient = fine_sum * (SPF ** -1.5) + bend_factor * laplace(laplace(fine_control))
    coarse_gradient = coarse_sum * (SPC ** -1.5) + bend_factor * laplace(laplace(coarse_control))
    return fine_gradient, coarse_gradient
```

```python
import itertools

import jax
import jax.numpy as jnp
import numpy as np
from jax import lax
from jax.experimental import pallas as pl
from jax.experimental.pallas import tpu as pltpu
from jax.sharding import PartitionSpec as P

SPF = 8
SPC = 32
BEND = 0.01
FB = 96
MESH = pl.DeviceIdType.MESH
F32 = jnp.float32
BF16 = jnp.bfloat16


def beta(t):
    m = np.abs(t)
    r = 2.0 - m
    return np.where(m < 1.0, 2.0 / 3.0 - m * m + 0.5 * m**3, np.where(m < 2.0, r**3 / 6.0, 0.0))


def basis(voxels, points, spacing, first):
    v = np.arange(voxels)[:, None] + 0.5
    c = (np.arange(points)[None, :] + first) * spacing + 0.5 * spacing
    return beta((v - c) / spacing)


def halves(w):
    hi = np.asarray(w, np.float32).astype(jnp.bfloat16)
    lo = (np.asarray(w, np.float64) - hi.astype(np.float64)).astype(np.float32).astype(jnp.bfloat16)
    return hi, lo


W4 = beta((np.arange(4)[:, None] + 4.5 - 4.0 * np.arange(4)[None, :]) / 4.0) / 24.0
TWO = np.array([1.0, 4.0, 6.0, 4.0, 1.0]) / 8.0


def spread(c, step):
    out = np.zeros((len(c) - 1) * step + 1)
    out[::step] = c
    return out


C29 = np.convolve(np.convolve(TWO, spread(TWO, 2)), spread(TWO, 4))


def y_matrix(sy):
    rows = np.zeros((24, sy))
    rows[:12] = basis(sy, 12, SPF, -2).T * SPF**-1.5
    rows[16:22] = basis(sy, 6, SPC, -2).T * SPC**-1.5
    hi, lo = halves(rows)
    return np.concatenate([np.concatenate([hi, hi], 1), np.concatenate([lo, lo], 1)], 0)


def z_matrices(sz):
    out = []
    for a in range(3):
        cols = np.zeros((sz, 128))
        cols[:, FB : FB + 20] = basis(sz, 20, SPF, -2)
        cols[:, 32 * a : 32 * a + 8] = basis(sz, 8, SPC, -2)
        hi, lo = halves(cols)
        half = np.concatenate([hi, lo], 1)
        out.append(np.concatenate([half, half], 0))
    return np.stack(out)


def d_matrix(sz):
    d = np.zeros((sz, sz), np.float32)
    for shift, value in ((-2, 1.0), (-1, -8.0), (1, 8.0), (2, -1.0)):
        for v in range(sz):
            if 0 <= v + shift < sz:
                d[v + shift, v] = value
    return np.concatenate([d, d], 0).astype(jnp.bfloat16)


def split(x):
    hi = x.astype(BF16)
    return hi, (x - hi.astype(F32)).astype(BF16)


def lanes(shape):
    return lax.broadcasted_iota(jnp.int32, shape, len(shape) - 1)


def roll(x, shift, axis):
    return pltpu.roll(x, shift % x.shape[axis] if isinstance(shift, int) else shift, axis)


def kernel(dims, w_hbm, f_hbm, ctl, cctl, wy, wz, dz_w, fine_out, coarse_out,
           wb, fb, sp, hys, hyr, hzs, hzr, cz, dzb, xs, zs, e, csend, crecv, zg, yg, xg,
           fxr, fys, fyr, fzs, fzr, fw,
           img_sem, hs, hr, cs, cr, gs, gr, fs, fr):
    nx, ny, nz = dims
    pos = (lax.axis_index("gx"), lax.axis_index("gy"), lax.axis_index("gz"))
    gx, gy, gz = pos
    has = [{-1: pos[i] > 0, 1: pos[i] < dims[i] - 1} for i in range(3)]

    def exists(d):
        cond = None
        for i in range(3):
            if d[i]:
                cond = has[i][d[i]] if cond is None else jnp.logical_and(cond, has[i][d[i]])
        return cond

    def at(d):
        return tuple(pos[i] + d[i] for i in range(3))

    def ring(axis, o):
        t = lax.rem(pos[axis] + o, dims[axis])
        return tuple(t if i == axis else pos[i] for i in range(3)), t

    neighbours = [d for d in itertools.product((-1, 0, 1), repeat=3) if any(d)]
    diagonal = [d for d in neighbours if sum(map(abs, d)) > 1]

    chunks = 8
    planes = 8
    for c in range(chunks):
        part = pl.ds(c * planes, planes)
        pltpu.make_async_copy(w_hbm.at[part], wb.at[part], img_sem.at[0, c]).start()
        pltpu.make_async_copy(f_hbm.at[part], fb.at[part], img_sem.at[1, c]).start()

    bar = pltpu.get_barrier_semaphore()
    for axis in range(3):
        for o in range(1, dims[axis]):
            pl.semaphore_signal(bar, inc=1, device_id=ring(axis, o)[0], device_id_type=MESH)
    for d in diagonal:
        @pl.when(exists(d))
        def _(d=d):
            pl.semaphore_signal(bar, inc=1, device_id=at(d), device_id_type=MESH)
    wide = [1 + h[-1].astype(jnp.int32) + h[1].astype(jnp.int32) for h in has]
    greeted = wide[0] * wide[1] * wide[2] - 1 - (wide[0] + wide[1] + wide[2] - 3) + (nx + ny + nz - 3)

    zero8 = jnp.zeros((8, 128), F32)
    for side, d in ((0, -1), (1, 1)):
        @pl.when(jnp.logical_not(has[0][d]))
        def _(side=side):
            sp[66 * side : 66 * side + 2, 8:72, :] = jnp.zeros((2, 64, 128), F32)
            fxr[side] = jnp.zeros(fxr.shape[1:], F32)

        @pl.when(jnp.logical_not(has[1][d]))
        def _(side=side):
            hyr[side] = jnp.zeros(hyr.shape[1:], F32)
            fyr[side] = jnp.zeros(fyr.shape[1:], F32)

        @pl.when(jnp.logical_not(has[2][d]))
        def _(side=side):
            hzr[side] = jnp.zeros(hzr.shape[1:], F32)
            fzr[side] = jnp.zeros(fzr.shape[1:], F32)

    hzs[...] = jnp.zeros(hzs.shape, F32)

    lane64 = lanes((64, 128))

    def sum_chunk(c, _):
        base = pl.multiple_of(c * planes, planes)
        part = pl.ds(base, planes)
        pltpu.make_async_copy(w_hbm.at[part], wb.at[part], img_sem.at[0, c]).wait()
        pltpu.make_async_copy(f_hbm.at[part], fb.at[part], img_sem.at[1, c]).wait()
        packed = jnp.zeros((64, 128), F32)
        for j in range(planes):
            w = wb[base + j]
            f = fb[base + j]
            s = w + f
            wb[base + j] = w - f
            sp[base + j + 2, 8:72, :] = s
            hys[0, base + j] = s[0:2]
            hys[1, base + j] = s[62:64]
            packed = jnp.where(lane64 // 4 == j, roll(s, 4 * j + 2, 1), packed)
            hi, lo = split(s)
            dzb[base + j] = jnp.dot(jnp.concatenate([hi, lo], 1), dz_w[...], preferred_element_type=F32)
        h = c // 4
        q = lax.rem(c, 4)
        hzs[h] = jnp.where(lane64 // 32 == q, pltpu.roll(packed, 32 * q, 1), hzs[h])
        return 0

    lax.fori_loop(0, chunks, sum_chunk, 0)
    pl.semaphore_wait(bar, greeted)

    def halo(k):
        axis, side = k // 2, k % 2
        d = [0, 0, 0]
        d[axis] = 2 * side - 1
        if axis == 0:
            src = sp.at[pl.ds(2 if side == 0 else 64, 2), pl.ds(8, 64), :]
            dst = sp.at[pl.ds(66 if side == 0 else 0, 2), pl.ds(8, 64), :]
        elif axis == 1:
            src, dst = hys.at[side], hyr.at[1 - side]
        else:
            src, dst = hzs, hzr.at[1 - side]
        return d, pltpu.make_async_remote_copy(
            src_ref=src, dst_ref=dst, send_sem=hs.at[k], recv_sem=hr.at[k],
            device_id=at(d), device_id_type=MESH)

    def fine_copy(k):
        axis, side = k // 2, k % 2
        d = [0, 0, 0]
        d[axis] = 2 * side - 1
        if axis == 0:
            src, dst = e.at[:, pl.ds(10 * side, 2)], fxr.at[1 - side]
        elif axis == 1:
            src, dst = fys.at[side], fyr.at[1 - side]
        else:
            src, dst = fzs.at[side], fzr.at[1 - side]
        return d, pltpu.make_async_remote_copy(
            src_ref=src, dst_ref=dst, send_sem=fs.at[k], recv_sem=fr.at[k],
            device_id=at(d), device_id_type=MESH)

    def start(make, k):
        d, copy = make(k)
        pl.when(exists(d))(lambda: copy.start())

    def sent(make, k):
        d, copy = make(k)
        pl.when(exists(d))(lambda: copy.wait_send())

    def arrived(make, k):
        d, copy = make(k)
        pl.when(exists([-v for v in d]))(lambda: copy.wait_recv())

    for k in (4, 5, 2, 3, 0, 1):
        start(halo, k)

    row16 = lax.broadcasted_iota(jnp.int32, (16, 128), 0)
    lane16 = lanes((16, 128))
    row_g = row16 - 2 + gy * 8
    lane_g = lane16 - (FB + 2) + gz * 16
    in_grid = (row_g >= 0) & (row_g < ny * 8) & (lane_g >= 0) & (lane_g < nz * 16)

    def lap(centre, low, high):
        total = roll(centre, 1, 0) + roll(centre, -1, 0) + roll(centre, 1, 1) + roll(centre, -1, 1)
        if low is not None:
            total = total + low
        if high is not None:
            total = total + high
        return total - 6.0 * centre

    def fine_bend(a, _):
        for j in range(8):
            block = jnp.concatenate([ctl[a, j], jnp.zeros((8, 112), F32)], 1)
            block = jnp.concatenate([block, zero8], 0)
            fw[j + 2] = roll(roll(block, 2, 0), FB + 2, 1)
        zero16 = jnp.zeros((16, 128), F32)
        for j in (0, 1, 10, 11):
            fw[j] = zero16
        first = []
        for j in range(12):
            if j in (0, 11):
                first.append(None)
                continue
            low = fw[j - 1] if 0 < j else None
            high = fw[j + 1] if j < 11 else None
            value = lap(fw[j], low, high)
            p = gx * 8 + j - 2
            ok = in_grid & (p >= 0) & (p < nx * 8)
            first.append(jnp.where(ok, value, 0.0))
        for j in range(12):
            centre = first[j] if first[j] is not None else zero16
            low = first[j - 1] if j > 0 else None
            high = first[j + 1] if j < 11 else None
            e[a, j] = BEND * lap(centre, low, high)
        return 0

    lax.fori_loop(0, 3, fine_bend, 0)

    kx, ky, kz = cctl.shape[1:]
    shape = (ky, kz)
    crow = lax.broadcasted_iota(jnp.int32, (ky, 128), 0)
    clane = lanes((ky, 128))

    def clap(centre, low, high):
        total = jnp.where(crow > 0, roll(centre, 1, 0), 0.0) + jnp.where(crow < ky - 1, roll(centre, -1, 0), 0.0)
        total = total + roll(centre, 1, 1) + roll(centre, -1, 1)
        if low is not None:
            total = total + low
        if high is not None:
            total = total + high
        return jnp.where(clane < kz, total - 6.0 * centre, 0.0)

    def coarse_bend(a, _):
        field = [jnp.concatenate([cctl[a, j], jnp.zeros((ky, 128 - kz), F32)], 1) for j in range(kx)]
        for _level in range(2):
            field = [clap(field[j], field[j - 1] if j else None, field[j + 1] if j < kx - 1 else None)
                     for j in range(kx)]
        for j in range(kx):
            coarse_out[a, j] = BEND * field[j][:, :kz]
        return 0

    lax.fori_loop(0, 3, coarse_bend, 0)

    for k in range(6):
        arrived(halo, k)

    def place_y(x, _):
        sp[x + 2, 6:8, :] = hyr[0, x]
        sp[x + 2, 72:74, :] = hyr[1, x]
        return 0

    lax.fori_loop(0, 64, place_y, 0, unroll=8)

    m4 = lane64 % 4
    for h in range(2):
        u = jnp.where(m4 < 2, hzr[0, h], hzr[1, h])
        a_part = jnp.where(m4 < 2, -roll(u, -2, 1), roll(u, 2, 1))
        b_part = jnp.where(m4 == 1, 8.0 * roll(u, -1, 1), jnp.where(m4 == 2, -8.0 * roll(u, 1, 1), 0.0))
        cz[h] = a_part + b_part
    edge = (lane64 < 2) | (lane64 >= 126)

    def z_fix(c, _):
        base = pl.multiple_of(c * planes, planes)
        q = lax.rem(c, 4)
        part = pltpu.roll(cz[c // 4], lax.rem(128 - 32 * q, 128), 1)
        for j in range(planes):
            dzb[base + j] = dzb[base + j] + jnp.where(edge, roll(part, -(4 * j + 2), 1), 0.0)
        return 0

    lax.fori_loop(0, chunks, z_fix, 0)

    groups = 16
    slabs = groups + 3

    def column(yt, _):
        r0 = pl.multiple_of(8 * yt, 8)

        def put(a, g, value):
            xs[pl.ds(r0, 8), pl.ds(pl.multiple_of((a * slabs + g) * 128, 128), 128)] = value

        def pair(gg, acc):
            acc = [list(row) for row in acc]
            x0 = 8 * gg
            c = [sp[x0 + i, pl.ds(r0 + 8, 8), :] for i in range(12)]
            for sub in range(2):
                for k in range(4):
                    i = 4 * sub + k
                    plane = x0 + i + 2
                    sx = (c[i] - c[i + 4]) + 8.0 * (c[i + 3] - c[i + 1])
                    ym2 = sp[plane, pl.ds(r0 + 6, 8), :]
                    ym1 = sp[plane, pl.ds(r0 + 7, 8), :]
                    yp1 = sp[plane, pl.ds(r0 + 9, 8), :]
                    yp2 = sp[plane, pl.ds(r0 + 10, 8), :]
                    sy = (ym2 - yp2) + 8.0 * (yp1 - ym1)
                    sz = dzb[x0 + i, pl.ds(r0, 8), :]
                    diff = wb[x0 + i, pl.ds(r0, 8), :]
                    for a, s in enumerate((sx, sy, sz)):
                        f = diff * s
                        for m in range(4):
                            acc[a][m] = acc[a][m] + float(W4[k, m]) * f
                for a in range(3):
                    put(a, 2 * gg + sub, acc[a][0])
                    acc[a] = [acc[a][1], acc[a][2], acc[a][3], jnp.zeros((8, 128), F32)]
            return tuple(tuple(row) for row in acc)

        acc = lax.fori_loop(0, groups // 2, pair, tuple(tuple(zero8 for _ in range(4)) for _ in range(3)))
        for a in range(3):
            for m in range(3):
                put(a, groups + m, acc[a][m])
        return 0

    lax.fori_loop(0, 8, column, 0)

    for a in range(3):
        x = xs[:, a * slabs * 128 : (a + 1) * slabs * 128]
        hi, lo = split(x)
        y = jnp.dot(wy[...], jnp.concatenate([hi, lo], 0), preferred_element_type=F32)
        y = y[:24] + y[24:]
        y = jnp.concatenate([y[:, 128 * i : 128 * (i + 1)] for i in range(slabs)], 0)
        hi, lo = split(y)
        z = jnp.dot(jnp.concatenate([hi, lo], 1), wz[a], preferred_element_type=F32)
        z = z[:, :128] + z[:, 128:]
        for i in range(slabs):
            zs[a, i] = z[24 * i : 24 * (i + 1)]

    total = [zs[0, i, 16:24, :] + zs[1, i, 16:24, :] + zs[2, i, 16:24, :] for i in range(slabs)]
    for jj in range(6):
        v = None
        for i in range(slabs):
            tap = i - 8 * jj + 25
            if 0 <= tap < 29:
                term = float(C29[tap]) * total[i]
                v = term if v is None else v + term
        for dy in range(3):
            csend[jj // 2, dy, jj % 2] = v[2 * dy : 2 * dy + 2]

    def coarse_copy(d):
        slot = 9 * (d[0] + 1) + 3 * (d[1] + 1) + d[2] + 1
        return pltpu.make_async_remote_copy(
            src_ref=csend.at[d[0] + 1, d[1] + 1], dst_ref=crecv.at[slot],
            send_sem=cs.at[slot], recv_sem=cr.at[slot], device_id=at(d), device_id_type=MESH)

    far_first = sorted(neighbours, key=lambda d: -sum(map(abs, d)))
    for d in far_first:
        pl.when(exists(d))(lambda d=d: coarse_copy(d).start())

    for a in range(3):
        for j in range(12):
            v = e[a, j]
            for k in range(5):
                i = 2 * j - 4 + k
                if 0 <= i < slabs:
                    v = v + float(TWO[k]) * zs[a, i, 0:16, :]
            e[a, j] = v
    for k in (0, 1):
        start(fine_copy, k)

    own = csend[1, 1]
    low = jnp.zeros((2, 2, 128), F32)
    high = jnp.zeros((2, 2, 128), F32)
    for d in sorted(neighbours, key=lambda d: sum(map(abs, d))):
        back = tuple(-v for v in d)
        pl.when(exists(back))(lambda d=d: coarse_copy(d).wait_recv())
        slot = 9 * (d[0] + 1) + 3 * (d[1] + 1) + d[2] + 1
        piece = jnp.where(exists(back), crecv[slot], 0.0)
        if d[2] == 0:
            own = own + piece
        elif d[2] == 1:
            low = low + piece
        else:
            high = high + piece
    l4 = lanes((2, 2, 128))
    r_in = l4 % 32
    inner = l4 < 96
    own = jnp.where(inner & (r_in >= 2) & (r_in < 6), own, 0.0)
    own = own + jnp.where(inner & (r_in >= 2) & (r_in < 4), roll(low, -4, 2), 0.0)
    own = own + jnp.where(inner & (r_in >= 4) & (r_in < 6), roll(high, 4, 2), 0.0)
    shift = lax.rem(4 * gz + 126, 128)
    zg[gz] = jnp.stack([pltpu.roll(own[i], shift, 1) for i in range(2)])

    def gather_copy(axis, o):
        device, _ = ring(axis, o)
        if axis == 2:
            src = dst = zg.at[gz]
        elif axis == 1:
            src = dst = yg.at[:, gy]
        else:
            src, dst = yg, xg.at[gx]
        return pltpu.make_async_remote_copy(
            src_ref=src, dst_ref=dst, send_sem=gs.at[axis, o], recv_sem=gr.at[axis, o],
            device_id=device, device_id_type=MESH)

    def offsets(axis):
        n = dims[axis]
        return sorted(range(1, n), key=lambda o: -min(o, n - o))

    def gather_start(axis):
        for o in offsets(axis):
            gather_copy(axis, o).start()

    def gather_wait(axis):
        n = dims[axis]
        for o in reversed(offsets(axis)):
            s = lax.rem(pos[axis] + n - o, n)
            dst = (xg.at[s], yg.at[:, s], zg.at[s])[axis]
            src = yg if axis == 0 else dst
            pltpu.make_async_remote_copy(
                src_ref=src, dst_ref=dst, send_sem=gs.at[axis, o], recv_sem=gr.at[axis, o],
                device_id=ring(axis, o)[0], device_id_type=MESH).wait_recv()

    gather_start(2)

    for k in (0, 1):
        sent(fine_copy, k)
        arrived(fine_copy, k)
    for a in range(3):
        for j in range(8):
            v = e[a, j + 2]
            if j < 2:
                v = v + fxr[0, a, j]
            if j >= 6:
                v = v + fxr[1, a, j - 6]
            e[a, j + 2] = v
            fys[0, 8 * a + j] = v[0:2]
            fys[1, 8 * a + j] = v[10:12]
    for k in (2, 3):
        start(fine_copy, k)

    gather_wait(2)
    line = zg[0]
    for s in range(1, nz):
        line = line + zg[s]
    yg[:, gy] = line
    gather_start(1)

    for k in (2, 3):
        arrived(fine_copy, k)
    lane8 = lanes((8, 128))
    pack0 = zero8
    pack1 = zero8
    zero4 = jnp.zeros((4, 128), F32)
    for a in range(3):
        for j in range(8):
            s = 8 * a + j
            v = e[a, j + 2]
            edges = jnp.concatenate([fyr[0, s], zero4, fyr[1, s]], 0)
            v = roll(v, -2, 0)[0:8] + edges
            e[a, j + 2, 0:8, :] = v
            turned = roll(v, 2 * s - FB, 1)
            pack0 = jnp.where(lane8 // 2 == s, turned, pack0)
            pack1 = jnp.where(lane8 // 2 == s + 9, turned, pack1)
    fzs[0] = pack0
    fzs[1] = pack1
    for k in (4, 5):
        start(fine_copy, k)

    gather_wait(1)
    xg[gx] = yg[...]
    gather_start(0)

    for k in (4, 5):
        arrived(fine_copy, k)
    p0 = fzr[0]
    p1 = fzr[1]
    for a in range(3):
        for j in range(8):
            s = 8 * a + j
            v = roll(e[a, j + 2, 0:8, :], -(FB + 2), 1)
            v = v + jnp.where(lane8 < 2, roll(p0, -(18 + 2 * s), 1), 0.0)
            v = v + jnp.where((lane8 >= 14) & (lane8 < 16), roll(p1, 14 - 2 * s, 1), 0.0)
            fine_out[a, j] = v[:, :16]

    gather_wait(0)
    for g in range(nx):
        for p in range(2):
            rows = xg[g, p].reshape(ky, 128)
            for a in range(3):
                coarse_out[a, 2 * g + p] = coarse_out[a, 2 * g + p] + rows[:, 32 * a : 32 * a + kz]

    for k in range(6):
        sent(halo, k)
    for k in range(2, 6):
        sent(fine_copy, k)
    for d in neighbours:
        pl.when(exists(d))(lambda d=d: coarse_copy(d).wait_send())
    for axis in range(3):
        for o in range(1, dims[axis]):
            gather_copy(axis, o).wait_send()


def per_device(dims, warped_image, fixed_image, fine_control, coarse_control):
    sx, sy, sz = warped_image.shape
    kx, ky, kz = coarse_control.shape[1:]
    nx, ny, nz = dims
    wide = max(dims)
    slabs = 19
    vmem = pl.BlockSpec(memory_space=pltpu.VMEM)
    hbm = pl.BlockSpec(memory_space=pl.ANY)
    v = lambda *shape: pltpu.VMEM(shape, F32)
    dma = pltpu.SemaphoreType.DMA
    return pl.pallas_call(
        lambda *refs: kernel(dims, *refs),
        out_shape=(
            jax.ShapeDtypeStruct(fine_control.shape, F32),
            jax.ShapeDtypeStruct(coarse_control.shape, F32),
        ),
        in_specs=[hbm, hbm, vmem, vmem, vmem, vmem, vmem],
        out_specs=(vmem, vmem),
        scratch_shapes=[
            v(sx, sy, sz), v(sx, sy, sz), v(sx + 4, sy + 16, sz),
            v(2, sx, 2, sz), v(2, sx, 2, sz), v(2, sy, 128), v(2, 2, sy, 128), v(2, sy, 128),
            v(sx, sy, sz), v(sy, 3 * slabs * 128), v(3, slabs, 24, 128), v(3, 12, 16, 128),
            v(3, 3, 2, 2, 128), v(27, 2, 2, 128), v(nz, 2, 2, 128), v(2, ny, 2, 128), v(nx, 2, ny, 2, 128),
            v(2, 3, 2, 16, 128), v(2, 24, 2, 128), v(2, 24, 2, 128), v(2, 8, 128), v(2, 8, 128), v(12, 16, 128),
            dma((2, 8)), dma((6,)), dma((6,)), dma((27,)), dma((27,)),
            dma((3, wide)), dma((3, wide)), dma((6,)), dma((6,)),
        ],
        compiler_params=pltpu.CompilerParams(collective_id=0, has_side_effects=True, vmem_limit_bytes=48 << 20),
        name="gradient",
    )(warped_image, fixed_image, fine_control, coarse_control,
      jnp.asarray(y_matrix(sy)), jnp.asarray(z_matrices(sz)), jnp.asarray(d_matrix(sz)))


def solution(mesh):
    dims = tuple(mesh.shape[a] for a in ("gx", "gy", "gz"))
    in_specs = (P("gx", "gy", "gz"), P("gx", "gy", "gz"), P(None, "gx", "gy", "gz"), P())
    out_specs = (P(None, "gx", "gy", "gz"), P())
    return jax.shard_map(
        lambda *args: per_device(dims, *args), mesh=mesh, in_specs=in_specs, out_specs=out_specs, check_vma=False
    )
```

```python
import itertools

import jax
import jax.numpy as jnp
import numpy as np
from jax import lax
from jax.experimental import pallas as pl
from jax.experimental.pallas import tpu as pltpu
from jax.sharding import PartitionSpec as P

SPF = 8
SPC = 32
BEND = 0.01
FB = 0
MESH = pl.DeviceIdType.MESH
F32 = jnp.float32
BF16 = jnp.bfloat16


def beta(t):
    m = np.abs(t)
    r = 2.0 - m
    return np.where(m < 1.0, 2.0 / 3.0 - m * m + 0.5 * m**3, np.where(m < 2.0, r**3 / 6.0, 0.0))


def basis(voxels, points, spacing, first):
    v = np.arange(voxels)[:, None] + 0.5
    c = (np.arange(points)[None, :] + first) * spacing + 0.5 * spacing
    return beta((v - c) / spacing)


def halves(w):
    hi = np.asarray(w, np.float32).astype(jnp.bfloat16)
    lo = (np.asarray(w, np.float64) - hi.astype(np.float64)).astype(np.float32).astype(jnp.bfloat16)
    return hi, lo


W4 = beta((np.arange(4)[:, None] + 4.5 - 4.0 * np.arange(4)[None, :]) / 4.0) / 24.0
TWO = np.array([1.0, 4.0, 6.0, 4.0, 1.0]) / 8.0


def spread(c, step):
    out = np.zeros((len(c) - 1) * step + 1)
    out[::step] = c
    return out


C29 = np.convolve(np.convolve(TWO, spread(TWO, 2)), spread(TWO, 4))


def y_matrix(sy):
    rows = np.zeros((24, sy))
    rows[:12] = basis(sy, 12, SPF, -2).T * SPF**-1.5
    rows[16:22] = basis(sy, 6, SPC, -2).T * SPC**-1.5
    hi, lo = halves(rows)
    return np.concatenate([np.concatenate([hi, hi], 1), np.concatenate([lo, lo], 1)], 0)


def stacked(cols):
    hi, lo = halves(cols)
    half = np.concatenate([hi, lo], 1)
    return np.concatenate([half, half], 0)


def z_matrices(sz):
    fine = np.zeros((sz, 128))
    fine[:, FB : FB + 20] = basis(sz, 20, SPF, -2)
    out = [stacked(fine)]
    for a in range(3):
        cols = np.zeros((sz, 128))
        for piece in range(4):
            first = 32 * piece + 8 * a
            cols[:, first : first + 8] = basis(sz, 8, SPC, -2)
        out.append(stacked(cols))
    return np.stack(out)


def d_matrix(sz):
    d = np.zeros((sz, sz), np.float32)
    for shift, value in ((-2, 1.0), (-1, -8.0), (1, 8.0), (2, -1.0)):
        for v in range(sz):
            if 0 <= v + shift < sz:
                d[v + shift, v] = value
    return np.concatenate([d, d], 0).astype(jnp.bfloat16)


def h_matrix(sz):
    h = np.zeros((128, sz), np.float32)
    for lane in range(128):
        h[lane, (sz - 2, sz - 1, 0, 1)[lane % 4]] = 1.0
    return np.concatenate([h, h], 0).astype(jnp.bfloat16)


def split(x):
    hi = x.astype(BF16)
    return hi, (x - hi.astype(F32)).astype(BF16)


def lanes(shape):
    return lax.broadcasted_iota(jnp.int32, shape, len(shape) - 1)


def roll(x, shift, axis):
    return pltpu.roll(x, shift % x.shape[axis] if isinstance(shift, int) else shift, axis)


class Place:
    def __init__(self, dims):
        self.dims = dims
        self.pos = tuple(lax.axis_index(a) for a in ("gx", "gy", "gz"))
        self.has = [{-1: p > 0, 1: p < n - 1} for p, n in zip(self.pos, dims)]

    def exists(self, d):
        cond = None
        for i in range(3):
            if d[i]:
                one = self.has[i][d[i]]
                cond = one if cond is None else jnp.logical_and(cond, one)
        return cond

    def at(self, d):
        return tuple(self.pos[i] + d[i] for i in range(3))

    def ring(self, axis, o):
        t = lax.rem(self.pos[axis] + o, self.dims[axis])
        return tuple(t if i == axis else self.pos[i] for i in range(3)), t

    def seen(self, dx, dy):
        return self.exists((dx, dy, 0))

    def if_seen(self, dx, dy, fn):
        if dx or dy:
            pl.when(self.seen(dx, dy))(fn)
        else:
            fn()

    def beside(self, dx, dy, o):
        gx, gy, gz = self.pos
        return (gx + dx, gy + dy, lax.rem(gz + o, self.dims[2]))

    def start(self, make, k):
        d, copy = make(k)
        pl.when(self.exists(d))(lambda: copy.start())

    def sent(self, make, k):
        d, copy = make(k)
        pl.when(self.exists(d))(lambda: copy.wait_send())

    def arrived(self, make, k):
        d, copy = make(k)
        pl.when(self.exists([-v for v in d]))(lambda: copy.wait_recv())


def ring_order(n):
    return sorted(range(n), key=lambda o: -min(o, n - o))


SIDES = list(itertools.product((-1, 0, 1), repeat=2))


def layers(dims, w_hbm, f_hbm, ctl_h, dz_h, sp, diff, dzb, cz, e,
           ctl, dz_w, small_sem, wb, fb, hys, hyr, hzs, hzr, fw, img_sem, hs, hr):
    nx, ny, nz = dims
    here = Place(dims)
    pos = here.pos
    gx, gy, gz = pos
    has, exists, at, ring, seen, if_seen, beside = (
        here.has, here.exists, here.at, here.ring, here.seen, here.if_seen, here.beside)
    start, sent, arrived = here.start, here.sent, here.arrived
    sides = SIDES
    zero8 = jnp.zeros((8, 128), F32)
    lane64 = lanes((64, 128))

    bar = pltpu.get_barrier_semaphore()
    count = 0
    for axis in range(3):
        for side in (-1, 1):
            d = tuple(side if i == axis else 0 for i in range(3))
            pl.when(exists(d))(lambda d=d: pl.semaphore_signal(bar, inc=1, device_id=at(d), device_id_type=MESH))
            count = count + has[axis][side].astype(jnp.int32)

    chunks = 8
    planes = 8
    for c in range(chunks):
        part = pl.ds(c * planes, planes)
        pltpu.make_async_copy(w_hbm.at[part], wb.at[part], img_sem.at[0, c]).start()
        pltpu.make_async_copy(f_hbm.at[part], fb.at[part], img_sem.at[1, c]).start()
    small = [pltpu.make_async_copy(dz_h, dz_w, small_sem.at[0]), pltpu.make_async_copy(ctl_h, ctl, small_sem.at[1])]
    for copy in small:
        copy.start()

    for side, d in ((0, -1), (1, 1)):
        @pl.when(jnp.logical_not(has[0][d]))
        def _(side=side):
            sp[66 * side : 66 * side + 2, 8:72, :] = jnp.zeros((2, 64, 128), F32)

        @pl.when(jnp.logical_not(has[1][d]))
        def _(side=side):
            hyr[side] = jnp.zeros(hyr.shape[1:], F32)

        @pl.when(jnp.logical_not(has[2][d]))
        def _(side=side):
            hzr[side] = jnp.zeros(hzr.shape[1:], F32)

    hzs[...] = jnp.zeros(hzs.shape, F32)


    def sum_chunk(c, _):
        base = pl.multiple_of(c * planes, planes)
        part = pl.ds(base, planes)
        pltpu.make_async_copy(w_hbm.at[part], wb.at[part], img_sem.at[0, c]).wait()
        pltpu.make_async_copy(f_hbm.at[part], fb.at[part], img_sem.at[1, c]).wait()
        h = c // 4
        group = lane64 // 4 - 8 * lax.rem(c, 4)
        packed = hzs[h]
        for j in range(planes):
            w = wb[base + j]
            f = fb[base + j]
            s = w + f
            diff[base + j] = w - f
            sp[base + j + 2, 8:72, :] = s
            hys[0, base + j] = s[0:2]
            hys[1, base + j] = s[62:64]
            turned = pltpu.roll(s, 32 * lax.rem(c, 4) + 4 * j + 2, 1)
            packed = jnp.where(group == j, turned, packed)
        hzs[h] = packed
        return 0

    lax.fori_loop(0, chunks, sum_chunk, 0)
    pl.semaphore_wait(bar, count)

    def halo(k):
        axis, side = k // 2, k % 2
        d = [0, 0, 0]
        d[axis] = 2 * side - 1
        if axis == 0:
            src = sp.at[pl.ds(2 if side == 0 else 64, 2), pl.ds(8, 64), :]
            dst = sp.at[pl.ds(66 if side == 0 else 0, 2), pl.ds(8, 64), :]
        elif axis == 1:
            src, dst = hys.at[side], hyr.at[1 - side]
        else:
            src, dst = hzs, hzr.at[1 - side]
        return d, pltpu.make_async_remote_copy(
            src_ref=src, dst_ref=dst, send_sem=hs.at[k], recv_sem=hr.at[k],
            device_id=at(d), device_id_type=MESH)

    for k in (4, 5, 2, 3, 0, 1):
        start(halo, k)

    small[0].wait()

    def dz_chunk(c, _):
        base = pl.multiple_of(c * 16, 16)
        for half in range(2):
            parts = [jnp.concatenate(split(sp[base + 8 * half + j + 2, 8:72, :]), 1) for j in range(8)]
            out = jnp.dot(jnp.concatenate(parts, 0), dz_w[...], preferred_element_type=F32)
            for j in range(8):
                dzb[base + 8 * half + j] = out[64 * j : 64 * (j + 1)]
        return 0

    lax.fori_loop(0, 4, dz_chunk, 0)

    small[1].wait()

    row16 = lax.broadcasted_iota(jnp.int32, (16, 128), 0)
    lane16 = lanes((16, 128))
    row_g = row16 - 2 + gy * 8
    lane_g = lane16 - (FB + 2) + gz * 16
    in_grid = (row_g >= 0) & (row_g < ny * 8) & (lane_g >= 0) & (lane_g < nz * 16)

    def lap(centre, low, high):
        total = roll(centre, 1, 0) + roll(centre, -1, 0) + roll(centre, 1, 1) + roll(centre, -1, 1)
        if low is not None:
            total = total + low
        if high is not None:
            total = total + high
        return total - 6.0 * centre

    def fine_bend(a, _):
        for j in range(8):
            block = jnp.concatenate([ctl[a, j], jnp.zeros((8, 112), F32)], 1)
            block = jnp.concatenate([block, zero8], 0)
            fw[j + 2] = roll(roll(block, 2, 0), FB + 2, 1)
        zero16 = jnp.zeros((16, 128), F32)
        for j in (0, 1, 10, 11):
            fw[j] = zero16
        first = []
        for j in range(12):
            if j in (0, 11):
                first.append(None)
                continue
            low = fw[j - 1] if 0 < j else None
            high = fw[j + 1] if j < 11 else None
            value = lap(fw[j], low, high)
            p = gx * 8 + j - 2
            ok = in_grid & (p >= 0) & (p < nx * 8)
            first.append(jnp.where(ok, value, 0.0))
        for j in range(12):
            centre = first[j] if first[j] is not None else zero16
            low = first[j - 1] if j > 0 else None
            high = first[j + 1] if j < 11 else None
            e[a, j] = BEND * lap(centre, low, high)
        return 0

    lax.fori_loop(0, 3, fine_bend, 0)

    for k in range(6):
        arrived(halo, k)

    def place_y(x, _):
        sp[x + 2, 6:8, :] = hyr[0, x]
        sp[x + 2, 72:74, :] = hyr[1, x]
        return 0

    lax.fori_loop(0, 64, place_y, 0, unroll=8)

    m4 = lane64 % 4
    for h in range(2):
        u = jnp.where(m4 < 2, hzr[0, h], hzr[1, h])
        a_part = jnp.where(m4 < 2, -roll(u, -2, 1), roll(u, 2, 1))
        b_part = jnp.where(m4 == 1, 8.0 * roll(u, -1, 1), jnp.where(m4 == 2, -8.0 * roll(u, 1, 1), 0.0))
        cz[h] = a_part + b_part
    for k in range(6):
        sent(halo, k)


def gradient(dims, sp, diff, dzb, cz, e0, cctl_h, wy_h, wz_h, h_h, fine_out, coarse_out,
             cctl, wy, wz, h_w, small_sem, dz2, xs, zs, e, csend, crecv, yg, xg, mix,
             fxr, fys, fyr, fzs, fzr, cs, cr, gs, gr, fs, fr):
    nx, ny, nz = dims
    here = Place(dims)
    pos = here.pos
    gx, gy, gz = pos
    has, exists, at, ring, seen, if_seen, beside = (
        here.has, here.exists, here.at, here.ring, here.seen, here.if_seen, here.beside)
    start, sent, arrived = here.start, here.sent, here.arrived
    sides = SIDES
    zero8 = jnp.zeros((8, 128), F32)
    lane64 = lanes((64, 128))

    small = [pltpu.make_async_copy(src, dst, small_sem.at[i]) for i, (src, dst) in enumerate(
        ((h_h, h_w), (wy_h, wy), (wz_h, wz), (cctl_h, cctl)))]
    for copy in small:
        copy.start()

    bar = pltpu.get_barrier_semaphore()
    for dx, dy in sides:
        def greet(dx=dx, dy=dy):
            for o in ring_order(nz):
                if dx or dy or o:
                    pl.semaphore_signal(bar, inc=1, device_id=beside(dx, dy, o), device_id_type=MESH)
        if_seen(dx, dy, greet)
    for axis in range(2):
        for o in range(2, dims[axis] - 1):
            device, t = ring(axis, o)
            pl.when(jnp.abs(t - pos[axis]) > 1)(lambda device=device: pl.semaphore_signal(
                bar, inc=1, device_id=device, device_id_type=MESH))
        for o in (1, dims[axis] - 1):
            device, t = ring(axis, o)
            pl.when(jnp.abs(t - pos[axis]) > 1)(lambda device=device: pl.semaphore_signal(
                bar, inc=1, device_id=device, device_id_type=MESH))
    wide = [1 + h[-1].astype(jnp.int32) + h[1].astype(jnp.int32) for h in has]
    greeted = wide[0] * wide[1] * nz - 1 + (nx - wide[0]) + (ny - wide[1])

    for side, d in ((0, -1), (1, 1)):
        for axis, ref in enumerate((fxr, fyr, fzr)):
            @pl.when(jnp.logical_not(has[axis][d]))
            def _(side=side, ref=ref):
                ref[side] = jnp.zeros(ref.shape[1:], F32)
    for dx, dy in sides:
        if dx or dy:
            @pl.when(jnp.logical_not(seen(-dx, -dy)))
            def _(dx=dx, dy=dy):
                crecv[3 * (dx + 1) + dy + 1] = zero8

    def fine_copy(k):
        axis, side = k // 2, k % 2
        d = [0, 0, 0]
        d[axis] = 2 * side - 1
        if axis == 0:
            src, dst = e.at[:, pl.ds(10 * side, 2)], fxr.at[1 - side]
        elif axis == 1:
            src, dst = fys.at[side], fyr.at[1 - side]
        else:
            src, dst = fzs.at[side], fzr.at[1 - side]
        return d, pltpu.make_async_remote_copy(
            src_ref=src, dst_ref=dst, send_sem=fs.at[k], recv_sem=fr.at[k],
            device_id=at(d), device_id_type=MESH)

    small[0].wait()

    def z_fix(c, _):
        base = pl.multiple_of(c * 16, 16)
        layer = cz[c // 2]
        for half in range(2):
            group = lane64 // 4 - 16 * lax.rem(c, 2) - 8 * half
            parts = [jnp.concatenate(split(jnp.where(group == j, layer, 0.0)), 1) for j in range(8)]
            out = jnp.dot(jnp.concatenate(parts, 0), h_w[...], preferred_element_type=F32)
            for j in range(8):
                dz2[base + 8 * half + j] = dzb[base + 8 * half + j] + out[64 * j : 64 * (j + 1)]
        return 0

    lax.fori_loop(0, 4, z_fix, 0)

    groups = 16
    slabs = groups + 3

    def column(yt, _):
        r0 = pl.multiple_of(8 * yt, 8)

        def put(a, g, value):
            xs[pl.ds(r0, 8), pl.ds(pl.multiple_of((a * slabs + g) * 128, 128), 128)] = value

        def pair(gg, acc):
            acc = [list(row) for row in acc]
            x0 = 8 * gg
            c = [sp[x0 + i, pl.ds(r0 + 8, 8), :] for i in range(12)]
            for sub in range(2):
                for k in range(4):
                    i = 4 * sub + k
                    plane = x0 + i + 2
                    sx = (c[i] - c[i + 4]) + 8.0 * (c[i + 3] - c[i + 1])
                    ym2 = sp[plane, pl.ds(r0 + 6, 8), :]
                    ym1 = sp[plane, pl.ds(r0 + 7, 8), :]
                    yp1 = sp[plane, pl.ds(r0 + 9, 8), :]
                    yp2 = sp[plane, pl.ds(r0 + 10, 8), :]
                    sy = (ym2 - yp2) + 8.0 * (yp1 - ym1)
                    sz = dz2[x0 + i, pl.ds(r0, 8), :]
                    dv = diff[x0 + i, pl.ds(r0, 8), :]
                    for a, s in enumerate((sx, sy, sz)):
                        f = dv * s
                        for m in range(4):
                            acc[a][m] = acc[a][m] + float(W4[k, m]) * f
                for a in range(3):
                    put(a, 2 * gg + sub, acc[a][0])
                    acc[a] = [acc[a][1], acc[a][2], acc[a][3], jnp.zeros((8, 128), F32)]
            return tuple(tuple(row) for row in acc)

        acc = lax.fori_loop(0, groups // 2, pair, tuple(tuple(zero8 for _ in range(4)) for _ in range(3)))
        for a in range(3):
            for m in range(3):
                put(a, groups + m, acc[a][m])
        return 0

    lax.fori_loop(0, 8, column, 0)

    for copy in small[1:]:
        copy.wait()
    total = None
    for a in range(3):
        x = xs[:, a * slabs * 128 : (a + 1) * slabs * 128]
        hi, lo = split(x)
        y = jnp.dot(wy[...], jnp.concatenate([hi, lo], 0), preferred_element_type=F32)
        y = y[:24] + y[24:]
        pieces = [y[:, 128 * i : 128 * (i + 1)] for i in range(slabs)]
        hi, lo = split(jnp.concatenate([p[16:24] for p in pieces], 0))
        z = jnp.dot(jnp.concatenate([hi, lo], 1), wz[1 + a], preferred_element_type=F32)
        z = z[:, :128] + z[:, 128:]
        total = z if total is None else total + z
        hi, lo = split(jnp.concatenate([p[:16] for p in pieces], 0))
        z = jnp.dot(jnp.concatenate([hi, lo], 1), wz[0], preferred_element_type=F32)
        z = z[:, :128] + z[:, 128:]
        for i in range(slabs):
            zs[a, i] = z[16 * i : 16 * (i + 1)]

    lane8 = lanes((8, 128))
    taken = []
    for jj in range(6):
        v = None
        for i in range(slabs):
            tap = i - 8 * jj + 25
            if 0 <= tap < 29:
                term = float(C29[tap]) * total[8 * i : 8 * (i + 1)]
                v = term if v is None else v + term
        taken.append(v)
    for g in range(3):
        v = jnp.where(lane8 < 64, taken[2 * g], taken[2 * g + 1])
        csend[g] = jnp.where(lane8 // 32 % 2 == 0, v, roll(v, -1, 0))
    crecv[4, pl.ds(gz, 1), :] = csend[1, 2:3, :]

    def coarse_copy(dx, dy, o):
        slot = 3 * (dx + 1) + dy + 1
        return pltpu.make_async_remote_copy(
            src_ref=csend.at[dx + 1, pl.ds(2 * (dy + 1), 1), :], dst_ref=crecv.at[slot, pl.ds(gz, 1), :],
            send_sem=cs.at[slot, o], recv_sem=cr.at[slot, o], device_id=beside(dx, dy, o), device_id_type=MESH)

    def coarse_arrival(dx, dy, o):
        slot = 3 * (dx + 1) + dy + 1
        s = lax.rem(gz + nz - o, nz)
        return pltpu.make_async_remote_copy(
            src_ref=csend.at[dx + 1, pl.ds(2 * (dy + 1), 1), :], dst_ref=crecv.at[slot, pl.ds(s, 1), :],
            send_sem=cs.at[slot, o], recv_sem=cr.at[slot, o], device_id=beside(dx, dy, o), device_id_type=MESH)

    def coarse_all(fn):
        for o in ring_order(nz):
            for dx, dy in sorted(sides, key=lambda d: -abs(d[0]) - abs(d[1])):
                if o or dx or dy:
                    fn(dx, dy, o)

    pl.semaphore_wait(bar, greeted)
    coarse_all(lambda dx, dy, o: if_seen(dx, dy, lambda: coarse_copy(dx, dy, o).start()))

    for a in range(3):
        for j in range(12):
            v = e0[a, j]
            for k in range(5):
                i = 2 * j - 4 + k
                if 0 <= i < slabs:
                    v = v + float(TWO[k]) * zs[a, i]
            e[a, j] = v
    for k in (0, 1):
        start(fine_copy, k)

    coarse_all(lambda dx, dy, o: if_seen(-dx, -dy, lambda: coarse_arrival(dx, dy, o).wait_recv()))
    line = crecv[0]
    for i in range(1, 9):
        line = line + crecv[i]
    line = pltpu.roll(line, 0, 1, stride=4, stride_axis=0)
    place = lane8 % 32 + 2 - 4 * lax.broadcasted_iota(jnp.int32, (8, 128), 0)
    for a in range(3):
        piece = jnp.where((place >= 0) & (place < 8), roll(line, -2 - 8 * a, 1), 0.0)
        yg[a, pl.ds(gy, 1), :] = jnp.sum(piece, axis=0, keepdims=True)

    def gather_copy(axis, o):
        device, _ = ring(axis, o)
        if axis == 1:
            src = dst = yg.at[:, pl.ds(gy, 1), :]
        else:
            src, dst = yg, xg.at[gx]
        return pltpu.make_async_remote_copy(
            src_ref=src, dst_ref=dst, send_sem=gs.at[axis, o], recv_sem=gr.at[axis, o],
            device_id=device, device_id_type=MESH)

    def offsets(axis):
        return ring_order(dims[axis])[:-1]

    def gather_start(axis):
        for o in offsets(axis):
            gather_copy(axis, o).start()

    def gather_wait(axis):
        n = dims[axis]
        for o in reversed(offsets(axis)):
            s = lax.rem(pos[axis] + n - o, n)
            dst = (xg.at[s], yg.at[:, pl.ds(s, 1), :])[axis]
            src = yg if axis == 0 else dst
            pltpu.make_async_remote_copy(
                src_ref=src, dst_ref=dst, send_sem=gs.at[axis, o], recv_sem=gr.at[axis, o],
                device_id=ring(axis, o)[0], device_id_type=MESH).wait_recv()

    gather_start(1)

    kx, ky, kz = cctl.shape[1:]
    shape = (ky, kz)
    crow = lax.broadcasted_iota(jnp.int32, (ky, 128), 0)
    clane = lanes((ky, 128))

    def clap(centre, low, high):
        total = jnp.where(crow > 0, roll(centre, 1, 0), 0.0) + jnp.where(crow < ky - 1, roll(centre, -1, 0), 0.0)
        total = total + roll(centre, 1, 1) + roll(centre, -1, 1)
        if low is not None:
            total = total + low
        if high is not None:
            total = total + high
        return jnp.where(clane < kz, total - 6.0 * centre, 0.0)

    def coarse_bend(a, _):
        field = [jnp.concatenate([cctl[a, j], jnp.zeros((ky, 128 - kz), F32)], 1) for j in range(kx)]
        for _level in range(2):
            field = [clap(field[j], field[j - 1] if j else None, field[j + 1] if j < kx - 1 else None)
                     for j in range(kx)]
        for j in range(kx):
            coarse_out[a, j] = BEND * field[j][:, :kz]
        return 0

    lax.fori_loop(0, 3, coarse_bend, 0)

    for k in (0, 1):
        sent(fine_copy, k)
        arrived(fine_copy, k)
    for a in range(3):
        for j in range(8):
            v = e[a, j + 2]
            if j < 2:
                v = v + fxr[0, a, j]
            if j >= 6:
                v = v + fxr[1, a, j - 6]
            e[a, j + 2] = v
            fys[0, 8 * a + j] = v[0:2]
            fys[1, 8 * a + j] = v[10:12]
    for k in (2, 3):
        start(fine_copy, k)

    gather_wait(1)
    xg[gx] = yg[...]
    gather_start(0)

    for k in (2, 3):
        arrived(fine_copy, k)
    pack0 = zero8
    pack1 = zero8
    zero4 = jnp.zeros((4, 128), F32)
    for a in range(3):
        for j in range(8):
            s = 8 * a + j
            v = e[a, j + 2]
            edges = jnp.concatenate([fyr[0, s], zero4, fyr[1, s]], 0)
            v = roll(v, -2, 0)[0:8] + edges
            e[a, j + 2, 0:8, :] = v
            turned = roll(v, 2 * s - FB, 1)
            pack0 = jnp.where(lane8 // 2 == s, turned, pack0)
            pack1 = jnp.where(lane8 // 2 == s + 9, turned, pack1)
    fzs[0] = pack0
    fzs[1] = pack1
    for k in (4, 5):
        start(fine_copy, k)

    for k in (4, 5):
        arrived(fine_copy, k)
    p0 = fzr[0]
    p1 = fzr[1]
    for a in range(3):
        for j in range(8):
            s = 8 * a + j
            v = roll(e[a, j + 2, 0:8, :], -(FB + 2), 1)
            v = v + jnp.where(lane8 < 2, roll(p0, -(18 + 2 * s), 1), 0.0)
            v = v + jnp.where((lane8 >= 14) & (lane8 < 16), roll(p1, 14 - 2 * s, 1), 0.0)
            fine_out[a, j] = v[:, :16]

    gather_wait(0)
    for g in range(nx):
        for a in range(3):
            rows = xg[g, a]
            for p in range(2):
                for q in range(2):
                    mix[a, 2 * g + p, pl.ds(q, ny, stride=2), :] = roll(rows, -(64 * p + 32 * q), 1)
    for a in range(3):
        for j in range(kx):
            coarse_out[a, j] = coarse_out[a, j] + mix[a, j][:, :kz]

    for k in range(2, 6):
        sent(fine_copy, k)
    coarse_all(lambda dx, dy, o: if_seen(dx, dy, lambda: coarse_copy(dx, dy, o).wait_send()))
    for axis in range(2):
        for o in range(1, dims[axis]):
            gather_copy(axis, o).wait_send()


def per_device(dims, warped_image, fixed_image, fine_control, coarse_control):
    sx, sy, sz = warped_image.shape
    kx, ky, kz = coarse_control.shape[1:]
    nx, ny, nz = dims
    wide = max(dims)
    slabs = 19
    vmem = pl.BlockSpec(memory_space=pltpu.VMEM)
    hbm = pl.BlockSpec(memory_space=pltpu.HBM)
    v = lambda *shape: pltpu.VMEM(shape, F32)
    h = lambda *shape: pltpu.VMEM(shape, BF16)
    out = lambda *shape: jax.ShapeDtypeStruct(shape, F32)
    dma = pltpu.SemaphoreType.DMA
    far = lambda x: pltpu.with_memory_space_constraint(jnp.asarray(x), pltpu.HBM)
    local = pl.pallas_call(
        lambda *refs: layers(dims, *refs),
        out_shape=(out(sx + 4, sy + 16, sz), out(sx, sy, sz), out(sx, sy, sz), out(2, sy, 128), out(3, 12, 16, 128)),
        in_specs=[hbm] * 4,
        out_specs=(vmem,) * 5,
        scratch_shapes=[
            v(*fine_control.shape), h(2 * sz, sz), dma((2,)), v(sx, sy, sz), v(sx, sy, sz),
            v(2, sx, 2, sz), v(2, sx, 2, sz), v(2, sy, 128), v(2, 2, sy, 128), v(12, 16, 128),
            dma((2, 8)), dma((6,)), dma((6,)),
        ],
        compiler_params=pltpu.CompilerParams(collective_id=0, has_side_effects=True, vmem_limit_bytes=24 << 20),
        name="layers",
    )(far(warped_image), far(fixed_image), far(fine_control), far(d_matrix(sz)))
    return pl.pallas_call(
        lambda *refs: gradient(dims, *refs),
        out_shape=(out(*fine_control.shape), out(*coarse_control.shape)),
        in_specs=[vmem] * 5 + [hbm] * 4,
        out_specs=(vmem, vmem),
        scratch_shapes=[
            v(*coarse_control.shape), h(48, 2 * sy), h(4, 2 * sz, 256), h(256, sz), dma((4,)),
            v(sx, sy, sz), v(sy, 3 * slabs * 128), v(3, slabs, 16, 128), v(3, 12, 16, 128),
            v(3, 8, 128), v(9, nz, 128), v(3, ny, 128), v(nx, 3, ny, 128), v(3, kx, ky, 128),
            v(2, 3, 2, 16, 128), v(2, 24, 2, 128), v(2, 24, 2, 128), v(2, 8, 128), v(2, 8, 128),
            dma((9, nz)), dma((9, nz)), dma((2, wide)), dma((2, wide)), dma((6,)), dma((6,)),
        ],
        compiler_params=pltpu.CompilerParams(collective_id=1, has_side_effects=True, vmem_limit_bytes=24 << 20),
        name="gradient",
    )(*local, far(coarse_control), far(y_matrix(sy)), far(z_matrices(sz)), far(h_matrix(sz)))


def solution(mesh):
    dims = tuple(mesh.shape[a] for a in ("gx", "gy", "gz"))
    in_specs = (P("gx", "gy", "gz"), P("gx", "gy", "gz"), P(None, "gx", "gy", "gz"), P())
    out_specs = (P(None, "gx", "gy", "gz"), P())
    return jax.shard_map(
        lambda *args: per_device(dims, *args), mesh=mesh, in_specs=in_specs, out_specs=out_specs, check_vma=False
    )
```

```python
import itertools

import jax
import jax.numpy as jnp
import numpy as np
from jax import lax
from jax.experimental import pallas as pl
from jax.experimental.pallas import tpu as pltpu
from jax.sharding import PartitionSpec as P

SPF = 8
SPC = 32
BEND = 0.01
FB = 0
MESH = pl.DeviceIdType.MESH
F32 = jnp.float32
BF16 = jnp.bfloat16


def beta(t):
    m = np.abs(t)
    r = 2.0 - m
    return np.where(m < 1.0, 2.0 / 3.0 - m * m + 0.5 * m**3, np.where(m < 2.0, r**3 / 6.0, 0.0))


def basis(voxels, points, spacing, first):
    v = np.arange(voxels)[:, None] + 0.5
    c = (np.arange(points)[None, :] + first) * spacing + 0.5 * spacing
    return beta((v - c) / spacing)


def halves(w):
    hi = np.asarray(w, np.float32).astype(jnp.bfloat16)
    lo = (np.asarray(w, np.float64) - hi.astype(np.float64)).astype(np.float32).astype(jnp.bfloat16)
    return hi, lo


W4 = beta((np.arange(4)[:, None] + 4.5 - 4.0 * np.arange(4)[None, :]) / 4.0) / 24.0
TWO = np.array([1.0, 4.0, 6.0, 4.0, 1.0]) / 8.0


def spread(c, step):
    out = np.zeros((len(c) - 1) * step + 1)
    out[::step] = c
    return out


C29 = np.convolve(np.convolve(TWO, spread(TWO, 2)), spread(TWO, 4))


def y_matrix(sy):
    rows = np.zeros((24, sy))
    rows[:12] = basis(sy, 12, SPF, -2).T * SPF**-1.5
    rows[16:22] = basis(sy, 6, SPC, -2).T * SPC**-1.5
    hi, lo = halves(rows)
    return np.concatenate([np.concatenate([hi, hi], 1), np.concatenate([lo, lo], 1)], 0)


def stacked(cols):
    hi, lo = halves(cols)
    half = np.concatenate([hi, lo], 1)
    return np.concatenate([half, half], 0)


def z_matrices(sz):
    fine = np.zeros((sz, 128))
    fine[:, FB : FB + 20] = basis(sz, 20, SPF, -2)
    out = [stacked(fine)]
    for a in range(3):
        cols = np.zeros((sz, 128))
        for piece in range(4):
            first = 32 * piece + 8 * a
            cols[:, first : first + 8] = basis(sz, 8, SPC, -2)
        out.append(stacked(cols))
    return np.stack(out)


def d_matrix(sz):
    d = np.zeros((sz, sz), np.float32)
    for shift, value in ((-2, 1.0), (-1, -8.0), (1, 8.0), (2, -1.0)):
        for v in range(sz):
            if 0 <= v + shift < sz:
                d[v + shift, v] = value
    return np.concatenate([d, d], 0).astype(jnp.bfloat16)


def h_matrix(sz):
    h = np.zeros((128, sz), np.float32)
    for lane in range(128):
        h[lane, (sz - 2, sz - 1, 0, 1)[lane % 4]] = 1.0
    return np.concatenate([h, h], 0).astype(jnp.bfloat16)


def split(x):
    hi = x.astype(BF16)
    return hi, (x - hi.astype(F32)).astype(BF16)


def lanes(shape):
    return lax.broadcasted_iota(jnp.int32, shape, len(shape) - 1)


def roll(x, shift, axis):
    return pltpu.roll(x, shift % x.shape[axis] if isinstance(shift, int) else shift, axis)


class Place:
    def __init__(self, dims):
        self.dims = dims
        self.pos = tuple(lax.axis_index(a) for a in ("gx", "gy", "gz"))
        self.has = [{-1: p > 0, 1: p < n - 1} for p, n in zip(self.pos, dims)]

    def exists(self, d):
        cond = None
        for i in range(3):
            if d[i]:
                one = self.has[i][d[i]]
                cond = one if cond is None else jnp.logical_and(cond, one)
        return cond

    def at(self, d):
        return tuple(self.pos[i] + d[i] for i in range(3))

    def ring(self, axis, o):
        t = lax.rem(self.pos[axis] + o, self.dims[axis])
        return tuple(t if i == axis else self.pos[i] for i in range(3)), t

    def seen(self, dx, dy):
        return self.exists((dx, dy, 0))

    def if_seen(self, dx, dy, fn):
        if dx or dy:
            pl.when(self.seen(dx, dy))(fn)
        else:
            fn()

    def beside(self, dx, dy, o):
        gx, gy, gz = self.pos
        return (gx + dx, gy + dy, lax.rem(gz + o, self.dims[2]))

    def start(self, make, k):
        d, copy = make(k)
        pl.when(self.exists(d))(lambda: copy.start())

    def sent(self, make, k):
        d, copy = make(k)
        pl.when(self.exists(d))(lambda: copy.wait_send())

    def arrived(self, make, k):
        d, copy = make(k)
        pl.when(self.exists([-v for v in d]))(lambda: copy.wait_recv())


def ring_order(n):
    return sorted(range(n), key=lambda o: -min(o, n - o))


SIDES = list(itertools.product((-1, 0, 1), repeat=2))


def layers(dims, w_hbm, f_hbm, ctl_h, dz_h, sp, diff, dzb, cz, e,
           ctl, dz_w, small_sem, wb, fb, hys, hyr, hzs, hzr, fw, img_sem, hs, hr):
    nx, ny, nz = dims
    here = Place(dims)
    pos = here.pos
    gx, gy, gz = pos
    has, exists, at, ring, seen, if_seen, beside = (
        here.has, here.exists, here.at, here.ring, here.seen, here.if_seen, here.beside)
    start, sent, arrived = here.start, here.sent, here.arrived
    sides = SIDES
    zero8 = jnp.zeros((8, 128), F32)
    lane64 = lanes((64, 128))

    bar = pltpu.get_barrier_semaphore()
    count = 0
    for axis in range(3):
        for side in (-1, 1):
            d = tuple(side if i == axis else 0 for i in range(3))
            pl.when(exists(d))(lambda d=d: pl.semaphore_signal(bar, inc=1, device_id=at(d), device_id_type=MESH))
            count = count + has[axis][side].astype(jnp.int32)

    chunks = 4
    planes = 16
    for c in range(chunks):
        part = pl.ds(c * planes, planes)
        pltpu.make_async_copy(w_hbm.at[part], wb.at[part], img_sem.at[0, c]).start()
        pltpu.make_async_copy(f_hbm.at[part], fb.at[part], img_sem.at[1, c]).start()
    small = [pltpu.make_async_copy(dz_h, dz_w, small_sem.at[0]), pltpu.make_async_copy(ctl_h, ctl, small_sem.at[1])]
    for copy in small:
        copy.start()

    for side, d in ((0, -1), (1, 1)):
        @pl.when(jnp.logical_not(has[0][d]))
        def _(side=side):
            sp[66 * side : 66 * side + 2, 8:72, :] = jnp.zeros((2, 64, 128), F32)

        @pl.when(jnp.logical_not(has[1][d]))
        def _(side=side):
            hyr[side] = jnp.zeros(hyr.shape[1:], F32)

        @pl.when(jnp.logical_not(has[2][d]))
        def _(side=side):
            hzr[side] = jnp.zeros(hzr.shape[1:], F32)

    hzs[...] = jnp.zeros(hzs.shape, F32)

    def halo(k):
        axis, side = k // 2, k % 2
        d = [0, 0, 0]
        d[axis] = 2 * side - 1
        if axis == 0:
            src = sp.at[pl.ds(2 if side == 0 else 64, 2), pl.ds(8, 64), :]
            dst = sp.at[pl.ds(66 if side == 0 else 0, 2), pl.ds(8, 64), :]
        elif axis == 1:
            src, dst = hys.at[side], hyr.at[1 - side]
        else:
            src, dst = hzs, hzr.at[1 - side]
        return d, pltpu.make_async_remote_copy(
            src_ref=src, dst_ref=dst, send_sem=hs.at[k], recv_sem=hr.at[k],
            device_id=at(d), device_id_type=MESH)

    def part_of(k, c):
        axis, side = k // 2, k % 2
        if axis == 0:
            return halo(k)
        d = [0, 0, 0]
        d[axis] = 2 * side - 1
        if axis == 1:
            part = pl.ds(c * planes, planes)
            src, dst = hys.at[side, part], hyr.at[1 - side, part]
        else:
            src, dst = hzs.at[c // 2], hzr.at[1 - side, c // 2]
        return d, pltpu.make_async_remote_copy(
            src_ref=src, dst_ref=dst, send_sem=hs.at[k], recv_sem=hr.at[k],
            device_id=at(d), device_id_type=MESH)

    def send(k, c):
        d, copy = part_of(k, c)
        pl.when(exists(d))(lambda: copy.start())


    def sum_chunk(c, _):
        base = c * planes
        part = pl.ds(base, planes)
        pltpu.make_async_copy(w_hbm.at[part], wb.at[part], img_sem.at[0, c]).wait()
        pltpu.make_async_copy(f_hbm.at[part], fb.at[part], img_sem.at[1, c]).wait()
        h = c // 2
        group = lane64 // 4 - 16 * (c % 2)
        packed = hzs[h]
        for j in range(planes):
            w = wb[base + j]
            f = fb[base + j]
            s = w + f
            diff[base + j] = w - f
            sp[base + j + 2, 8:72, :] = s
            hys[0, base + j] = s[0:2]
            hys[1, base + j] = s[62:64]
            turned = roll(s, 64 * (c % 2) + 4 * j + 2, 1)
            packed = jnp.where(group == j, turned, packed)
        hzs[h] = packed
        return 0

    for c in range(chunks):
        sum_chunk(c, 0)
        if c == 1:
            pl.semaphore_wait(bar, count)
            for k in (2, 3):
                send(k, 0)
            send(0, 0)
        if c > 0:
            for k in (2, 3):
                send(k, c)
        if c % 2:
            for k in (4, 5):
                send(k, c)
    send(1, 0)

    small[0].wait()

    def dz_chunk(c, _):
        base = pl.multiple_of(c * 16, 16)
        for half in range(2):
            parts = [jnp.concatenate(split(sp[base + 8 * half + j + 2, 8:72, :]), 1) for j in range(8)]
            out = jnp.dot(jnp.concatenate(parts, 0), dz_w[...], preferred_element_type=F32)
            for j in range(8):
                dzb[base + 8 * half + j] = out[64 * j : 64 * (j + 1)]
        return 0

    lax.fori_loop(0, 4, dz_chunk, 0, unroll=True)

    small[1].wait()

    row16 = lax.broadcasted_iota(jnp.int32, (16, 128), 0)
    lane16 = lanes((16, 128))
    row_g = row16 - 2 + gy * 8
    lane_g = lane16 - (FB + 2) + gz * 16
    in_grid = (row_g >= 0) & (row_g < ny * 8) & (lane_g >= 0) & (lane_g < nz * 16)

    def lap(centre, low, high):
        total = roll(centre, 1, 0) + roll(centre, -1, 0) + roll(centre, 1, 1) + roll(centre, -1, 1)
        if low is not None:
            total = total + low
        if high is not None:
            total = total + high
        return total - 6.0 * centre

    def fine_bend(a, _):
        for j in range(8):
            block = jnp.concatenate([ctl[a, j], jnp.zeros((8, 112), F32)], 1)
            block = jnp.concatenate([block, zero8], 0)
            fw[j + 2] = roll(roll(block, 2, 0), FB + 2, 1)
        zero16 = jnp.zeros((16, 128), F32)
        for j in (0, 1, 10, 11):
            fw[j] = zero16
        first = []
        for j in range(12):
            if j in (0, 11):
                first.append(None)
                continue
            low = fw[j - 1] if 0 < j else None
            high = fw[j + 1] if j < 11 else None
            value = lap(fw[j], low, high)
            p = gx * 8 + j - 2
            ok = in_grid & (p >= 0) & (p < nx * 8)
            first.append(jnp.where(ok, value, 0.0))
        for j in range(12):
            centre = first[j] if first[j] is not None else zero16
            low = first[j - 1] if j > 0 else None
            high = first[j + 1] if j < 11 else None
            e[a, j] = BEND * lap(centre, low, high)
        return 0

    lax.fori_loop(0, 3, fine_bend, 0)

    for k in range(6):
        arrived(halo, k)

    def place_y(x, _):
        sp[x + 2, 6:8, :] = hyr[0, x]
        sp[x + 2, 72:74, :] = hyr[1, x]
        return 0

    lax.fori_loop(0, 64, place_y, 0, unroll=8)

    m4 = lane64 % 4
    for h in range(2):
        u = jnp.where(m4 < 2, hzr[0, h], hzr[1, h])
        a_part = jnp.where(m4 < 2, -roll(u, -2, 1), roll(u, 2, 1))
        b_part = jnp.where(m4 == 1, 8.0 * roll(u, -1, 1), jnp.where(m4 == 2, -8.0 * roll(u, 1, 1), 0.0))
        cz[h] = a_part + b_part
    for k in range(6):
        sent(halo, k)


def gradient(dims, sp, diff, dzb, cz, e0, cctl_h, wy_h, wz_h, h_h, fine_out, coarse_out,
             cctl, wy, wz, h_w, small_sem, dz2, xs, zs, e, csend, crecv, xg, total_rows, mix,
             fxr, fys, fyr, fzs, fzr, cs, cr, gs, gr, fs, fr):
    nx, ny, nz = dims
    here = Place(dims)
    pos = here.pos
    gx, gy, gz = pos
    has, exists, at, ring, seen, if_seen, beside = (
        here.has, here.exists, here.at, here.ring, here.seen, here.if_seen, here.beside)
    start, sent, arrived = here.start, here.sent, here.arrived
    sides = SIDES
    zero8 = jnp.zeros((8, 128), F32)
    lane64 = lanes((64, 128))

    small = [pltpu.make_async_copy(src, dst, small_sem.at[i]) for i, (src, dst) in enumerate(
        ((h_h, h_w), (wy_h, wy), (wz_h, wz), (cctl_h, cctl)))]
    for copy in small:
        copy.start()

    bar = pltpu.get_barrier_semaphore()
    plane = sorted(((ox, oy) for ox in range(nx) for oy in range(ny) if ox or oy),
                   key=lambda o: -min(o[1], ny - o[1]) - 0.5 * min(o[0], nx - o[0]))

    def in_plane(ox, oy):
        return (lax.rem(gx + ox, nx), lax.rem(gy + oy, ny), gz)

    for dx, dy in sides:
        def greet(dx=dx, dy=dy):
            for o in ring_order(nz)[:-1]:
                pl.semaphore_signal(bar, inc=1, device_id=beside(dx, dy, o), device_id_type=MESH)
        if_seen(dx, dy, greet)
    for ox, oy in plane:
        pl.semaphore_signal(bar, inc=1, device_id=in_plane(ox, oy), device_id_type=MESH)
    wide = [1 + h[-1].astype(jnp.int32) + h[1].astype(jnp.int32) for h in has]
    greeted = wide[0] * wide[1] * (nz - 1) + nx * ny - 1

    for side, d in ((0, -1), (1, 1)):
        for axis, ref in enumerate((fxr, fyr, fzr)):
            @pl.when(jnp.logical_not(has[axis][d]))
            def _(side=side, ref=ref):
                ref[side] = jnp.zeros(ref.shape[1:], F32)
    for dx, dy in sides:
        if dx or dy:
            @pl.when(jnp.logical_not(seen(-dx, -dy)))
            def _(dx=dx, dy=dy):
                crecv[3 * (dx + 1) + dy + 1] = zero8

    def fine_copy(k):
        axis, side = k // 2, k % 2
        d = [0, 0, 0]
        d[axis] = 2 * side - 1
        if axis == 0:
            src, dst = e.at[:, pl.ds(10 * side, 2)], fxr.at[1 - side]
        elif axis == 1:
            src, dst = fys.at[side], fyr.at[1 - side]
        else:
            src, dst = fzs.at[side], fzr.at[1 - side]
        return d, pltpu.make_async_remote_copy(
            src_ref=src, dst_ref=dst, send_sem=fs.at[k], recv_sem=fr.at[k],
            device_id=at(d), device_id_type=MESH)

    small[0].wait()

    def z_fix(c, _):
        base = pl.multiple_of(c * 16, 16)
        layer = cz[c // 2]
        for half in range(2):
            group = lane64 // 4 - 16 * lax.rem(c, 2) - 8 * half
            parts = [jnp.concatenate(split(jnp.where(group == j, layer, 0.0)), 1) for j in range(8)]
            out = jnp.dot(jnp.concatenate(parts, 0), h_w[...], preferred_element_type=F32)
            for j in range(8):
                dz2[base + 8 * half + j] = dzb[base + 8 * half + j] + out[64 * j : 64 * (j + 1)]
        return 0

    lax.fori_loop(0, 4, z_fix, 0, unroll=True)

    groups = 16
    slabs = groups + 3

    def column(yt, _):
        r0 = pl.multiple_of(8 * yt, 8)

        def put(a, g, value):
            xs[pl.ds(r0, 8), pl.ds(pl.multiple_of((a * slabs + g) * 128, 128), 128)] = value

        def pair(gg, acc):
            acc = [list(row) for row in acc]
            x0 = 8 * gg
            c = [sp[x0 + i, pl.ds(r0 + 8, 8), :] for i in range(12)]
            for sub in range(2):
                for k in range(4):
                    i = 4 * sub + k
                    plane = x0 + i + 2
                    sx = (c[i] - c[i + 4]) + 8.0 * (c[i + 3] - c[i + 1])
                    ym2 = sp[plane, pl.ds(r0 + 6, 8), :]
                    ym1 = sp[plane, pl.ds(r0 + 7, 8), :]
                    yp1 = sp[plane, pl.ds(r0 + 9, 8), :]
                    yp2 = sp[plane, pl.ds(r0 + 10, 8), :]
                    sy = (ym2 - yp2) + 8.0 * (yp1 - ym1)
                    sz = dz2[x0 + i, pl.ds(r0, 8), :]
                    dv = diff[x0 + i, pl.ds(r0, 8), :]
                    for a, s in enumerate((sx, sy, sz)):
                        f = dv * s
                        for m in range(4):
                            acc[a][m] = acc[a][m] + float(W4[k, m]) * f
                for a in range(3):
                    put(a, 2 * gg + sub, acc[a][0])
                    acc[a] = [acc[a][1], acc[a][2], acc[a][3], jnp.zeros((8, 128), F32)]
            return tuple(tuple(row) for row in acc)

        acc = lax.fori_loop(0, groups // 2, pair, tuple(tuple(zero8 for _ in range(4)) for _ in range(3)))
        for a in range(3):
            for m in range(3):
                put(a, groups + m, acc[a][m])
        return 0

    lax.fori_loop(0, 8, column, 0)

    for copy in small[1:]:
        copy.wait()
    total = None
    for a in range(3):
        x = xs[:, a * slabs * 128 : (a + 1) * slabs * 128]
        hi, lo = split(x)
        y = jnp.dot(wy[...], jnp.concatenate([hi, lo], 0), preferred_element_type=F32)
        y = y[:24] + y[24:]
        pieces = [y[:, 128 * i : 128 * (i + 1)] for i in range(slabs)]
        hi, lo = split(jnp.concatenate([p[16:24] for p in pieces], 0))
        z = jnp.dot(jnp.concatenate([hi, lo], 1), wz[1 + a], preferred_element_type=F32)
        z = z[:, :128] + z[:, 128:]
        total = z if total is None else total + z
        hi, lo = split(jnp.concatenate([p[:16] for p in pieces], 0))
        z = jnp.dot(jnp.concatenate([hi, lo], 1), wz[0], preferred_element_type=F32)
        z = z[:, :128] + z[:, 128:]
        for i in range(slabs):
            zs[a, i] = z[16 * i : 16 * (i + 1)]

    lane8 = lanes((8, 128))
    taken = []
    for jj in range(6):
        v = None
        for i in range(slabs):
            tap = i - 8 * jj + 25
            if 0 <= tap < 29:
                term = float(C29[tap]) * total[8 * i : 8 * (i + 1)]
                v = term if v is None else v + term
        taken.append(v)
    for g in range(3):
        v = jnp.where(lane8 < 64, taken[2 * g], taken[2 * g + 1])
        csend[g] = jnp.where(lane8 // 32 % 2 == 0, v, roll(v, -1, 0))
    crecv[4, pl.ds(gz, 1), :] = csend[1, 2:3, :]

    def coarse_copy(dx, dy, o):
        slot = 3 * (dx + 1) + dy + 1
        return pltpu.make_async_remote_copy(
            src_ref=csend.at[dx + 1, pl.ds(2 * (dy + 1), 1), :], dst_ref=crecv.at[slot, pl.ds(gz, 1), :],
            send_sem=cs.at[slot], recv_sem=cr.at[slot], device_id=beside(dx, dy, o), device_id_type=MESH)

    def coarse_line(dx, dy):
        slot = 3 * (dx + 1) + dy + 1
        rows = crecv.at[slot] if dx or dy else crecv.at[slot, pl.ds(0, nz - 1), :]
        return pltpu.make_async_remote_copy(
            src_ref=rows, dst_ref=rows, send_sem=cs.at[slot], recv_sem=cr.at[slot],
            device_id=beside(0, 0, 1), device_id_type=MESH)

    def coarse_all(fn):
        for o in ring_order(nz):
            for dx, dy in sorted(sides, key=lambda d: -abs(d[0]) - abs(d[1])):
                if o or dx or dy:
                    fn(dx, dy, o)

    pl.semaphore_wait(bar, greeted)
    coarse_all(lambda dx, dy, o: if_seen(dx, dy, lambda: coarse_copy(dx, dy, o).start()))

    for a in range(3):
        for j in range(12):
            v = e0[a, j]
            for k in range(5):
                i = 2 * j - 4 + k
                if 0 <= i < slabs:
                    v = v + float(TWO[k]) * zs[a, i]
            e[a, j] = v
    for k in (0, 1):
        start(fine_copy, k)

    kx, ky, kz = cctl.shape[1:]
    shape = (ky, kz)
    crow = lax.broadcasted_iota(jnp.int32, (ky, 128), 0)
    clane = lanes((ky, 128))

    def clap(centre, low, high):
        total = jnp.where(crow > 0, roll(centre, 1, 0), 0.0) + jnp.where(crow < ky - 1, roll(centre, -1, 0), 0.0)
        total = total + roll(centre, 1, 1) + roll(centre, -1, 1)
        if low is not None:
            total = total + low
        if high is not None:
            total = total + high
        return jnp.where(clane < kz, total - 6.0 * centre, 0.0)

    def coarse_bend(a, _):
        field = [jnp.concatenate([cctl[a, j], jnp.zeros((ky, 128 - kz), F32)], 1) for j in range(kx)]
        for _level in range(2):
            field = [clap(field[j], field[j - 1] if j else None, field[j + 1] if j < kx - 1 else None)
                     for j in range(kx)]
        for j in range(kx):
            coarse_out[a, j] = BEND * field[j][:, :kz]
        return 0

    lax.fori_loop(0, 3, coarse_bend, 0)

    for k in (0, 1):
        sent(fine_copy, k)
        arrived(fine_copy, k)
    for a in range(3):
        for j in range(8):
            v = e[a, j + 2]
            if j < 2:
                v = v + fxr[0, a, j]
            if j >= 6:
                v = v + fxr[1, a, j - 6]
            e[a, j + 2] = v
            fys[0, 8 * a + j] = v[0:2]
            fys[1, 8 * a + j] = v[10:12]
    for k in (2, 3):
        start(fine_copy, k)

    for dx, dy in sides:
        if_seen(-dx, -dy, lambda: coarse_line(dx, dy).wait_recv())
    line = crecv[0]
    for i in range(1, 9):
        line = line + crecv[i]
    line = pltpu.roll(line, 0, 1, stride=4, stride_axis=0)
    place = lane8 % 32 + 2 - 4 * lax.broadcasted_iota(jnp.int32, (8, 128), 0)
    for a in range(3):
        piece = jnp.where((place >= 0) & (place < 8), roll(line, -2 - 8 * a, 1), 0.0)
        xg[gx, a, pl.ds(gy, 1), :] = jnp.sum(piece, axis=0, keepdims=True)

    def gather_copy(ox, oy, sx, sy):
        slot = xg.at[sx, :, pl.ds(sy, 1), :]
        return pltpu.make_async_remote_copy(
            src_ref=slot, dst_ref=slot, send_sem=gs, recv_sem=gr,
            device_id=in_plane(ox, oy), device_id_type=MESH)

    def gather_plane():
        return pltpu.make_async_remote_copy(
            src_ref=total_rows, dst_ref=total_rows, send_sem=gs, recv_sem=gr,
            device_id=in_plane(0, 1), device_id_type=MESH)

    for ox, oy in plane:
        gather_copy(ox, oy, gx, gy).start()

    for k in (2, 3):
        arrived(fine_copy, k)
    pack0 = zero8
    pack1 = zero8
    zero4 = jnp.zeros((4, 128), F32)
    for a in range(3):
        for j in range(8):
            s = 8 * a + j
            v = e[a, j + 2]
            edges = jnp.concatenate([fyr[0, s], zero4, fyr[1, s]], 0)
            v = roll(v, -2, 0)[0:8] + edges
            e[a, j + 2, 0:8, :] = v
            turned = roll(v, 2 * s - FB, 1)
            pack0 = jnp.where(lane8 // 2 == s, turned, pack0)
            pack1 = jnp.where(lane8 // 2 == s + 9, turned, pack1)
    fzs[0] = pack0
    fzs[1] = pack1
    for k in (4, 5):
        start(fine_copy, k)

    for k in (4, 5):
        arrived(fine_copy, k)
    p0 = fzr[0]
    p1 = fzr[1]
    for a in range(3):
        for j in range(8):
            s = 8 * a + j
            v = roll(e[a, j + 2, 0:8, :], -(FB + 2), 1)
            v = v + jnp.where(lane8 < 2, roll(p0, -(18 + 2 * s), 1), 0.0)
            v = v + jnp.where((lane8 >= 14) & (lane8 < 16), roll(p1, 14 - 2 * s, 1), 0.0)
            fine_out[a, j] = v[:, :16]

    gather_plane().wait_recv()
    for g in range(nx):
        for a in range(3):
            rows = xg[g, a]
            for p in range(2):
                for q in range(2):
                    mix[a, 2 * g + p, pl.ds(q, ny, stride=2), :] = roll(rows, -(64 * p + 32 * q), 1)
    for a in range(3):
        for j in range(kx):
            coarse_out[a, j] = coarse_out[a, j] + mix[a, j][:, :kz]

    for k in range(2, 6):
        sent(fine_copy, k)
    for dx, dy in sides:
        if_seen(dx, dy, lambda: coarse_line(dx, dy).wait_send())
    gather_plane().wait_send()


def per_device(dims, warped_image, fixed_image, fine_control, coarse_control):
    sx, sy, sz = warped_image.shape
    kx, ky, kz = coarse_control.shape[1:]
    nx, ny, nz = dims
    slabs = 19
    vmem = pl.BlockSpec(memory_space=pltpu.VMEM)
    hbm = pl.BlockSpec(memory_space=pltpu.HBM)
    v = lambda *shape: pltpu.VMEM(shape, F32)
    h = lambda *shape: pltpu.VMEM(shape, BF16)
    out = lambda *shape: jax.ShapeDtypeStruct(shape, F32)
    dma = pltpu.SemaphoreType.DMA
    far = lambda x: pltpu.with_memory_space_constraint(jnp.asarray(x), pltpu.HBM)
    local = pl.pallas_call(
        lambda *refs: layers(dims, *refs),
        out_shape=(out(sx + 4, sy + 16, sz), out(sx, sy, sz), out(sx, sy, sz), out(2, sy, 128), out(3, 12, 16, 128)),
        in_specs=[hbm] * 4,
        out_specs=(vmem,) * 5,
        scratch_shapes=[
            v(*fine_control.shape), h(2 * sz, sz), dma((2,)), v(sx, sy, sz), v(sx, sy, sz),
            v(2, sx, 2, sz), v(2, sx, 2, sz), v(2, sy, 128), v(2, 2, sy, 128), v(12, 16, 128),
            dma((2, 4)), dma((6,)), dma((6,)),
        ],
        compiler_params=pltpu.CompilerParams(collective_id=0, has_side_effects=True, vmem_limit_bytes=24 << 20),
        name="layers",
    )(far(warped_image), far(fixed_image), far(fine_control), far(d_matrix(sz)))
    return pl.pallas_call(
        lambda *refs: gradient(dims, *refs),
        out_shape=(out(*fine_control.shape), out(*coarse_control.shape)),
        in_specs=[vmem] * 5 + [hbm] * 4,
        out_specs=(vmem, vmem),
        scratch_shapes=[
            v(*coarse_control.shape), h(48, 2 * sy), h(4, 2 * sz, 256), h(256, sz), dma((4,)),
            v(sx, sy, sz), v(sy, 3 * slabs * 128), v(3, slabs, 16, 128), v(3, 12, 16, 128),
            v(3, 8, 128), v(9, nz, 128), v(nx, 3, ny, 128), v(3 * (nx * ny - 1), 128), v(3, kx, ky, 128),
            v(2, 3, 2, 16, 128), v(2, 24, 2, 128), v(2, 24, 2, 128), v(2, 8, 128), v(2, 8, 128),
            dma((9,)), dma((9,)), dma, dma, dma((6,)), dma((6,)),
        ],
        compiler_params=pltpu.CompilerParams(collective_id=1, has_side_effects=True, vmem_limit_bytes=24 << 20),
        name="gradient",
    )(*local, far(coarse_control), far(y_matrix(sy)), far(z_matrices(sz)), far(h_matrix(sz)))


def solution(mesh):
    dims = tuple(mesh.shape[a] for a in ("gx", "gy", "gz"))
    in_specs = (P("gx", "gy", "gz"), P("gx", "gy", "gz"), P(None, "gx", "gy", "gz"), P())
    out_specs = (P(None, "gx", "gy", "gz"), P())
    return jax.shard_map(
        lambda *args: per_device(dims, *args), mesh=mesh, in_specs=in_specs, out_specs=out_specs, check_vma=False
    )
```

```python
import itertools

import jax
import jax.numpy as jnp
import numpy as np
from jax import lax
from jax.experimental import pallas as pl
from jax.experimental.pallas import tpu as pltpu
from jax.sharding import PartitionSpec as P

SPF = 8
SPC = 32
BEND = 0.01
FB = 0
MESH = pl.DeviceIdType.MESH
F32 = jnp.float32
BF16 = jnp.bfloat16


def beta(t):
    m = np.abs(t)
    r = 2.0 - m
    return np.where(m < 1.0, 2.0 / 3.0 - m * m + 0.5 * m**3, np.where(m < 2.0, r**3 / 6.0, 0.0))


def basis(voxels, points, spacing, first):
    v = np.arange(voxels)[:, None] + 0.5
    c = (np.arange(points)[None, :] + first) * spacing + 0.5 * spacing
    return beta((v - c) / spacing)


def halves(w):
    hi = np.asarray(w, np.float32).astype(jnp.bfloat16)
    lo = (np.asarray(w, np.float64) - hi.astype(np.float64)).astype(np.float32).astype(jnp.bfloat16)
    return hi, lo


W4 = beta((np.arange(4)[:, None] + 4.5 - 4.0 * np.arange(4)[None, :]) / 4.0) / 24.0
TWO = np.array([1.0, 4.0, 6.0, 4.0, 1.0]) / 8.0


def spread(c, step):
    out = np.zeros((len(c) - 1) * step + 1)
    out[::step] = c
    return out


C29 = np.convolve(np.convolve(TWO, spread(TWO, 2)), spread(TWO, 4))


def y_matrix(sy):
    rows = np.zeros((24, sy))
    rows[:12] = basis(sy, 12, SPF, -2).T * SPF**-1.5
    rows[16:22] = basis(sy, 6, SPC, -2).T * SPC**-1.5
    hi, lo = halves(rows)
    return np.concatenate([np.concatenate([hi, hi], 1), np.concatenate([lo, lo], 1)], 0)


def stacked(cols):
    hi, lo = halves(cols)
    half = np.concatenate([hi, lo], 1)
    return np.concatenate([half, half], 0)


def z_matrices(sz):
    fine = np.zeros((sz, 128))
    fine[:, FB : FB + 20] = basis(sz, 20, SPF, -2)
    out = [stacked(fine)]
    for a in range(3):
        cols = np.zeros((sz, 128))
        for piece in range(4):
            first = 32 * piece + 8 * a
            cols[:, first : first + 8] = basis(sz, 8, SPC, -2)
        out.append(stacked(cols))
    return np.stack(out)


def d_matrix(sz):
    d = np.zeros((sz, sz), np.float32)
    for shift, value in ((-2, 1.0), (-1, -8.0), (1, 8.0), (2, -1.0)):
        for v in range(sz):
            if 0 <= v + shift < sz:
                d[v + shift, v] = value
    return np.concatenate([d, d], 0).astype(jnp.bfloat16)


def h_matrix(sz):
    h = np.zeros((128, sz), np.float32)
    for lane in range(128):
        h[lane, (sz - 2, sz - 1, 0, 1)[lane % 4]] = 1.0
    return np.concatenate([h, h], 0).astype(jnp.bfloat16)


def split(x):
    hi = x.astype(BF16)
    return hi, (x - hi.astype(F32)).astype(BF16)


def lanes(shape):
    return lax.broadcasted_iota(jnp.int32, shape, len(shape) - 1)


def roll(x, shift, axis):
    return pltpu.roll(x, shift % x.shape[axis] if isinstance(shift, int) else shift, axis)


class Place:
    def __init__(self, dims):
        self.dims = dims
        self.pos = tuple(lax.axis_index(a) for a in ("gx", "gy", "gz"))
        self.has = [{-1: p > 0, 1: p < n - 1} for p, n in zip(self.pos, dims)]

    def exists(self, d):
        cond = None
        for i in range(3):
            if d[i]:
                one = self.has[i][d[i]]
                cond = one if cond is None else jnp.logical_and(cond, one)
        return cond

    def at(self, d):
        return tuple(self.pos[i] + d[i] for i in range(3))

    def ring(self, axis, o):
        t = lax.rem(self.pos[axis] + o, self.dims[axis])
        return tuple(t if i == axis else self.pos[i] for i in range(3)), t

    def seen(self, dx, dy):
        return self.exists((dx, dy, 0))

    def if_seen(self, dx, dy, fn):
        if dx or dy:
            pl.when(self.seen(dx, dy))(fn)
        else:
            fn()

    def beside(self, dx, dy, o):
        gx, gy, gz = self.pos
        return (gx + dx, gy + dy, lax.rem(gz + o, self.dims[2]))

    def start(self, make, k):
        d, copy = make(k)
        pl.when(self.exists(d))(lambda: copy.start())

    def sent(self, make, k):
        d, copy = make(k)
        pl.when(self.exists(d))(lambda: copy.wait_send())

    def arrived(self, make, k):
        d, copy = make(k)
        pl.when(self.exists([-v for v in d]))(lambda: copy.wait_recv())


def ring_order(n):
    return sorted(range(n), key=lambda o: -min(o, n - o))


SIDES = list(itertools.product((-1, 0, 1), repeat=2))


def gradient(dims, w_hbm, f_hbm, ctl_h, cctl_h, dz_h, h_h, wy_h, wz_h, fine_out, coarse_out,
             ctl, cctl, dz_w, h_w, wy, wz, small_sem, wb, fb, sp, diff, dzb, cz, e,
             hys, hyr, hzs, hzr, fw, xs, zs, csend, crecv, xg, total_rows, mix,
             fxr, fys, fyr, fzs, fzr, img_sem, hs, hr, cs, cr, gs, gr, fs, fr, near_sem, far_sem):
    nx, ny, nz = dims
    here = Place(dims)
    pos = here.pos
    gx, gy, gz = pos
    has, exists, at, ring, seen, if_seen, beside = (
        here.has, here.exists, here.at, here.ring, here.seen, here.if_seen, here.beside)
    start, sent, arrived = here.start, here.sent, here.arrived
    sides = SIDES
    zero8 = jnp.zeros((8, 128), F32)
    lane64 = lanes((64, 128))

    bar = pltpu.get_barrier_semaphore()
    odd = lax.rem(gx + gy + gz, 2) == 1
    even = jnp.logical_not(odd)
    faces = [tuple(side if i == axis else 0 for i in range(3)) for axis in range(3) for side in (-1, 1)]
    count = sum(has[axis][side].astype(jnp.int32) for axis in range(3) for side in (-1, 1))

    def greet_faces(sem):
        for d in faces:
            pl.when(exists(d))(lambda: pl.semaphore_signal(sem, inc=1, device_id=at(d), device_id_type=MESH))

    @pl.when(even)
    def _():
        greet_faces(bar)

    def near_done():
        @pl.when(odd)
        def _():
            pl.semaphore_wait(bar, count)
            greet_faces(near_sem)

        @pl.when(even)
        def _():
            pl.semaphore_wait(near_sem, count)

    chip = gx // 2
    lean = 2 * lax.rem(gx, 2) - 1
    next_chip = chip + lean
    has_next = (next_chip >= 0) & (next_chip < nx // 2)
    partner = (gx - lean, gy, gz)

    def greet_chip(c, y, z):
        device = (2 * c + lax.rem(y + z, 2), y, z)
        pl.semaphore_signal(bar, inc=1, device_id=device, device_id_type=MESH)

    def far_greetings():
        for dy in (-1, 1, 0):
            def line(dy=dy):
                for o in ring_order(nz)[:-1]:
                    greet_chip(chip, gy + dy, lax.rem(gz + o, nz))

                @pl.when(has_next)
                def _():
                    for o in ring_order(nz)[:-1]:
                        greet_chip(next_chip, gy + dy, lax.rem(gz + o, nz))
            if_seen(0, dy, line)
        for oc in range(nx // 2):
            for oy in ring_order(ny):
                def one(oc=oc, oy=oy):
                    greet_chip(lax.rem(chip + oc, nx // 2), lax.rem(gy + oy, ny), gz)
                if oc or oy:
                    one()
                else:
                    pl.when(odd)(one)

    def far_done():
        wide_x = 4 - (chip == 0).astype(jnp.int32) - (chip == nx // 2 - 1).astype(jnp.int32)
        wide_y = 1 + has[1][-1].astype(jnp.int32) + has[1][1].astype(jnp.int32)

        @pl.when(even)
        def _():
            pl.semaphore_wait(bar, wide_x * wide_y * (nz - 1) + nx * ny - 1)
            pl.semaphore_signal(far_sem, inc=1, device_id=partner, device_id_type=MESH)

        @pl.when(odd)
        def _():
            pl.semaphore_wait(far_sem, 1)

    chunks = 4
    planes = 16
    for c in range(chunks):
        part = pl.ds(c * planes, planes)
        pltpu.make_async_copy(w_hbm.at[part], wb.at[part], img_sem.at[0, c]).start()
        pltpu.make_async_copy(f_hbm.at[part], fb.at[part], img_sem.at[1, c]).start()
    small = [pltpu.make_async_copy(src, dst, small_sem.at[i]) for i, (src, dst) in enumerate(
        ((dz_h, dz_w), (ctl_h, ctl), (h_h, h_w), (wy_h, wy), (wz_h, wz), (cctl_h, cctl)))]
    for copy in small:
        copy.start()
    far_greetings()

    for side, d in ((0, -1), (1, 1)):
        @pl.when(jnp.logical_not(has[0][d]))
        def _(side=side):
            sp[66 * side : 66 * side + 2, 8:72, :] = jnp.zeros((2, 64, 128), F32)

        @pl.when(jnp.logical_not(has[1][d]))
        def _(side=side):
            hyr[side] = jnp.zeros(hyr.shape[1:], F32)

        @pl.when(jnp.logical_not(has[2][d]))
        def _(side=side):
            hzr[side] = jnp.zeros(hzr.shape[1:], F32)

    hzs[...] = jnp.zeros(hzs.shape, F32)

    def halo(k):
        axis, side = k // 2, k % 2
        d = [0, 0, 0]
        d[axis] = 2 * side - 1
        if axis == 0:
            src = sp.at[pl.ds(2 if side == 0 else 64, 2), pl.ds(8, 64), :]
            dst = sp.at[pl.ds(66 if side == 0 else 0, 2), pl.ds(8, 64), :]
        elif axis == 1:
            src, dst = hys.at[side], hyr.at[1 - side]
        else:
            src, dst = hzs, hzr.at[1 - side]
        return d, pltpu.make_async_remote_copy(
            src_ref=src, dst_ref=dst, send_sem=hs.at[k], recv_sem=hr.at[k],
            device_id=at(d), device_id_type=MESH)

    def part_of(k, c):
        axis, side = k // 2, k % 2
        if axis == 0:
            return halo(k)
        d = [0, 0, 0]
        d[axis] = 2 * side - 1
        if axis == 1:
            part = pl.ds(c * planes, planes)
            src, dst = hys.at[side, part], hyr.at[1 - side, part]
        else:
            src, dst = hzs.at[c // 2], hzr.at[1 - side, c // 2]
        return d, pltpu.make_async_remote_copy(
            src_ref=src, dst_ref=dst, send_sem=hs.at[k], recv_sem=hr.at[k],
            device_id=at(d), device_id_type=MESH)

    def send(k, c):
        d, copy = part_of(k, c)
        pl.when(exists(d))(lambda: copy.start())


    def sum_chunk(c, _):
        base = c * planes
        part = pl.ds(base, planes)
        pltpu.make_async_copy(w_hbm.at[part], wb.at[part], img_sem.at[0, c]).wait()
        pltpu.make_async_copy(f_hbm.at[part], fb.at[part], img_sem.at[1, c]).wait()
        h = c // 2
        group = lane64 // 4 - 16 * (c % 2)
        packed = hzs[h]
        for j in range(planes):
            w = wb[base + j]
            f = fb[base + j]
            s = w + f
            diff[base + j] = w - f
            sp[base + j + 2, 8:72, :] = s
            hys[0, base + j] = s[0:2]
            hys[1, base + j] = s[62:64]
            turned = roll(s, 64 * (c % 2) + 4 * j + 2, 1)
            packed = jnp.where(group == j, turned, packed)
        hzs[h] = packed
        return 0

    for c in range(chunks):
        sum_chunk(c, 0)
        if c == 1:
            near_done()
            for k in (2, 3):
                send(k, 0)
            send(0, 0)
        if c > 0:
            for k in (2, 3):
                send(k, c)
        if c % 2:
            for k in (4, 5):
                send(k, c)
    send(1, 0)

    small[0].wait()

    def dz_chunk(c, _):
        base = pl.multiple_of(c * 16, 16)
        for half in range(2):
            parts = [jnp.concatenate(split(sp[base + 8 * half + j + 2, 8:72, :]), 1) for j in range(8)]
            out = jnp.dot(jnp.concatenate(parts, 0), dz_w[...], preferred_element_type=F32)
            for j in range(8):
                dzb[base + 8 * half + j] = out[64 * j : 64 * (j + 1)]
        return 0

    lax.fori_loop(0, 4, dz_chunk, 0, unroll=True)

    for side, d in ((0, -1), (1, 1)):
        for axis, ref in enumerate((fxr, fyr, fzr)):
            @pl.when(jnp.logical_not(has[axis][d]))
            def _(side=side, ref=ref):
                ref[side] = jnp.zeros(ref.shape[1:], F32)
    for dx, dy in sides:
        if dx or dy:
            @pl.when(jnp.logical_not(seen(-dx, -dy)))
            def _(dx=dx, dy=dy):
                crecv[3 * (dx + 1) + dy + 1] = zero8

    small[1].wait()

    row16 = lax.broadcasted_iota(jnp.int32, (16, 128), 0)
    lane16 = lanes((16, 128))
    row_g = row16 - 2 + gy * 8
    lane_g = lane16 - (FB + 2) + gz * 16
    in_grid = (row_g >= 0) & (row_g < ny * 8) & (lane_g >= 0) & (lane_g < nz * 16)

    def lap(centre, low, high):
        total = roll(centre, 1, 0) + roll(centre, -1, 0) + roll(centre, 1, 1) + roll(centre, -1, 1)
        if low is not None:
            total = total + low
        if high is not None:
            total = total + high
        return total - 6.0 * centre

    def fine_bend(a, _):
        for j in range(8):
            block = jnp.concatenate([ctl[a, j], jnp.zeros((8, 112), F32)], 1)
            block = jnp.concatenate([block, zero8], 0)
            fw[j + 2] = roll(roll(block, 2, 0), FB + 2, 1)
        zero16 = jnp.zeros((16, 128), F32)
        for j in (0, 1, 10, 11):
            fw[j] = zero16
        first = []
        for j in range(12):
            if j in (0, 11):
                first.append(None)
                continue
            low = fw[j - 1] if 0 < j else None
            high = fw[j + 1] if j < 11 else None
            value = lap(fw[j], low, high)
            p = gx * 8 + j - 2
            ok = in_grid & (p >= 0) & (p < nx * 8)
            first.append(jnp.where(ok, value, 0.0))
        for j in range(12):
            centre = first[j] if first[j] is not None else zero16
            low = first[j - 1] if j > 0 else None
            high = first[j + 1] if j < 11 else None
            e[a, j] = BEND * lap(centre, low, high)
        return 0

    lax.fori_loop(0, 3, fine_bend, 0)

    for k in range(6):
        arrived(halo, k)

    def place_y(x, _):
        sp[x + 2, 6:8, :] = hyr[0, x]
        sp[x + 2, 72:74, :] = hyr[1, x]
        return 0

    lax.fori_loop(0, 64, place_y, 0, unroll=8)

    m4 = lane64 % 4
    for h in range(2):
        u = jnp.where(m4 < 2, hzr[0, h], hzr[1, h])
        a_part = jnp.where(m4 < 2, -roll(u, -2, 1), roll(u, 2, 1))
        b_part = jnp.where(m4 == 1, 8.0 * roll(u, -1, 1), jnp.where(m4 == 2, -8.0 * roll(u, 1, 1), 0.0))
        cz[h] = a_part + b_part
    plane = sorted(((ox, oy) for ox in range(nx) for oy in range(ny) if ox or oy),
                   key=lambda o: -min(o[1], ny - o[1]) - 0.5 * min(o[0], nx - o[0]))

    def in_plane(ox, oy):
        return (lax.rem(gx + ox, nx), lax.rem(gy + oy, ny), gz)

    def fine_copy(k):
        axis, side = k // 2, k % 2
        d = [0, 0, 0]
        d[axis] = 2 * side - 1
        if axis == 0:
            src, dst = e.at[:, pl.ds(10 * side, 2)], fxr.at[1 - side]
        elif axis == 1:
            src, dst = fys.at[side], fyr.at[1 - side]
        else:
            src, dst = fzs.at[side], fzr.at[1 - side]
        return d, pltpu.make_async_remote_copy(
            src_ref=src, dst_ref=dst, send_sem=fs.at[k], recv_sem=fr.at[k],
            device_id=at(d), device_id_type=MESH)

    small[2].wait()

    def z_fix(c, _):
        base = pl.multiple_of(c * 16, 16)
        layer = cz[c // 2]
        for half in range(2):
            group = lane64 // 4 - 16 * lax.rem(c, 2) - 8 * half
            parts = [jnp.concatenate(split(jnp.where(group == j, layer, 0.0)), 1) for j in range(8)]
            out = jnp.dot(jnp.concatenate(parts, 0), h_w[...], preferred_element_type=F32)
            for j in range(8):
                dzb[base + 8 * half + j] = dzb[base + 8 * half + j] + out[64 * j : 64 * (j + 1)]
        return 0

    lax.fori_loop(0, 4, z_fix, 0, unroll=True)

    groups = 16
    slabs = groups + 3

    def column(yt, _):
        r0 = pl.multiple_of(8 * yt, 8)

        def put(a, g, value):
            xs[pl.ds(r0, 8), pl.ds(pl.multiple_of((a * slabs + g) * 128, 128), 128)] = value

        def pair(gg, acc):
            acc = [list(row) for row in acc]
            x0 = 8 * gg
            c = [sp[x0 + i, pl.ds(r0 + 8, 8), :] for i in range(12)]
            for sub in range(2):
                for k in range(4):
                    i = 4 * sub + k
                    plane = x0 + i + 2
                    sx = (c[i] - c[i + 4]) + 8.0 * (c[i + 3] - c[i + 1])
                    ym2 = sp[plane, pl.ds(r0 + 6, 8), :]
                    ym1 = sp[plane, pl.ds(r0 + 7, 8), :]
                    yp1 = sp[plane, pl.ds(r0 + 9, 8), :]
                    yp2 = sp[plane, pl.ds(r0 + 10, 8), :]
                    sy = (ym2 - yp2) + 8.0 * (yp1 - ym1)
                    sz = dzb[x0 + i, pl.ds(r0, 8), :]
                    dv = diff[x0 + i, pl.ds(r0, 8), :]
                    for a, s in enumerate((sx, sy, sz)):
                        f = dv * s
                        for m in range(4):
                            acc[a][m] = acc[a][m] + float(W4[k, m]) * f
                for a in range(3):
                    put(a, 2 * gg + sub, acc[a][0])
                    acc[a] = [acc[a][1], acc[a][2], acc[a][3], jnp.zeros((8, 128), F32)]
            return tuple(tuple(row) for row in acc)

        acc = lax.fori_loop(0, groups // 2, pair, tuple(tuple(zero8 for _ in range(4)) for _ in range(3)))
        for a in range(3):
            for m in range(3):
                put(a, groups + m, acc[a][m])
        return 0

    lax.fori_loop(0, 8, column, 0)

    for copy in small[3:]:
        copy.wait()
    total = None
    for a in range(3):
        x = xs[:, a * slabs * 128 : (a + 1) * slabs * 128]
        hi, lo = split(x)
        y = jnp.dot(wy[...], jnp.concatenate([hi, lo], 0), preferred_element_type=F32)
        y = y[:24] + y[24:]
        pieces = [y[:, 128 * i : 128 * (i + 1)] for i in range(slabs)]
        hi, lo = split(jnp.concatenate([p[16:24] for p in pieces], 0))
        z = jnp.dot(jnp.concatenate([hi, lo], 1), wz[1 + a], preferred_element_type=F32)
        z = z[:, :128] + z[:, 128:]
        total = z if total is None else total + z
        hi, lo = split(jnp.concatenate([p[:16] for p in pieces], 0))
        z = jnp.dot(jnp.concatenate([hi, lo], 1), wz[0], preferred_element_type=F32)
        z = z[:, :128] + z[:, 128:]
        for i in range(slabs):
            zs[a, i] = z[16 * i : 16 * (i + 1)]

    lane8 = lanes((8, 128))
    taken = []
    for jj in range(6):
        v = None
        for i in range(slabs):
            tap = i - 8 * jj + 25
            if 0 <= tap < 29:
                term = float(C29[tap]) * total[8 * i : 8 * (i + 1)]
                v = term if v is None else v + term
        taken.append(v)
    for g in range(3):
        v = jnp.where(lane8 < 64, taken[2 * g], taken[2 * g + 1])
        csend[g] = jnp.where(lane8 // 32 % 2 == 0, v, roll(v, -1, 0))
    crecv[4, pl.ds(gz, 1), :] = csend[1, 2:3, :]

    def coarse_copy(dx, dy, o):
        slot = 3 * (dx + 1) + dy + 1
        return pltpu.make_async_remote_copy(
            src_ref=csend.at[dx + 1, pl.ds(2 * (dy + 1), 1), :], dst_ref=crecv.at[slot, pl.ds(gz, 1), :],
            send_sem=cs.at[slot], recv_sem=cr.at[slot], device_id=beside(dx, dy, o), device_id_type=MESH)

    def coarse_line(dx, dy):
        slot = 3 * (dx + 1) + dy + 1
        rows = crecv.at[slot] if dx or dy else crecv.at[slot, pl.ds(0, nz - 1), :]
        return pltpu.make_async_remote_copy(
            src_ref=rows, dst_ref=rows, send_sem=cs.at[slot], recv_sem=cr.at[slot],
            device_id=beside(0, 0, 1), device_id_type=MESH)

    def coarse_all(fn):
        for o in ring_order(nz):
            for dx, dy in sorted(sides, key=lambda d: -abs(d[0]) - abs(d[1])):
                if o or dx or dy:
                    fn(dx, dy, o)

    far_done()
    coarse_all(lambda dx, dy, o: if_seen(dx, dy, lambda: coarse_copy(dx, dy, o).start()))

    for a in range(3):
        for j in range(12):
            v = e[a, j]
            for k in range(5):
                i = 2 * j - 4 + k
                if 0 <= i < slabs:
                    v = v + float(TWO[k]) * zs[a, i]
            e[a, j] = v
    for k in (0, 1):
        start(fine_copy, k)

    kx, ky, kz = cctl.shape[1:]
    shape = (ky, kz)
    crow = lax.broadcasted_iota(jnp.int32, (ky, 128), 0)
    clane = lanes((ky, 128))

    def clap(centre, low, high):
        total = jnp.where(crow > 0, roll(centre, 1, 0), 0.0) + jnp.where(crow < ky - 1, roll(centre, -1, 0), 0.0)
        total = total + roll(centre, 1, 1) + roll(centre, -1, 1)
        if low is not None:
            total = total + low
        if high is not None:
            total = total + high
        return jnp.where(clane < kz, total - 6.0 * centre, 0.0)

    def coarse_bend(a, _):
        field = [jnp.concatenate([cctl[a, j], jnp.zeros((ky, 128 - kz), F32)], 1) for j in range(kx)]
        for _level in range(2):
            field = [clap(field[j], field[j - 1] if j else None, field[j + 1] if j < kx - 1 else None)
                     for j in range(kx)]
        for j in range(kx):
            coarse_out[a, j] = BEND * field[j][:, :kz]
        return 0

    lax.fori_loop(0, 3, coarse_bend, 0)

    for k in (0, 1):
        sent(fine_copy, k)
        arrived(fine_copy, k)
    for a in range(3):
        for j in range(8):
            v = e[a, j + 2]
            if j < 2:
                v = v + fxr[0, a, j]
            if j >= 6:
                v = v + fxr[1, a, j - 6]
            e[a, j + 2] = v
            fys[0, 8 * a + j] = v[0:2]
            fys[1, 8 * a + j] = v[10:12]
    for k in (2, 3):
        start(fine_copy, k)

    for dx, dy in sides:
        if_seen(-dx, -dy, lambda: coarse_line(dx, dy).wait_recv())
    line = crecv[0]
    for i in range(1, 9):
        line = line + crecv[i]
    line = pltpu.roll(line, 0, 1, stride=4, stride_axis=0)
    place = lane8 % 32 + 2 - 4 * lax.broadcasted_iota(jnp.int32, (8, 128), 0)
    for a in range(3):
        piece = jnp.where((place >= 0) & (place < 8), roll(line, -2 - 8 * a, 1), 0.0)
        xg[gx, a, pl.ds(gy, 1), :] = jnp.sum(piece, axis=0, keepdims=True)

    def gather_copy(ox, oy, sx, sy):
        slot = xg.at[sx, :, pl.ds(sy, 1), :]
        return pltpu.make_async_remote_copy(
            src_ref=slot, dst_ref=slot, send_sem=gs, recv_sem=gr,
            device_id=in_plane(ox, oy), device_id_type=MESH)

    def gather_plane():
        return pltpu.make_async_remote_copy(
            src_ref=total_rows, dst_ref=total_rows, send_sem=gs, recv_sem=gr,
            device_id=in_plane(0, 1), device_id_type=MESH)

    for ox, oy in plane:
        gather_copy(ox, oy, gx, gy).start()

    for k in (2, 3):
        arrived(fine_copy, k)
    pack0 = zero8
    pack1 = zero8
    zero4 = jnp.zeros((4, 128), F32)
    for a in range(3):
        for j in range(8):
            s = 8 * a + j
            v = e[a, j + 2]
            edges = jnp.concatenate([fyr[0, s], zero4, fyr[1, s]], 0)
            v = roll(v, -2, 0)[0:8] + edges
            e[a, j + 2, 0:8, :] = v
            turned = roll(v, 2 * s - FB, 1)
            pack0 = jnp.where(lane8 // 2 == s, turned, pack0)
            pack1 = jnp.where(lane8 // 2 == s + 9, turned, pack1)
    fzs[0] = pack0
    fzs[1] = pack1
    for k in (4, 5):
        start(fine_copy, k)

    for k in (4, 5):
        arrived(fine_copy, k)
    p0 = fzr[0]
    p1 = fzr[1]
    for a in range(3):
        for j in range(8):
            s = 8 * a + j
            v = roll(e[a, j + 2, 0:8, :], -(FB + 2), 1)
            v = v + jnp.where(lane8 < 2, roll(p0, -(18 + 2 * s), 1), 0.0)
            v = v + jnp.where((lane8 >= 14) & (lane8 < 16), roll(p1, 14 - 2 * s, 1), 0.0)
            fine_out[a, j] = v[:, :16]

    gather_plane().wait_recv()
    for g in range(nx):
        for a in range(3):
            rows = xg[g, a]
            for p in range(2):
                for q in range(2):
                    mix[a, 2 * g + p, pl.ds(q, ny, stride=2), :] = roll(rows, -(64 * p + 32 * q), 1)
    for a in range(3):
        for j in range(kx):
            coarse_out[a, j] = coarse_out[a, j] + mix[a, j][:, :kz]

    for k in range(6):
        sent(halo, k)
    for k in range(2, 6):
        sent(fine_copy, k)
    for dx, dy in sides:
        if_seen(dx, dy, lambda: coarse_line(dx, dy).wait_send())
    gather_plane().wait_send()


def per_device(dims, warped_image, fixed_image, fine_control, coarse_control):
    sx, sy, sz = warped_image.shape
    kx, ky, kz = coarse_control.shape[1:]
    nx, ny, nz = dims
    slabs = 19
    vmem = pl.BlockSpec(memory_space=pltpu.VMEM)
    hbm = pl.BlockSpec(memory_space=pltpu.HBM)
    v = lambda *shape: pltpu.VMEM(shape, F32)
    h = lambda *shape: pltpu.VMEM(shape, BF16)
    out = lambda *shape: jax.ShapeDtypeStruct(shape, F32)
    dma = pltpu.SemaphoreType.DMA
    flag = pltpu.SemaphoreType.REGULAR
    far = lambda x: pltpu.with_memory_space_constraint(jnp.asarray(x), pltpu.HBM)
    return pl.pallas_call(
        lambda *refs: gradient(dims, *refs),
        out_shape=(out(*fine_control.shape), out(*coarse_control.shape)),
        in_specs=[hbm] * 8,
        out_specs=(vmem, vmem),
        scratch_shapes=[
            v(*fine_control.shape), v(*coarse_control.shape), h(2 * sz, sz), h(256, sz), h(48, 2 * sy),
            h(4, 2 * sz, 256), dma((6,)), v(sx, sy, sz), v(sx, sy, sz), v(sx + 4, sy + 16, sz), v(sx, sy, sz),
            v(sx, sy, sz), v(2, sy, 128), v(3, 12, 16, 128),
            v(2, sx, 2, sz), v(2, sx, 2, sz), v(2, sy, 128), v(2, 2, sy, 128), v(12, 16, 128),
            v(sy, 3 * slabs * 128), v(3, slabs, 16, 128), v(3, 8, 128), v(9, nz, 128),
            v(nx, 3, ny, 128), v(3 * (nx * ny - 1), 128), v(3, kx, ky, 128),
            v(2, 3, 2, 16, 128), v(2, 24, 2, 128), v(2, 24, 2, 128), v(2, 8, 128), v(2, 8, 128),
            dma((2, 4)), dma((6,)), dma((6,)), dma((9,)), dma((9,)), dma, dma, dma((6,)), dma((6,)), flag, flag,
        ],
        compiler_params=pltpu.CompilerParams(collective_id=0, has_side_effects=True, vmem_limit_bytes=48 << 20),
        name="gradient",
    )(far(warped_image), far(fixed_image), far(fine_control), far(coarse_control), far(d_matrix(sz)),
      far(h_matrix(sz)), far(y_matrix(sy)), far(z_matrices(sz)))


def solution(mesh):
    dims = tuple(mesh.shape[a] for a in ("gx", "gy", "gz"))
    in_specs = (P("gx", "gy", "gz"), P("gx", "gy", "gz"), P(None, "gx", "gy", "gz"), P())
    out_specs = (P(None, "gx", "gy", "gz"), P())
    return jax.shard_map(
        lambda *args: per_device(dims, *args), mesh=mesh, in_specs=in_specs, out_specs=out_specs, check_vma=False
    )
```

```python
import itertools

import jax
import jax.numpy as jnp
import numpy as np
from jax import lax
from jax.experimental import pallas as pl
from jax.experimental.pallas import tpu as pltpu
from jax.sharding import PartitionSpec as P

SPF = 8
SPC = 32
BEND = 0.01
FB = 0
MESH = pl.DeviceIdType.MESH
F32 = jnp.float32
BF16 = jnp.bfloat16


def beta(t):
    m = np.abs(t)
    r = 2.0 - m
    return np.where(m < 1.0, 2.0 / 3.0 - m * m + 0.5 * m**3, np.where(m < 2.0, r**3 / 6.0, 0.0))


def basis(voxels, points, spacing, first):
    v = np.arange(voxels)[:, None] + 0.5
    c = (np.arange(points)[None, :] + first) * spacing + 0.5 * spacing
    return beta((v - c) / spacing)


def halves(w):
    hi = np.asarray(w, np.float32).astype(jnp.bfloat16)
    lo = (np.asarray(w, np.float64) - hi.astype(np.float64)).astype(np.float32).astype(jnp.bfloat16)
    return hi, lo


W4 = beta((np.arange(4)[:, None] + 4.5 - 4.0 * np.arange(4)[None, :]) / 4.0) / 24.0
TWO = np.array([1.0, 4.0, 6.0, 4.0, 1.0]) / 8.0


def spread(c, step):
    out = np.zeros((len(c) - 1) * step + 1)
    out[::step] = c
    return out


C29 = np.convolve(np.convolve(TWO, spread(TWO, 2)), spread(TWO, 4))


def y_matrix(sy):
    rows = np.zeros((24, sy))
    rows[:12] = basis(sy, 12, SPF, -2).T * SPF**-1.5
    rows[16:22] = basis(sy, 6, SPC, -2).T * SPC**-1.5
    hi, lo = halves(rows)
    return np.concatenate([np.concatenate([hi, hi], 1), np.concatenate([lo, lo], 1)], 0)


def stacked(cols):
    hi, lo = halves(cols)
    half = np.concatenate([hi, lo], 1)
    return np.concatenate([half, half], 0)


def z_matrices(sz):
    fine = np.zeros((sz, 128))
    fine[:, FB : FB + 20] = basis(sz, 20, SPF, -2)
    out = [stacked(fine)]
    for a in range(3):
        cols = np.zeros((sz, 128))
        for piece in range(4):
            first = 32 * piece + 8 * a
            cols[:, first : first + 8] = basis(sz, 8, SPC, -2)
        out.append(stacked(cols))
    return np.stack(out)


def d_matrix(sz):
    d = np.zeros((sz, sz), np.float32)
    for shift, value in ((-2, 1.0), (-1, -8.0), (1, 8.0), (2, -1.0)):
        for v in range(sz):
            if 0 <= v + shift < sz:
                d[v + shift, v] = value
    return np.concatenate([d, d], 0).astype(jnp.bfloat16)


def h_matrix(sz):
    h = np.zeros((128, sz), np.float32)
    for lane in range(128):
        h[lane, (sz - 2, sz - 1, 0, 1)[lane % 4]] = 1.0
    return np.concatenate([h, h], 0).astype(jnp.bfloat16)


def split(x):
    hi = x.astype(BF16)
    return hi, (x - hi.astype(F32)).astype(BF16)


def lanes(shape):
    return lax.broadcasted_iota(jnp.int32, shape, len(shape) - 1)


def roll(x, shift, axis):
    return pltpu.roll(x, shift % x.shape[axis] if isinstance(shift, int) else shift, axis)


class Place:
    def __init__(self, dims):
        self.dims = dims
        self.pos = tuple(lax.axis_index(a) for a in ("gx", "gy", "gz"))
        self.has = [{-1: p > 0, 1: p < n - 1} for p, n in zip(self.pos, dims)]

    def exists(self, d):
        cond = None
        for i in range(3):
            if d[i]:
                one = self.has[i][d[i]]
                cond = one if cond is None else jnp.logical_and(cond, one)
        return cond

    def at(self, d):
        return tuple(self.pos[i] + d[i] for i in range(3))

    def ring(self, axis, o):
        t = lax.rem(self.pos[axis] + o, self.dims[axis])
        return tuple(t if i == axis else self.pos[i] for i in range(3)), t

    def seen(self, dx, dy):
        return self.exists((dx, dy, 0))

    def if_seen(self, dx, dy, fn):
        if dx or dy:
            pl.when(self.seen(dx, dy))(fn)
        else:
            fn()

    def beside(self, dx, dy, o):
        gx, gy, gz = self.pos
        return (gx + dx, gy + dy, lax.rem(gz + o, self.dims[2]))

    def start(self, make, k):
        d, copy = make(k)
        pl.when(self.exists(d))(lambda: copy.start())

    def sent(self, make, k):
        d, copy = make(k)
        pl.when(self.exists(d))(lambda: copy.wait_send())

    def arrived(self, make, k):
        d, copy = make(k)
        pl.when(self.exists([-v for v in d]))(lambda: copy.wait_recv())


def ring_order(n):
    return sorted(range(n), key=lambda o: -min(o, n - o))


SIDES = list(itertools.product((-1, 0, 1), repeat=2))


def gradient(dims, w_hbm, f_hbm, ctl_h, cctl_h, dz_h, h_h, wy_h, wz_h, fine_out, coarse_out,
             ctl, cctl, dz_w, h_w, wy, wz, small_sem, wb, fb, sp, diff, dzb, cz, e,
             hxr, hys, hyr, hzs, hzr, fw, xs, zs, csend, crecv, xg, total_rows, mix,
             fxr, fys, fyr, fzs, fzr, img_sem, hs, hr, cs, cr, gs, gr, fs, fr, near_sem, far_sem):
    nx, ny, nz = dims
    here = Place(dims)
    pos = here.pos
    gx, gy, gz = pos
    has, exists, at, ring, seen, if_seen, beside = (
        here.has, here.exists, here.at, here.ring, here.seen, here.if_seen, here.beside)
    start, sent, arrived = here.start, here.sent, here.arrived
    sides = SIDES
    zero8 = jnp.zeros((8, 128), F32)
    lane64 = lanes((64, 128))

    bar = pltpu.get_barrier_semaphore()
    odd = lax.rem(gx + gy + gz, 2) == 1
    even = jnp.logical_not(odd)
    faces = [tuple(side if i == axis else 0 for i in range(3)) for axis in range(3) for side in (-1, 1)]
    count = sum(has[axis][side].astype(jnp.int32) for axis in range(3) for side in (-1, 1))

    def greet_faces(sem):
        for d in faces:
            pl.when(exists(d))(lambda: pl.semaphore_signal(sem, inc=1, device_id=at(d), device_id_type=MESH))

    @pl.when(even)
    def _():
        greet_faces(bar)

    def near_done():
        @pl.when(odd)
        def _():
            pl.semaphore_wait(bar, count)
            greet_faces(near_sem)

        @pl.when(even)
        def _():
            pl.semaphore_wait(near_sem, count)

    chip = gx // 2
    lean = 2 * lax.rem(gx, 2) - 1
    next_chip = chip + lean
    has_next = (next_chip >= 0) & (next_chip < nx // 2)
    partner = (gx - lean, gy, gz)

    same = lax.rem(gy + gz, 2)
    parity = (same, 1 - same)
    line_z = [lax.rem(gz + o, nz) for o in range(nz)]
    line_y = [lax.rem(gy + o, ny) for o in range(ny)]

    def greet_chip(first, y, z, steps):
        device = (first + parity[steps % 2], y, z)
        pl.semaphore_signal(bar, inc=1, device_id=device, device_id_type=MESH)

    def far_greetings():
        for dy in (-1, 1, 0):
            def line(dy=dy):
                for o in ring_order(nz)[:-1]:
                    greet_chip(2 * chip, gy + dy, line_z[o], dy + o)

                @pl.when(has_next)
                def _():
                    for o in ring_order(nz)[:-1]:
                        greet_chip(2 * next_chip, gy + dy, line_z[o], dy + o)
            if_seen(0, dy, line)
        for oc in range(nx // 2):
            first = 2 * lax.rem(chip + oc, nx // 2)
            for oy in ring_order(ny):
                def one(first=first, oy=oy):
                    greet_chip(first, line_y[oy], gz, oy)
                if oc or oy:
                    one()
                else:
                    pl.when(odd)(one)

    def far_done():
        wide_x = 4 - (chip == 0).astype(jnp.int32) - (chip == nx // 2 - 1).astype(jnp.int32)
        wide_y = 1 + has[1][-1].astype(jnp.int32) + has[1][1].astype(jnp.int32)

        @pl.when(even)
        def _():
            pl.semaphore_wait(bar, wide_x * wide_y * (nz - 1) + nx * ny - 1)
            pl.semaphore_signal(far_sem, inc=1, device_id=partner, device_id_type=MESH)

        @pl.when(odd)
        def _():
            pl.semaphore_wait(far_sem, 1)

    chunks = 8
    planes = 8
    for c in range(chunks):
        part = pl.ds(c * planes, planes)
        pltpu.make_async_copy(w_hbm.at[part], wb.at[part], img_sem.at[0, c]).start()
        pltpu.make_async_copy(f_hbm.at[part], fb.at[part], img_sem.at[1, c]).start()
    small = [pltpu.make_async_copy(src, dst, small_sem.at[i]) for i, (src, dst) in enumerate(
        ((dz_h, dz_w), (ctl_h, ctl), (h_h, h_w), (wy_h, wy), (wz_h, wz), (cctl_h, cctl)))]
    for copy in small:
        copy.start()
    far_greetings()

    for side, d in ((0, -1), (1, 1)):
        @pl.when(jnp.logical_not(has[0][d]))
        def _(side=side):
            hxr[side] = jnp.zeros(hxr.shape[1:], F32)

        @pl.when(jnp.logical_not(has[1][d]))
        def _(side=side):
            hyr[side] = jnp.zeros(hyr.shape[1:], F32)

        @pl.when(jnp.logical_not(has[2][d]))
        def _(side=side):
            hzr[side] = jnp.zeros(hzr.shape[1:], F32)

    hzs[...] = jnp.zeros(hzs.shape, F32)
    for first in (0, 66):
        sp[first : first + 2, 8:72, :] = jnp.zeros((2, 64, 128), F32)

    def halo(k):
        axis, side = k // 2, k % 2
        d = [0, 0, 0]
        d[axis] = 2 * side - 1
        if axis == 0:
            src = sp.at[pl.ds(2 if side == 0 else 64, 2), pl.ds(8, 64), :]
            dst = hxr.at[1 - side]
        elif axis == 1:
            src, dst = hys.at[side], hyr.at[1 - side]
        else:
            src, dst = hzs, hzr.at[1 - side]
        return d, pltpu.make_async_remote_copy(
            src_ref=src, dst_ref=dst, send_sem=hs.at[k], recv_sem=hr.at[k],
            device_id=at(d), device_id_type=MESH)

    def part_of(k, c):
        axis, side = k // 2, k % 2
        if axis == 0:
            return halo(k)
        d = [0, 0, 0]
        d[axis] = 2 * side - 1
        if axis == 1:
            part = pl.ds(c * planes, planes)
            src, dst = hys.at[side, part], hyr.at[1 - side, part]
        else:
            src, dst = hzs.at[c // 4], hzr.at[1 - side, c // 4]
        return d, pltpu.make_async_remote_copy(
            src_ref=src, dst_ref=dst, send_sem=hs.at[k], recv_sem=hr.at[k],
            device_id=at(d), device_id_type=MESH)

    def send(k, c):
        d, copy = part_of(k, c)
        pl.when(exists(d))(lambda: copy.start())


    def sum_chunk(c, _):
        base = c * planes
        part = pl.ds(base, planes)
        pltpu.make_async_copy(w_hbm.at[part], wb.at[part], img_sem.at[0, c]).wait()
        pltpu.make_async_copy(f_hbm.at[part], fb.at[part], img_sem.at[1, c]).wait()
        h = c // 4
        group = lane64 // 4 - 8 * (c % 4)
        packed = hzs[h]
        for j in range(planes):
            w = wb[base + j]
            f = fb[base + j]
            s = w + f
            diff[base + j] = w - f
            sp[base + j + 2, 8:72, :] = s
            hys[0, base + j] = s[0:2]
            hys[1, base + j] = s[62:64]
            turned = roll(s, 32 * (c % 4) + 4 * j + 2, 1)
            packed = jnp.where(group == j, turned, packed)
        hzs[h] = packed
        return 0

    for c in range(chunks):
        sum_chunk(c, 0)
        if c == 3:
            near_done()
            send(0, 0)
            for k in (2, 3):
                for early in range(3):
                    send(k, early)
        if c >= 3:
            for k in (2, 3):
                send(k, c)
        if c % 4 == 3:
            for k in (4, 5):
                send(k, c)
    send(1, 0)
    small[0].wait()

    def dz_chunk(c, _):
        base = pl.multiple_of(c * 16, 16)
        for half in range(2):
            parts = [jnp.concatenate(split(sp[base + 8 * half + j + 2, 8:72, :]), 1) for j in range(8)]
            out = jnp.dot(jnp.concatenate(parts, 0), dz_w[...], preferred_element_type=F32)
            for j in range(8):
                dzb[base + 8 * half + j] = out[64 * j : 64 * (j + 1)]
        return 0

    lax.fori_loop(0, 4, dz_chunk, 0, unroll=True)

    groups = 16
    slabs = groups + 3
    even4 = 0.5 * (W4 + W4[::-1])
    odd4 = 0.5 * (W4 - W4[::-1])

    def column(axes):
        per = 4

        def one(yt, _):
            r0 = pl.multiple_of(8 * yt, 8)

            def put(a, g, value):
                xs[pl.ds(r0, 8), pl.ds(pl.multiple_of((a * slabs + g) * 128, 128), 128)] = value

            def some(gg, acc):
                acc = [list(row) for row in acc]
                x0 = 4 * per * gg
                if 0 in axes:
                    c = [sp[x0 + i, pl.ds(r0 + 8, 8), :] for i in range(4 * per + 4)]
                for sub in range(per):
                    force = [[] for _ in axes]
                    for k in range(4):
                        i = 4 * sub + k
                        dv = diff[x0 + i, pl.ds(r0, 8), :]
                        for n, a in enumerate(axes):
                            if a == 0:
                                s = (c[i] - c[i + 4]) + 8.0 * (c[i + 3] - c[i + 1])
                            elif a == 1:
                                ym2, ym1, yp1, yp2 = (
                                    sp[x0 + i + 2, pl.ds(r0 + o, 8), :] for o in (6, 7, 9, 10))
                                s = (ym2 - yp2) + 8.0 * (yp1 - ym1)
                            else:
                                s = dzb[x0 + i, pl.ds(r0, 8), :]
                            force[n].append(dv * s)
                    for n, a in enumerate(axes):
                        f = force[n]
                        e0, e1, o0, o1 = f[0] + f[3], f[1] + f[2], f[0] - f[3], f[1] - f[2]
                        for m in range(2):
                            both = float(even4[0, m]) * e0 + float(even4[1, m]) * e1
                            diff4 = float(odd4[0, m]) * o0 + float(odd4[1, m]) * o1
                            acc[n][m] = acc[n][m] + (both + diff4)
                            acc[n][3 - m] = acc[n][3 - m] + (both - diff4)
                        put(a, per * gg + sub, acc[n][0])
                        acc[n] = [acc[n][1], acc[n][2], acc[n][3], zero8]
                return tuple(tuple(row) for row in acc)

            acc = lax.fori_loop(0, groups // per, some, tuple(tuple(zero8 for _ in range(4)) for _ in axes))
            for n, a in enumerate(axes):
                for m in range(3):
                    put(a, groups + m, acc[n][m])
            return 0

        return one

    lax.fori_loop(1, 7, column((0, 1)), 0)
    lax.fori_loop(0, 2, lambda i, _: column((0,))(7 * i, 0), 0)

    for side, d in ((0, -1), (1, 1)):
        for axis, ref in enumerate((fxr, fyr, fzr)):
            @pl.when(jnp.logical_not(has[axis][d]))
            def _(side=side, ref=ref):
                ref[side] = jnp.zeros(ref.shape[1:], F32)
    for dx, dy in sides:
        if dx or dy:
            @pl.when(jnp.logical_not(seen(-dx, -dy)))
            def _(dx=dx, dy=dy):
                crecv[3 * (dx + 1) + dy + 1] = zero8

    for k in range(6):
        arrived(halo, k)

    def place_y(x, _):
        sp[x + 2, 6:8, :] = hyr[0, x]
        sp[x + 2, 72:74, :] = hyr[1, x]
        return 0

    lax.fori_loop(0, 64, place_y, 0, unroll=8)

    m4 = lane64 % 4
    for h in range(2):
        u = jnp.where(m4 < 2, hzr[0, h], hzr[1, h])
        a_part = jnp.where(m4 < 2, -roll(u, -2, 1), roll(u, 2, 1))
        b_part = jnp.where(m4 == 1, 8.0 * roll(u, -1, 1), jnp.where(m4 == 2, -8.0 * roll(u, 1, 1), 0.0))
        cz[h] = a_part + b_part
    plane = sorted(((ox, oy) for ox in range(nx) for oy in range(ny) if ox or oy),
                   key=lambda o: -min(o[1], ny - o[1]) - 0.5 * min(o[0], nx - o[0]))

    def in_plane(ox, oy):
        return (lax.rem(gx + ox, nx), lax.rem(gy + oy, ny), gz)

    def fine_copy(k):
        axis, side = k // 2, k % 2
        d = [0, 0, 0]
        d[axis] = 2 * side - 1
        if axis == 0:
            src, dst = e.at[:, pl.ds(10 * side, 2)], fxr.at[1 - side]
        elif axis == 1:
            src, dst = fys.at[side], fyr.at[1 - side]
        else:
            src, dst = fzs.at[side], fzr.at[1 - side]
        return d, pltpu.make_async_remote_copy(
            src_ref=src, dst_ref=dst, send_sem=fs.at[k], recv_sem=fr.at[k],
            device_id=at(d), device_id_type=MESH)

    small[2].wait()

    def z_fix(c, _):
        base = pl.multiple_of(c * 16, 16)
        layer = cz[c // 2]
        for half in range(2):
            group = lane64 // 4 - 16 * lax.rem(c, 2) - 8 * half
            parts = [jnp.concatenate(split(jnp.where(group == j, layer, 0.0)), 1) for j in range(8)]
            out = jnp.dot(jnp.concatenate(parts, 0), h_w[...], preferred_element_type=F32)
            for j in range(8):
                dzb[base + 8 * half + j] = dzb[base + 8 * half + j] + out[64 * j : 64 * (j + 1)]
        return 0

    lax.fori_loop(0, 4, z_fix, 0, unroll=True)

    outer = (
        (0, diff[0] * (hxr[0, 0] - 8.0 * hxr[0, 1]), diff[1] * hxr[0, 1], 0),
        (groups - 1, diff[62] * -hxr[1, 0], diff[63] * (8.0 * hxr[1, 0] - hxr[1, 1]), 2),
    )
    for g, f0, f1, k in outer:
        for m in range(4):
            part = slice(128 * (g + m), 128 * (g + m + 1))
            xs[:, part] = xs[:, part] + (float(W4[k, m]) * f0 + float(W4[k + 1, m]) * f1)

    lax.fori_loop(1, 7, column((2,)), 0)
    lax.fori_loop(0, 2, lambda i, _: column((1, 2))(7 * i, 0), 0)

    for copy in small[3:]:
        copy.wait()
    total = None
    for a in range(3):
        x = xs[:, a * slabs * 128 : (a + 1) * slabs * 128]
        hi, lo = split(x)
        y = jnp.dot(wy[...], jnp.concatenate([hi, lo], 0), preferred_element_type=F32)
        y = y[:24] + y[24:]
        pieces = [y[:, 128 * i : 128 * (i + 1)] for i in range(slabs)]
        hi, lo = split(jnp.concatenate([p[16:24] for p in pieces], 0))
        z = jnp.dot(jnp.concatenate([hi, lo], 1), wz[1 + a], preferred_element_type=F32)
        z = z[:, :128] + z[:, 128:]
        total = z if total is None else total + z
        for i in range(slabs):
            zs[a, i] = pieces[i][:16]

    lane8 = lanes((8, 128))
    taken = []
    for jj in range(6):
        v = None
        for i in range(slabs):
            tap = i - 8 * jj + 25
            if 0 <= tap < 29:
                term = float(C29[tap]) * total[8 * i : 8 * (i + 1)]
                v = term if v is None else v + term
        taken.append(v)
    for g in range(3):
        v = jnp.where(lane8 < 64, taken[2 * g], taken[2 * g + 1])
        csend[g] = jnp.where(lane8 // 32 % 2 == 0, v, roll(v, -1, 0))
    crecv[4, pl.ds(gz, 1), :] = csend[1, 2:3, :]

    def coarse_copy(dx, dy, o):
        slot = 3 * (dx + 1) + dy + 1
        return pltpu.make_async_remote_copy(
            src_ref=csend.at[dx + 1, pl.ds(2 * (dy + 1), 1), :], dst_ref=crecv.at[slot, pl.ds(gz, 1), :],
            send_sem=cs.at[slot], recv_sem=cr.at[slot], device_id=beside(dx, dy, o), device_id_type=MESH)

    def coarse_line(dx, dy):
        slot = 3 * (dx + 1) + dy + 1
        rows = crecv.at[slot] if dx or dy else crecv.at[slot, pl.ds(0, nz - 1), :]
        return pltpu.make_async_remote_copy(
            src_ref=rows, dst_ref=rows, send_sem=cs.at[slot], recv_sem=cr.at[slot],
            device_id=beside(0, 0, 1), device_id_type=MESH)

    def coarse_all(fn):
        for o in ring_order(nz):
            for dx, dy in sorted(sides, key=lambda d: -abs(d[0]) - abs(d[1])):
                if o or dx or dy:
                    fn(dx, dy, o)

    far_done()
    coarse_all(lambda dx, dy, o: if_seen(dx, dy, lambda: coarse_copy(dx, dy, o).start()))

    small[1].wait()

    row16 = lax.broadcasted_iota(jnp.int32, (16, 128), 0)
    lane16 = lanes((16, 128))
    row_g = row16 - 2 + gy * 8
    lane_g = lane16 - (FB + 2) + gz * 16
    in_grid = (row_g >= 0) & (row_g < ny * 8) & (lane_g >= 0) & (lane_g < nz * 16)

    def lap(centre, low, high):
        total = roll(centre, 1, 0) + roll(centre, -1, 0) + roll(centre, 1, 1) + roll(centre, -1, 1)
        if low is not None:
            total = total + low
        if high is not None:
            total = total + high
        return total - 6.0 * centre

    def fine_bend(a, _):
        for j in range(8):
            block = jnp.concatenate([ctl[a, j], jnp.zeros((8, 112), F32)], 1)
            block = jnp.concatenate([block, zero8], 0)
            fw[j + 2] = roll(roll(block, 2, 0), FB + 2, 1)
        zero16 = jnp.zeros((16, 128), F32)
        for j in (0, 1, 10, 11):
            fw[j] = zero16
        first = []
        for j in range(12):
            if j in (0, 11):
                first.append(None)
                continue
            low = fw[j - 1] if 0 < j else None
            high = fw[j + 1] if j < 11 else None
            value = lap(fw[j], low, high)
            p = gx * 8 + j - 2
            ok = in_grid & (p >= 0) & (p < nx * 8)
            first.append(jnp.where(ok, value, 0.0))
        for j in range(12):
            centre = first[j] if first[j] is not None else zero16
            low = first[j - 1] if j > 0 else None
            high = first[j + 1] if j < 11 else None
            e[a, j] = BEND * lap(centre, low, high)
        return 0

    lax.fori_loop(0, 3, fine_bend, 0)

    for a in range(3):
        hi, lo = split(zs[a].reshape(16 * slabs, 128))
        z = jnp.dot(jnp.concatenate([hi, lo], 1), wz[0], preferred_element_type=F32)
        z = z[:, :128] + z[:, 128:]
        for j in range(12):
            v = e[a, j]
            for k in range(5):
                i = 2 * j - 4 + k
                if 0 <= i < slabs:
                    v = v + float(TWO[k]) * z[16 * i : 16 * (i + 1)]
            e[a, j] = v
    for k in (0, 1):
        start(fine_copy, k)

    kx, ky, kz = cctl.shape[1:]
    shape = (ky, kz)
    crow = lax.broadcasted_iota(jnp.int32, (ky, 128), 0)
    clane = lanes((ky, 128))

    def clap(centre, low, high):
        total = jnp.where(crow > 0, roll(centre, 1, 0), 0.0) + jnp.where(crow < ky - 1, roll(centre, -1, 0), 0.0)
        total = total + roll(centre, 1, 1) + roll(centre, -1, 1)
        if low is not None:
            total = total + low
        if high is not None:
            total = total + high
        return jnp.where(clane < kz, total - 6.0 * centre, 0.0)

    def coarse_bend(a, _):
        field = [jnp.concatenate([cctl[a, j], jnp.zeros((ky, 128 - kz), F32)], 1) for j in range(kx)]
        for _level in range(2):
            field = [clap(field[j], field[j - 1] if j else None, field[j + 1] if j < kx - 1 else None)
                     for j in range(kx)]
        for j in range(kx):
            coarse_out[a, j] = BEND * field[j][:, :kz]
        return 0

    lax.fori_loop(0, 3, coarse_bend, 0)

    for k in (0, 1):
        sent(fine_copy, k)
        arrived(fine_copy, k)
    for a in range(3):
        for j in range(8):
            v = e[a, j + 2]
            if j < 2:
                v = v + fxr[0, a, j]
            if j >= 6:
                v = v + fxr[1, a, j - 6]
            e[a, j + 2] = v
            fys[0, 8 * a + j] = v[0:2]
            fys[1, 8 * a + j] = v[10:12]
    for k in (2, 3):
        start(fine_copy, k)

    for dx, dy in sides:
        if_seen(-dx, -dy, lambda: coarse_line(dx, dy).wait_recv())
    line = crecv[0]
    for i in range(1, 9):
        line = line + crecv[i]
    line = pltpu.roll(line, 0, 1, stride=4, stride_axis=0)
    place = lane8 % 32 + 2 - 4 * lax.broadcasted_iota(jnp.int32, (8, 128), 0)
    for a in range(3):
        piece = jnp.where((place >= 0) & (place < 8), roll(line, -2 - 8 * a, 1), 0.0)
        xg[gx, a, pl.ds(gy, 1), :] = jnp.sum(piece, axis=0, keepdims=True)

    def gather_copy(ox, oy, sx, sy):
        slot = xg.at[sx, :, pl.ds(sy, 1), :]
        return pltpu.make_async_remote_copy(
            src_ref=slot, dst_ref=slot, send_sem=gs, recv_sem=gr,
            device_id=in_plane(ox, oy), device_id_type=MESH)

    def gather_plane():
        return pltpu.make_async_remote_copy(
            src_ref=total_rows, dst_ref=total_rows, send_sem=gs, recv_sem=gr,
            device_id=in_plane(0, 1), device_id_type=MESH)

    for ox, oy in plane:
        gather_copy(ox, oy, gx, gy).start()

    for k in (2, 3):
        arrived(fine_copy, k)
    pack0 = zero8
    pack1 = zero8
    zero4 = jnp.zeros((4, 128), F32)
    for a in range(3):
        for j in range(8):
            s = 8 * a + j
            v = e[a, j + 2]
            edges = jnp.concatenate([fyr[0, s], zero4, fyr[1, s]], 0)
            v = roll(v, -2, 0)[0:8] + edges
            e[a, j + 2, 0:8, :] = v
            turned = roll(v, 2 * s - FB, 1)
            pack0 = jnp.where(lane8 // 2 == s, turned, pack0)
            pack1 = jnp.where(lane8 // 2 == s + 9, turned, pack1)
    fzs[0] = pack0
    fzs[1] = pack1
    for k in (4, 5):
        start(fine_copy, k)

    for k in (4, 5):
        arrived(fine_copy, k)
    p0 = fzr[0]
    p1 = fzr[1]
    for a in range(3):
        for j in range(8):
            s = 8 * a + j
            v = roll(e[a, j + 2, 0:8, :], -(FB + 2), 1)
            v = v + jnp.where(lane8 < 2, roll(p0, -(18 + 2 * s), 1), 0.0)
            v = v + jnp.where((lane8 >= 14) & (lane8 < 16), roll(p1, 14 - 2 * s, 1), 0.0)
            fine_out[a, j] = v[:, :16]

    gather_plane().wait_recv()
    for g in range(nx):
        for a in range(3):
            rows = xg[g, a]
            for p in range(2):
                for q in range(2):
                    mix[a, 2 * g + p, pl.ds(q, ny, stride=2), :] = roll(rows, -(64 * p + 32 * q), 1)
    for a in range(3):
        for j in range(kx):
            coarse_out[a, j] = coarse_out[a, j] + mix[a, j][:, :kz]

    for k in range(6):
        sent(halo, k)
    for k in range(2, 6):
        sent(fine_copy, k)
    for dx, dy in sides:
        if_seen(dx, dy, lambda: coarse_line(dx, dy).wait_send())
    gather_plane().wait_send()


def per_device(dims, warped_image, fixed_image, fine_control, coarse_control):
    sx, sy, sz = warped_image.shape
    kx, ky, kz = coarse_control.shape[1:]
    nx, ny, nz = dims
    slabs = 19
    vmem = pl.BlockSpec(memory_space=pltpu.VMEM)
    hbm = pl.BlockSpec(memory_space=pltpu.HBM)
    v = lambda *shape: pltpu.VMEM(shape, F32)
    h = lambda *shape: pltpu.VMEM(shape, BF16)
    out = lambda *shape: jax.ShapeDtypeStruct(shape, F32)
    dma = pltpu.SemaphoreType.DMA
    flag = pltpu.SemaphoreType.REGULAR
    far = lambda x: pltpu.with_memory_space_constraint(jnp.asarray(x), pltpu.HBM)
    return pl.pallas_call(
        lambda *refs: gradient(dims, *refs),
        out_shape=(out(*fine_control.shape), out(*coarse_control.shape)),
        in_specs=[hbm] * 8,
        out_specs=(vmem, vmem),
        scratch_shapes=[
            v(*fine_control.shape), v(*coarse_control.shape), h(2 * sz, sz), h(256, sz), h(48, 2 * sy),
            h(4, 2 * sz, 256), dma((6,)), v(sx, sy, sz), v(sx, sy, sz), v(sx + 4, sy + 16, sz), v(sx, sy, sz),
            v(sx, sy, sz), v(2, sy, 128), v(3, 12, 16, 128),
            v(2, 2, sy, sz), v(2, sx, 2, sz), v(2, sx, 2, sz), v(2, sy, 128), v(2, 2, sy, 128), v(12, 16, 128),
            v(sy, 3 * slabs * 128), v(3, slabs, 16, 128), v(3, 8, 128), v(9, nz, 128),
            v(nx, 3, ny, 128), v(3 * (nx * ny - 1), 128), v(3, kx, ky, 128),
            v(2, 3, 2, 16, 128), v(2, 24, 2, 128), v(2, 24, 2, 128), v(2, 8, 128), v(2, 8, 128),
            dma((2, 8)), dma((6,)), dma((6,)), dma((9,)), dma((9,)), dma, dma, dma((6,)), dma((6,)), flag, flag,
        ],
        compiler_params=pltpu.CompilerParams(collective_id=0, has_side_effects=True, vmem_limit_bytes=48 << 20),
        name="gradient",
    )(far(warped_image), far(fixed_image), far(fine_control), far(coarse_control), far(d_matrix(sz)),
      far(h_matrix(sz)), far(y_matrix(sy)), far(z_matrices(sz)))


def solution(mesh):
    dims = tuple(mesh.shape[a] for a in ("gx", "gy", "gz"))
    in_specs = (P("gx", "gy", "gz"), P("gx", "gy", "gz"), P(None, "gx", "gy", "gz"), P())
    out_specs = (P(None, "gx", "gy", "gz"), P())
    return jax.shard_map(
        lambda *args: per_device(dims, *args), mesh=mesh, in_specs=in_specs, out_specs=out_specs, check_vma=False
    )
```

```python
import itertools

import jax
import jax.numpy as jnp
import numpy as np
from jax import lax
from jax.experimental import pallas as pl
from jax.experimental.pallas import tpu as pltpu
from jax.sharding import PartitionSpec as P

SPF = 8
SPC = 32
BEND = 0.01
FB = 0
MESH = pl.DeviceIdType.MESH
F32 = jnp.float32
BF16 = jnp.bfloat16


def beta(t):
    m = np.abs(t)
    r = 2.0 - m
    return np.where(m < 1.0, 2.0 / 3.0 - m * m + 0.5 * m**3, np.where(m < 2.0, r**3 / 6.0, 0.0))


def basis(voxels, points, spacing, first):
    v = np.arange(voxels)[:, None] + 0.5
    c = (np.arange(points)[None, :] + first) * spacing + 0.5 * spacing
    return beta((v - c) / spacing)


def halves(w):
    hi = np.asarray(w, np.float32).astype(jnp.bfloat16)
    lo = (np.asarray(w, np.float64) - hi.astype(np.float64)).astype(np.float32).astype(jnp.bfloat16)
    return hi, lo


W4 = beta((np.arange(4)[:, None] + 4.5 - 4.0 * np.arange(4)[None, :]) / 4.0) / 24.0
TWO = np.array([1.0, 4.0, 6.0, 4.0, 1.0]) / 8.0


def spread(c, step):
    out = np.zeros((len(c) - 1) * step + 1)
    out[::step] = c
    return out


C29 = np.convolve(np.convolve(TWO, spread(TWO, 2)), spread(TWO, 4))


def y_matrix(sy):
    rows = np.zeros((24, sy))
    rows[:12] = basis(sy, 12, SPF, -2).T * SPF**-1.5
    rows[16:22] = basis(sy, 6, SPC, -2).T * SPC**-1.5
    hi, lo = halves(rows)
    return np.concatenate([np.concatenate([hi, hi], 1), np.concatenate([lo, lo], 1)], 0)


def stacked(cols):
    hi, lo = halves(cols)
    half = np.concatenate([hi, lo], 1)
    return np.concatenate([half, half], 0)


def z_matrices(sz):
    fine = np.zeros((sz, 128))
    fine[:, FB : FB + 20] = basis(sz, 20, SPF, -2)
    out = [stacked(fine)]
    for a in range(3):
        cols = np.zeros((sz, 128))
        for piece in range(4):
            first = 32 * piece + 8 * a
            cols[:, first : first + 8] = basis(sz, 8, SPC, -2)
        out.append(stacked(cols))
    return np.stack(out)


def d_matrix(sz):
    d = np.zeros((sz, sz), np.float32)
    for shift, value in ((-2, 1.0), (-1, -8.0), (1, 8.0), (2, -1.0)):
        for v in range(sz):
            if 0 <= v + shift < sz:
                d[v + shift, v] = value
    return np.concatenate([d, d], 0).astype(jnp.bfloat16)


def h_matrix(sz):
    h = np.zeros((128, sz), np.float32)
    for lane in range(128):
        h[lane, (sz - 2, sz - 1, 0, 1)[lane % 4]] = 1.0
    return np.concatenate([h, h], 0).astype(jnp.bfloat16)


def split(x):
    hi = x.astype(BF16)
    return hi, (x - hi.astype(F32)).astype(BF16)


def lanes(shape):
    return lax.broadcasted_iota(jnp.int32, shape, len(shape) - 1)


def roll(x, shift, axis):
    return pltpu.roll(x, shift % x.shape[axis] if isinstance(shift, int) else shift, axis)


class Place:
    def __init__(self, dims):
        self.dims = dims
        self.pos = tuple(lax.axis_index(a) for a in ("gx", "gy", "gz"))
        self.has = [{-1: p > 0, 1: p < n - 1} for p, n in zip(self.pos, dims)]

    def exists(self, d):
        cond = None
        for i in range(3):
            if d[i]:
                one = self.has[i][d[i]]
                cond = one if cond is None else jnp.logical_and(cond, one)
        return cond

    def at(self, d):
        return tuple(self.pos[i] + d[i] for i in range(3))

    def ring(self, axis, o):
        t = lax.rem(self.pos[axis] + o, self.dims[axis])
        return tuple(t if i == axis else self.pos[i] for i in range(3)), t

    def seen(self, dx, dy):
        return self.exists((dx, dy, 0))

    def if_seen(self, dx, dy, fn):
        if dx or dy:
            pl.when(self.seen(dx, dy))(fn)
        else:
            fn()

    def beside(self, dx, dy, o):
        gx, gy, gz = self.pos
        return (gx + dx, gy + dy, lax.rem(gz + o, self.dims[2]))

    def start(self, make, k):
        d, copy = make(k)
        pl.when(self.exists(d))(lambda: copy.start())

    def sent(self, make, k):
        d, copy = make(k)
        pl.when(self.exists(d))(lambda: copy.wait_send())

    def arrived(self, make, k):
        d, copy = make(k)
        pl.when(self.exists([-v for v in d]))(lambda: copy.wait_recv())


def ring_order(n):
    return sorted(range(n), key=lambda o: -min(o, n - o))


SIDES = list(itertools.product((-1, 0, 1), repeat=2))


def gradient(dims, w_hbm, f_hbm, ctl_h, cctl_h, dz_h, h_h, wy_h, wz_h, fine_out, coarse_out,
             ctl, cctl, dz_w, h_w, wy, wz, small_sem, wb, fb, sp, diff, dzb, cz, e,
             hxr, hys, hyr, hzs, hzr, fw, xs, zs, csend, crecv, xg, total_rows, mix,
             fxr, fys, fyr, fzs, fzr, img_sem, hs, hr, cs, cr, gs, gr, fs, fr, near_sem, far_sem):
    nx, ny, nz = dims
    here = Place(dims)
    pos = here.pos
    gx, gy, gz = pos
    has, exists, at, ring, seen, if_seen, beside = (
        here.has, here.exists, here.at, here.ring, here.seen, here.if_seen, here.beside)
    start, sent, arrived = here.start, here.sent, here.arrived
    sides = SIDES
    zero8 = jnp.zeros((8, 128), F32)
    lane64 = lanes((64, 128))

    bar = pltpu.get_barrier_semaphore()
    odd = lax.rem(gx + gy + gz, 2) == 1
    even = jnp.logical_not(odd)
    faces = [tuple(side if i == axis else 0 for i in range(3)) for axis in range(3) for side in (-1, 1)]
    count = sum(has[axis][side].astype(jnp.int32) for axis in range(3) for side in (-1, 1))

    def greet_faces(sem):
        for d in faces:
            pl.when(exists(d))(lambda: pl.semaphore_signal(sem, inc=1, device_id=at(d), device_id_type=MESH))

    @pl.when(even)
    def _():
        greet_faces(bar)

    def near_done():
        @pl.when(odd)
        def _():
            pl.semaphore_wait(bar, count)
            greet_faces(near_sem)

        @pl.when(even)
        def _():
            pl.semaphore_wait(near_sem, count)

    chip = gx // 2
    lean = 2 * lax.rem(gx, 2) - 1
    next_chip = chip + lean
    has_next = (next_chip >= 0) & (next_chip < nx // 2)
    partner = (gx - lean, gy, gz)

    same = lax.rem(gy + gz, 2)
    parity = (same, 1 - same)
    line_z = [lax.rem(gz + o, nz) for o in range(nz)]
    line_y = [lax.rem(gy + o, ny) for o in range(ny)]

    def greet_chip(first, y, z, steps):
        device = (first + parity[steps % 2], y, z)
        pl.semaphore_signal(bar, inc=1, device_id=device, device_id_type=MESH)

    def far_greetings():
        for dy in (-1, 1, 0):
            def line(dy=dy):
                for o in ring_order(nz)[:-1]:
                    greet_chip(2 * chip, gy + dy, line_z[o], dy + o)

                @pl.when(has_next)
                def _():
                    for o in ring_order(nz)[:-1]:
                        greet_chip(2 * next_chip, gy + dy, line_z[o], dy + o)
            if_seen(0, dy, line)
        for oc in range(nx // 2):
            first = 2 * lax.rem(chip + oc, nx // 2)
            for oy in ring_order(ny):
                def one(first=first, oy=oy):
                    greet_chip(first, line_y[oy], gz, oy)
                if oc or oy:
                    one()
                else:
                    pl.when(odd)(one)

    def far_done():
        wide_x = 4 - (chip == 0).astype(jnp.int32) - (chip == nx // 2 - 1).astype(jnp.int32)
        wide_y = 1 + has[1][-1].astype(jnp.int32) + has[1][1].astype(jnp.int32)

        @pl.when(even)
        def _():
            pl.semaphore_wait(bar, wide_x * wide_y * (nz - 1) + nx * ny - 1)
            pl.semaphore_signal(far_sem, inc=1, device_id=partner, device_id_type=MESH)

        @pl.when(odd)
        def _():
            pl.semaphore_wait(far_sem, 1)

    chunks = 8
    planes = 8
    for c in range(chunks):
        part = pl.ds(c * planes, planes)
        pltpu.make_async_copy(w_hbm.at[part], wb.at[part], img_sem.at[0, c]).start()
        pltpu.make_async_copy(f_hbm.at[part], fb.at[part], img_sem.at[1, c]).start()
    small = [pltpu.make_async_copy(src, dst, small_sem.at[i]) for i, (src, dst) in enumerate(
        ((dz_h, dz_w), (ctl_h, ctl), (h_h, h_w), (wy_h, wy), (wz_h, wz), (cctl_h, cctl)))]
    for copy in small:
        copy.start()
    far_greetings()

    for side, d in ((0, -1), (1, 1)):
        @pl.when(jnp.logical_not(has[0][d]))
        def _(side=side):
            hxr[side] = jnp.zeros(hxr.shape[1:], F32)

        @pl.when(jnp.logical_not(has[1][d]))
        def _(side=side):
            hyr[side] = jnp.zeros(hyr.shape[1:], F32)

        @pl.when(jnp.logical_not(has[2][d]))
        def _(side=side):
            hzr[side] = jnp.zeros(hzr.shape[1:], F32)

    hzs[...] = jnp.zeros(hzs.shape, F32)
    for first in (0, 66):
        sp[first : first + 2, 8:72, :] = jnp.zeros((2, 64, 128), F32)

    def halo(k):
        axis, side = k // 2, k % 2
        d = [0, 0, 0]
        d[axis] = 2 * side - 1
        if axis == 0:
            src = sp.at[pl.ds(2 if side == 0 else 64, 2), pl.ds(8, 64), :]
            dst = hxr.at[1 - side]
        elif axis == 1:
            src, dst = hys.at[side], hyr.at[1 - side]
        else:
            src, dst = hzs, hzr.at[1 - side]
        return d, pltpu.make_async_remote_copy(
            src_ref=src, dst_ref=dst, send_sem=hs.at[k], recv_sem=hr.at[k],
            device_id=at(d), device_id_type=MESH)

    def part_of(k, c):
        axis, side = k // 2, k % 2
        if axis == 0:
            return halo(k)
        d = [0, 0, 0]
        d[axis] = 2 * side - 1
        if axis == 1:
            part = pl.ds(c * planes, planes)
            src, dst = hys.at[side, part], hyr.at[1 - side, part]
        else:
            src, dst = hzs.at[c // 4], hzr.at[1 - side, c // 4]
        return d, pltpu.make_async_remote_copy(
            src_ref=src, dst_ref=dst, send_sem=hs.at[k], recv_sem=hr.at[k],
            device_id=at(d), device_id_type=MESH)

    def send(k, c):
        d, copy = part_of(k, c)
        pl.when(exists(d))(lambda: copy.start())


    def sum_chunk(c, _):
        base = c * planes
        part = pl.ds(base, planes)
        pltpu.make_async_copy(w_hbm.at[part], wb.at[part], img_sem.at[0, c]).wait()
        pltpu.make_async_copy(f_hbm.at[part], fb.at[part], img_sem.at[1, c]).wait()
        h = c // 4
        group = lane64 // 4 - 8 * (c % 4)
        packed = hzs[h]
        for j in range(planes):
            w = wb[base + j]
            f = fb[base + j]
            s = w + f
            diff[base + j] = w - f
            sp[base + j + 2, 8:72, :] = s
            hys[0, base + j] = s[0:2]
            hys[1, base + j] = s[62:64]
            turned = roll(s, 32 * (c % 4) + 4 * j + 2, 1)
            packed = jnp.where(group == j, turned, packed)
        hzs[h] = packed
        return 0

    for c in range(chunks):
        sum_chunk(c, 0)
        if c == 3:
            near_done()
            send(0, 0)
            for k in (2, 3):
                for early in range(3):
                    send(k, early)
        if c >= 3:
            for k in (2, 3):
                send(k, c)
        if c % 4 == 3:
            for k in (4, 5):
                send(k, c)
    send(1, 0)
    small[0].wait()

    def dz_chunk(c, _):
        base = pl.multiple_of(c * 16, 16)
        for half in range(2):
            parts = [jnp.concatenate(split(sp[base + 8 * half + j + 2, 8:72, :]), 1) for j in range(8)]
            out = jnp.dot(jnp.concatenate(parts, 0), dz_w[...], preferred_element_type=F32)
            for j in range(8):
                dzb[base + 8 * half + j] = out[64 * j : 64 * (j + 1)]
        return 0

    lax.fori_loop(0, 4, dz_chunk, 0, unroll=True)

    groups = 16
    slabs = groups + 3
    even4 = 0.5 * (W4 + W4[::-1])
    odd4 = 0.5 * (W4 - W4[::-1])

    def column(axes):
        per = 4

        def one(yt, _):
            r0 = pl.multiple_of(8 * yt, 8)

            def put(a, g, value):
                xs[pl.ds(r0, 8), pl.ds(pl.multiple_of((a * slabs + g) * 128, 128), 128)] = value

            def some(gg, acc):
                acc = [list(row) for row in acc]
                x0 = 4 * per * gg
                if 0 in axes:
                    c = [sp[x0 + i, pl.ds(r0 + 8, 8), :] for i in range(4 * per + 4)]
                for sub in range(per):
                    force = [[] for _ in axes]
                    for k in range(4):
                        i = 4 * sub + k
                        dv = diff[x0 + i, pl.ds(r0, 8), :]
                        for n, a in enumerate(axes):
                            if a == 0:
                                s = (c[i] - c[i + 4]) + 8.0 * (c[i + 3] - c[i + 1])
                            elif a == 1:
                                ym2, ym1, yp1, yp2 = (
                                    sp[x0 + i + 2, pl.ds(r0 + o, 8), :] for o in (6, 7, 9, 10))
                                s = (ym2 - yp2) + 8.0 * (yp1 - ym1)
                            else:
                                s = dzb[x0 + i, pl.ds(r0, 8), :]
                            force[n].append(dv * s)
                    for n, a in enumerate(axes):
                        f = force[n]
                        e0, e1, o0, o1 = f[0] + f[3], f[1] + f[2], f[0] - f[3], f[1] - f[2]
                        for m in range(2):
                            both = float(even4[0, m]) * e0 + float(even4[1, m]) * e1
                            diff4 = float(odd4[0, m]) * o0 + float(odd4[1, m]) * o1
                            acc[n][m] = acc[n][m] + (both + diff4)
                            acc[n][3 - m] = acc[n][3 - m] + (both - diff4)
                        put(a, per * gg + sub, acc[n][0])
                        acc[n] = [acc[n][1], acc[n][2], acc[n][3], zero8]
                return tuple(tuple(row) for row in acc)

            acc = lax.fori_loop(0, groups // per, some, tuple(tuple(zero8 for _ in range(4)) for _ in axes))
            for n, a in enumerate(axes):
                for m in range(3):
                    put(a, groups + m, acc[n][m])
            return 0

        return one

    lax.fori_loop(1, 7, column((0, 1)), 0)
    lax.fori_loop(0, 2, lambda i, _: column((0,))(7 * i, 0), 0)

    for side, d in ((0, -1), (1, 1)):
        for axis, ref in enumerate((fxr, fyr, fzr)):
            @pl.when(jnp.logical_not(has[axis][d]))
            def _(side=side, ref=ref):
                ref[side] = jnp.zeros(ref.shape[1:], F32)
    for dx, dy in sides:
        if dx or dy:
            @pl.when(jnp.logical_not(seen(-dx, -dy)))
            def _(dx=dx, dy=dy):
                crecv[3 * (dx + 1) + dy + 1] = zero8

    for k in range(6):
        arrived(halo, k)

    def place_y(x, _):
        sp[x + 2, 6:8, :] = hyr[0, x]
        sp[x + 2, 72:74, :] = hyr[1, x]
        return 0

    lax.fori_loop(0, 64, place_y, 0, unroll=8)

    m4 = lane64 % 4
    for h in range(2):
        u = jnp.where(m4 < 2, hzr[0, h], hzr[1, h])
        a_part = jnp.where(m4 < 2, -roll(u, -2, 1), roll(u, 2, 1))
        b_part = jnp.where(m4 == 1, 8.0 * roll(u, -1, 1), jnp.where(m4 == 2, -8.0 * roll(u, 1, 1), 0.0))
        cz[h] = a_part + b_part
    plane = sorted(((ox, oy) for ox in range(nx) for oy in range(ny) if ox or oy),
                   key=lambda o: -min(o[1], ny - o[1]) - 0.5 * min(o[0], nx - o[0]))

    def in_plane(ox, oy):
        return (lax.rem(gx + ox, nx), lax.rem(gy + oy, ny), gz)

    def fine_copy(k):
        axis, side = k // 2, k % 2
        d = [0, 0, 0]
        d[axis] = 2 * side - 1
        if axis == 0:
            src, dst = e.at[:, pl.ds(10 * side, 2)], fxr.at[1 - side]
        elif axis == 1:
            src, dst = fys.at[side], fyr.at[1 - side]
        else:
            src, dst = fzs.at[side], fzr.at[1 - side]
        return d, pltpu.make_async_remote_copy(
            src_ref=src, dst_ref=dst, send_sem=fs.at[k], recv_sem=fr.at[k],
            device_id=at(d), device_id_type=MESH)

    small[2].wait()

    def z_fix(c, _):
        base = pl.multiple_of(c * 16, 16)
        layer = cz[c // 2]
        for half in range(2):
            group = lane64 // 4 - 16 * lax.rem(c, 2) - 8 * half
            parts = [jnp.concatenate(split(jnp.where(group == j, layer, 0.0)), 1) for j in range(8)]
            out = jnp.dot(jnp.concatenate(parts, 0), h_w[...], preferred_element_type=F32)
            for j in range(8):
                dzb[base + 8 * half + j] = dzb[base + 8 * half + j] + out[64 * j : 64 * (j + 1)]
        return 0

    lax.fori_loop(0, 4, z_fix, 0, unroll=True)

    outer = (
        (0, diff[0] * (hxr[0, 0] - 8.0 * hxr[0, 1]), diff[1] * hxr[0, 1], 0),
        (groups - 1, diff[62] * -hxr[1, 0], diff[63] * (8.0 * hxr[1, 0] - hxr[1, 1]), 2),
    )
    for g, f0, f1, k in outer:
        for m in range(4):
            part = slice(128 * (g + m), 128 * (g + m + 1))
            xs[:, part] = xs[:, part] + (float(W4[k, m]) * f0 + float(W4[k + 1, m]) * f1)

    lax.fori_loop(1, 7, column((2,)), 0)
    lax.fori_loop(0, 2, lambda i, _: column((1, 2))(7 * i, 0), 0)

    for copy in small[3:]:
        copy.wait()
    total = None
    for a in range(3):
        x = xs[:, a * slabs * 128 : (a + 1) * slabs * 128]
        hi, lo = split(x)
        y = jnp.dot(wy[...], jnp.concatenate([hi, lo], 0), preferred_element_type=F32)
        y = y[:24] + y[24:]
        pieces = [y[:, 128 * i : 128 * (i + 1)] for i in range(slabs)]
        hi, lo = split(jnp.concatenate([p[16:24] for p in pieces], 0))
        z = jnp.dot(jnp.concatenate([hi, lo], 1), wz[1 + a], preferred_element_type=F32)
        z = z[:, :128] + z[:, 128:]
        total = z if total is None else total + z
        for i in range(slabs):
            zs[a, i] = pieces[i][:16]

    lane8 = lanes((8, 128))
    taken = []
    for jj in range(6):
        v = None
        for i in range(slabs):
            tap = i - 8 * jj + 25
            if 0 <= tap < 29:
                term = float(C29[tap]) * total[8 * i : 8 * (i + 1)]
                v = term if v is None else v + term
        taken.append(v)
    for g in range(3):
        v = jnp.where(lane8 < 64, taken[2 * g], taken[2 * g + 1])
        csend[g] = jnp.where(lane8 // 32 % 2 == 0, v, roll(v, -1, 0))
    crecv[4, pl.ds(gz, 1), :] = csend[1, 2:3, :]

    def coarse_copy(dx, dy, o):
        slot = 3 * (dx + 1) + dy + 1
        return pltpu.make_async_remote_copy(
            src_ref=csend.at[dx + 1, pl.ds(2 * (dy + 1), 1), :], dst_ref=crecv.at[slot, pl.ds(gz, 1), :],
            send_sem=cs.at[slot], recv_sem=cr.at[slot], device_id=beside(dx, dy, o), device_id_type=MESH)

    def coarse_line(dx, dy):
        slot = 3 * (dx + 1) + dy + 1
        rows = crecv.at[slot] if dx or dy else crecv.at[slot, pl.ds(0, nz - 1), :]
        return pltpu.make_async_remote_copy(
            src_ref=rows, dst_ref=rows, send_sem=cs.at[slot], recv_sem=cr.at[slot],
            device_id=beside(0, 0, 1), device_id_type=MESH)

    def coarse_all(fn):
        for o in ring_order(nz):
            for dx, dy in sorted(sides, key=lambda d: -abs(d[0]) - abs(d[1])):
                if o or dx or dy:
                    fn(dx, dy, o)

    far_done()
    coarse_all(lambda dx, dy, o: if_seen(dx, dy, lambda: coarse_copy(dx, dy, o).start()))

    small[1].wait()

    row16 = lax.broadcasted_iota(jnp.int32, (16, 128), 0)
    lane16 = lanes((16, 128))
    row_g = row16 - 2 + gy * 8
    lane_g = lane16 - (FB + 2) + gz * 16
    in_grid = (row_g >= 0) & (row_g < ny * 8) & (lane_g >= 0) & (lane_g < nz * 16)

    def lap(centre, low, high):
        total = roll(centre, 1, 0) + roll(centre, -1, 0) + roll(centre, 1, 1) + roll(centre, -1, 1)
        if low is not None:
            total = total + low
        if high is not None:
            total = total + high
        return total - 6.0 * centre

    def fine_bend(a, _):
        for j in range(8):
            block = jnp.concatenate([ctl[a, j], jnp.zeros((8, 112), F32)], 1)
            block = jnp.concatenate([block, zero8], 0)
            fw[j + 2] = roll(roll(block, 2, 0), FB + 2, 1)
        zero16 = jnp.zeros((16, 128), F32)
        for j in (0, 1, 10, 11):
            fw[j] = zero16
        first = []
        for j in range(12):
            if j in (0, 11):
                first.append(None)
                continue
            low = fw[j - 1] if 0 < j else None
            high = fw[j + 1] if j < 11 else None
            value = lap(fw[j], low, high)
            p = gx * 8 + j - 2
            ok = in_grid & (p >= 0) & (p < nx * 8)
            first.append(jnp.where(ok, value, 0.0))
        for j in range(12):
            centre = first[j] if first[j] is not None else zero16
            low = first[j - 1] if j > 0 else None
            high = first[j + 1] if j < 11 else None
            e[a, j] = BEND * lap(centre, low, high)
        return 0

    lax.fori_loop(0, 3, fine_bend, 0)

    for a in range(3):
        hi, lo = split(zs[a].reshape(16 * slabs, 128))
        z = jnp.dot(jnp.concatenate([hi, lo], 1), wz[0], preferred_element_type=F32)
        z = z[:, :128] + z[:, 128:]
        for j in range(12):
            v = e[a, j]
            for k in range(5):
                i = 2 * j - 4 + k
                if 0 <= i < slabs:
                    v = v + float(TWO[k]) * z[16 * i : 16 * (i + 1)]
            e[a, j] = v
    for k in (0, 1):
        start(fine_copy, k)

    kx, ky, kz = cctl.shape[1:]
    shape = (ky, kz)
    crow = lax.broadcasted_iota(jnp.int32, (ky, 128), 0)
    clane = lanes((ky, 128))

    def clap(centre, low, high):
        total = jnp.where(crow > 0, roll(centre, 1, 0), 0.0) + jnp.where(crow < ky - 1, roll(centre, -1, 0), 0.0)
        total = total + roll(centre, 1, 1) + roll(centre, -1, 1)
        if low is not None:
            total = total + low
        if high is not None:
            total = total + high
        return jnp.where(clane < kz, total - 6.0 * centre, 0.0)

    def coarse_bend(a, _):
        field = [jnp.concatenate([cctl[a, j], jnp.zeros((ky, 128 - kz), F32)], 1) for j in range(kx)]
        for _level in range(2):
            field = [clap(field[j], field[j - 1] if j else None, field[j + 1] if j < kx - 1 else None)
                     for j in range(kx)]
        for j in range(kx):
            coarse_out[a, j] = BEND * field[j][:, :kz]
        return 0

    lax.fori_loop(0, 3, coarse_bend, 0)

    for k in (0, 1):
        sent(fine_copy, k)
        arrived(fine_copy, k)
    for a in range(3):
        for j in range(8):
            v = e[a, j + 2]
            if j < 2:
                v = v + fxr[0, a, j]
            if j >= 6:
                v = v + fxr[1, a, j - 6]
            e[a, j + 2] = v
            fys[0, 8 * a + j] = v[0:2]
            fys[1, 8 * a + j] = v[10:12]
    for k in (2, 3):
        start(fine_copy, k)

    for dx, dy in sides:
        if_seen(-dx, -dy, lambda: coarse_line(dx, dy).wait_recv())
    line = crecv[0]
    for i in range(1, 9):
        line = line + crecv[i]
    line = pltpu.roll(line, 0, 1, stride=4, stride_axis=0)
    place = lane8 % 32 + 2 - 4 * lax.broadcasted_iota(jnp.int32, (8, 128), 0)
    for a in range(3):
        piece = jnp.where((place >= 0) & (place < 8), roll(line, -2 - 8 * a, 1), 0.0)
        xg[gx, a, pl.ds(gy, 1), :] = jnp.sum(piece, axis=0, keepdims=True)

    def gather_copy(ox, oy, sx, sy):
        slot = xg.at[sx, :, pl.ds(sy, 1), :]
        return pltpu.make_async_remote_copy(
            src_ref=slot, dst_ref=slot, send_sem=gs, recv_sem=gr,
            device_id=in_plane(ox, oy), device_id_type=MESH)

    def gather_plane():
        return pltpu.make_async_remote_copy(
            src_ref=total_rows, dst_ref=total_rows, send_sem=gs, recv_sem=gr,
            device_id=in_plane(0, 1), device_id_type=MESH)

    for ox, oy in plane:
        gather_copy(ox, oy, gx, gy).start()

    for k in (2, 3):
        arrived(fine_copy, k)
    pack0 = zero8
    pack1 = zero8
    zero4 = jnp.zeros((4, 128), F32)
    for a in range(3):
        for j in range(8):
            s = 8 * a + j
            v = e[a, j + 2]
            edges = jnp.concatenate([fyr[0, s], zero4, fyr[1, s]], 0)
            v = roll(v, -2, 0)[0:8] + edges
            e[a, j + 2, 0:8, :] = v
            turned = roll(v, 2 * s - FB, 1)
            pack0 = jnp.where(lane8 // 2 == s, turned, pack0)
            pack1 = jnp.where(lane8 // 2 == s + 9, turned, pack1)
    fzs[0] = pack0
    fzs[1] = pack1
    for k in (4, 5):
        start(fine_copy, k)

    for k in (4, 5):
        arrived(fine_copy, k)
    p0 = fzr[0]
    p1 = fzr[1]
    for a in range(3):
        for j in range(8):
            s = 8 * a + j
            v = roll(e[a, j + 2, 0:8, :], -(FB + 2), 1)
            v = v + jnp.where(lane8 < 2, roll(p0, -(18 + 2 * s), 1), 0.0)
            v = v + jnp.where((lane8 >= 14) & (lane8 < 16), roll(p1, 14 - 2 * s, 1), 0.0)
            fine_out[a, j] = v[:, :16]

    gather_plane().wait_recv()
    for g in range(nx):
        for a in range(3):
            rows = xg[g, a]
            for p in range(2):
                for q in range(2):
                    mix[a, 2 * g + p, pl.ds(q, ny, stride=2), :] = roll(rows, -(64 * p + 32 * q), 1)
    for a in range(3):
        for j in range(kx):
            coarse_out[a, j] = coarse_out[a, j] + mix[a, j][:, :kz]

    for k in range(6):
        sent(halo, k)
    for k in range(2, 6):
        sent(fine_copy, k)
    for dx, dy in sides:
        if_seen(dx, dy, lambda: coarse_line(dx, dy).wait_send())
    gather_plane().wait_send()


def write_out(fine, coarse, fine_out, coarse_out, sem):
    copies = [pltpu.make_async_copy(coarse, coarse_out, sem.at[0]), pltpu.make_async_copy(fine, fine_out, sem.at[1])]
    for copy in copies:
        copy.start()
    for copy in copies:
        copy.wait()


def per_device(dims, warped_image, fixed_image, fine_control, coarse_control):
    sx, sy, sz = warped_image.shape
    kx, ky, kz = coarse_control.shape[1:]
    nx, ny, nz = dims
    slabs = 19
    vmem = pl.BlockSpec(memory_space=pltpu.VMEM)
    hbm = pl.BlockSpec(memory_space=pltpu.HBM)
    v = lambda *shape: pltpu.VMEM(shape, F32)
    h = lambda *shape: pltpu.VMEM(shape, BF16)
    out = lambda *shape: jax.ShapeDtypeStruct(shape, F32)
    dma = pltpu.SemaphoreType.DMA
    flag = pltpu.SemaphoreType.REGULAR
    far = lambda x: pltpu.with_memory_space_constraint(jnp.asarray(x), pltpu.HBM)
    results = pl.pallas_call(
        lambda *refs: gradient(dims, *refs),
        out_shape=(out(*fine_control.shape), out(*coarse_control.shape)),
        in_specs=[hbm] * 8,
        out_specs=(vmem, vmem),
        scratch_shapes=[
            v(*fine_control.shape), v(*coarse_control.shape), h(2 * sz, sz), h(256, sz), h(48, 2 * sy),
            h(4, 2 * sz, 256), dma((6,)), v(sx, sy, sz), v(sx, sy, sz), v(sx + 4, sy + 16, sz), v(sx, sy, sz),
            v(sx, sy, sz), v(2, sy, 128), v(3, 12, 16, 128),
            v(2, 2, sy, sz), v(2, sx, 2, sz), v(2, sx, 2, sz), v(2, sy, 128), v(2, 2, sy, 128), v(12, 16, 128),
            v(sy, 3 * slabs * 128), v(3, slabs, 16, 128), v(3, 8, 128), v(9, nz, 128),
            v(nx, 3, ny, 128), v(3 * (nx * ny - 1), 128), v(3, kx, ky, 128),
            v(2, 3, 2, 16, 128), v(2, 24, 2, 128), v(2, 24, 2, 128), v(2, 8, 128), v(2, 8, 128),
            dma((2, 8)), dma((6,)), dma((6,)), dma((9,)), dma((9,)), dma, dma, dma((6,)), dma((6,)), flag, flag,
        ],
        compiler_params=pltpu.CompilerParams(collective_id=0, has_side_effects=True, vmem_limit_bytes=48 << 20),
        name="gradient",
    )(far(warped_image), far(fixed_image), far(fine_control), far(coarse_control), far(d_matrix(sz)),
      far(h_matrix(sz)), far(y_matrix(sy)), far(z_matrices(sz)))
    return pl.pallas_call(
        write_out,
        out_shape=(out(*fine_control.shape), out(*coarse_control.shape)),
        in_specs=[vmem] * 2,
        out_specs=(hbm, hbm),
        scratch_shapes=[dma((2,))],
        compiler_params=pltpu.CompilerParams(vmem_limit_bytes=1 << 20),
        name="write_out",
    )(*results)


def solution(mesh):
    dims = tuple(mesh.shape[a] for a in ("gx", "gy", "gz"))
    in_specs = (P("gx", "gy", "gz"), P("gx", "gy", "gz"), P(None, "gx", "gy", "gz"), P())
    out_specs = (P(None, "gx", "gy", "gz"), P())
    return jax.shard_map(
        lambda *args: per_device(dims, *args), mesh=mesh, in_specs=in_specs, out_specs=out_specs, check_vma=False
    )
```

```python
import itertools

import jax
import jax.numpy as jnp
import numpy as np
from jax import lax
from jax.experimental import pallas as pl
from jax.experimental.pallas import tpu as pltpu
from jax.sharding import PartitionSpec as P

SPF = 8
SPC = 32
BEND = 0.01
FB = 0
MESH = pl.DeviceIdType.MESH
F32 = jnp.float32
BF16 = jnp.bfloat16


def beta(t):
    m = np.abs(t)
    r = 2.0 - m
    return np.where(m < 1.0, 2.0 / 3.0 - m * m + 0.5 * m**3, np.where(m < 2.0, r**3 / 6.0, 0.0))


def basis(voxels, points, spacing, first):
    v = np.arange(voxels)[:, None] + 0.5
    c = (np.arange(points)[None, :] + first) * spacing + 0.5 * spacing
    return beta((v - c) / spacing)


def halves(w):
    hi = np.asarray(w, np.float32).astype(jnp.bfloat16)
    lo = (np.asarray(w, np.float64) - hi.astype(np.float64)).astype(np.float32).astype(jnp.bfloat16)
    return hi, lo


W4 = beta((np.arange(4)[:, None] + 4.5 - 4.0 * np.arange(4)[None, :]) / 4.0) / 24.0
TWO = np.array([1.0, 4.0, 6.0, 4.0, 1.0]) / 8.0


def spread(c, step):
    out = np.zeros((len(c) - 1) * step + 1)
    out[::step] = c
    return out


C29 = np.convolve(np.convolve(TWO, spread(TWO, 2)), spread(TWO, 4))


def y_matrix(sy):
    rows = np.zeros((24, sy))
    rows[:12] = basis(sy, 12, SPF, -2).T * SPF**-1.5
    rows[16:22] = basis(sy, 6, SPC, -2).T * SPC**-1.5
    hi, lo = halves(rows)
    return np.concatenate([np.concatenate([hi, hi], 1), np.concatenate([lo, lo], 1)], 0)


def stacked(cols):
    hi, lo = halves(cols)
    half = np.concatenate([hi, lo], 1)
    return np.concatenate([half, half], 0)


def z_matrices(sz):
    fine = np.zeros((sz, 128))
    fine[:, FB : FB + 20] = basis(sz, 20, SPF, -2)
    out = [stacked(fine)]
    for a in range(3):
        cols = np.zeros((sz, 128))
        for piece in range(4):
            first = 32 * piece + 8 * a
            cols[:, first : first + 8] = basis(sz, 8, SPC, -2)
        out.append(stacked(cols))
    return np.stack(out)


def d_matrix(sz):
    d = np.zeros((sz, sz), np.float32)
    for shift, value in ((-2, 1.0), (-1, -8.0), (1, 8.0), (2, -1.0)):
        for v in range(sz):
            if 0 <= v + shift < sz:
                d[v + shift, v] = value
    return np.concatenate([d, d], 0).astype(jnp.bfloat16)


def h_matrix(sz):
    h = np.zeros((128, sz), np.float32)
    for lane in range(128):
        h[lane, (sz - 2, sz - 1, 0, 1)[lane % 4]] = 1.0
    return np.concatenate([h, h], 0).astype(jnp.bfloat16)


def split(x):
    hi = x.astype(BF16)
    return hi, (x - hi.astype(F32)).astype(BF16)


def lanes(shape):
    return lax.broadcasted_iota(jnp.int32, shape, len(shape) - 1)


def roll(x, shift, axis):
    return pltpu.roll(x, shift % x.shape[axis] if isinstance(shift, int) else shift, axis)


class Place:
    def __init__(self, dims):
        self.dims = dims
        self.pos = tuple(lax.axis_index(a) for a in ("gx", "gy", "gz"))
        self.has = [{-1: p > 0, 1: p < n - 1} for p, n in zip(self.pos, dims)]

    def exists(self, d):
        cond = None
        for i in range(3):
            if d[i]:
                one = self.has[i][d[i]]
                cond = one if cond is None else jnp.logical_and(cond, one)
        return cond

    def at(self, d):
        return tuple(self.pos[i] + d[i] for i in range(3))

    def ring(self, axis, o):
        t = lax.rem(self.pos[axis] + o, self.dims[axis])
        return tuple(t if i == axis else self.pos[i] for i in range(3)), t

    def seen(self, dx, dy):
        return self.exists((dx, dy, 0))

    def if_seen(self, dx, dy, fn):
        if dx or dy:
            pl.when(self.seen(dx, dy))(fn)
        else:
            fn()

    def beside(self, dx, dy, o):
        gx, gy, gz = self.pos
        return (gx + dx, gy + dy, lax.rem(gz + o, self.dims[2]))

    def start(self, make, k):
        d, copy = make(k)
        pl.when(self.exists(d))(lambda: copy.start())

    def sent(self, make, k):
        d, copy = make(k)
        pl.when(self.exists(d))(lambda: copy.wait_send())

    def arrived(self, make, k):
        d, copy = make(k)
        pl.when(self.exists([-v for v in d]))(lambda: copy.wait_recv())


def ring_order(n):
    return sorted(range(n), key=lambda o: -min(o, n - o))


SIDES = list(itertools.product((-1, 0, 1), repeat=2))


def gradient(dims, w_hbm, f_hbm, ctl_h, cctl_h, dz_h, h_h, wy_h, wz_h, fine_out, coarse_out,
             ctl, cctl, dz_w, h_w, wy, wz, small_sem, wb, fb, sp, diff, dzb, cz, e,
             hxr, hys, hyr, hzs, hzr, fw, xs, zs, csend, crecv, xg, total_rows, mix,
             fxr, fys, fyr, fzs, fzr, img_sem, hs, hr, cs, cr, gs, gr, fs, fr, near_sem, far_sem):
    nx, ny, nz = dims
    here = Place(dims)
    pos = here.pos
    gx, gy, gz = pos
    has, exists, at, ring, seen, if_seen, beside = (
        here.has, here.exists, here.at, here.ring, here.seen, here.if_seen, here.beside)
    start, sent, arrived = here.start, here.sent, here.arrived
    sides = SIDES
    zero8 = jnp.zeros((8, 128), F32)
    lane64 = lanes((64, 128))

    bar = pltpu.get_barrier_semaphore()
    odd = lax.rem(gx + gy + gz, 2) == 1
    even = jnp.logical_not(odd)
    faces = [tuple(side if i == axis else 0 for i in range(3)) for axis in range(3) for side in (-1, 1)]
    count = sum(has[axis][side].astype(jnp.int32) for axis in range(3) for side in (-1, 1))

    def greet_faces(sem):
        for d in faces:
            pl.when(exists(d))(lambda: pl.semaphore_signal(sem, inc=1, device_id=at(d), device_id_type=MESH))

    @pl.when(even)
    def _():
        greet_faces(bar)

    def near_done():
        @pl.when(odd)
        def _():
            pl.semaphore_wait(bar, count)
            greet_faces(near_sem)

        @pl.when(even)
        def _():
            pl.semaphore_wait(near_sem, count)

    chip = gx // 2
    lean = 2 * lax.rem(gx, 2) - 1
    next_chip = chip + lean
    has_next = (next_chip >= 0) & (next_chip < nx // 2)
    partner = (gx - lean, gy, gz)

    same = lax.rem(gy + gz, 2)
    parity = (same, 1 - same)
    line_z = [lax.rem(gz + o, nz) for o in range(nz)]
    line_y = [lax.rem(gy + o, ny) for o in range(ny)]

    def greet_chip(first, y, z, steps):
        device = (first + parity[steps % 2], y, z)
        pl.semaphore_signal(bar, inc=1, device_id=device, device_id_type=MESH)

    def far_greetings():
        for dy in (-1, 1, 0):
            def line(dy=dy):
                for o in ring_order(nz)[:-1]:
                    greet_chip(2 * chip, gy + dy, line_z[o], dy + o)

                @pl.when(has_next)
                def _():
                    for o in ring_order(nz)[:-1]:
                        greet_chip(2 * next_chip, gy + dy, line_z[o], dy + o)
            if_seen(0, dy, line)
        for oc in range(nx // 2):
            first = 2 * lax.rem(chip + oc, nx // 2)
            for oy in ring_order(ny):
                def one(first=first, oy=oy):
                    greet_chip(first, line_y[oy], gz, oy)
                if oc or oy:
                    one()
                else:
                    pl.when(odd)(one)

    def far_done():
        wide_x = 4 - (chip == 0).astype(jnp.int32) - (chip == nx // 2 - 1).astype(jnp.int32)
        wide_y = 1 + has[1][-1].astype(jnp.int32) + has[1][1].astype(jnp.int32)

        @pl.when(even)
        def _():
            pl.semaphore_wait(bar, wide_x * wide_y * (nz - 1) + nx * ny - 1)
            pl.semaphore_signal(far_sem, inc=1, device_id=partner, device_id_type=MESH)

        @pl.when(odd)
        def _():
            pl.semaphore_wait(far_sem, 1)

    chunks = 8
    planes = 8
    for c in range(chunks):
        part = pl.ds(c * planes, planes)
        pltpu.make_async_copy(w_hbm.at[part], wb.at[part], img_sem.at[0, c]).start()
        pltpu.make_async_copy(f_hbm.at[part], fb.at[part], img_sem.at[1, c]).start()
    small = [pltpu.make_async_copy(src, dst, small_sem.at[i]) for i, (src, dst) in enumerate(
        ((dz_h, dz_w), (ctl_h, ctl), (h_h, h_w), (wy_h, wy), (wz_h, wz), (cctl_h, cctl)))]
    for copy in small:
        copy.start()
    far_greetings()

    for side, d in ((0, -1), (1, 1)):
        @pl.when(jnp.logical_not(has[0][d]))
        def _(side=side):
            hxr[side] = jnp.zeros(hxr.shape[1:], F32)

        @pl.when(jnp.logical_not(has[1][d]))
        def _(side=side):
            hyr[side] = jnp.zeros(hyr.shape[1:], F32)

        @pl.when(jnp.logical_not(has[2][d]))
        def _(side=side):
            hzr[side] = jnp.zeros(hzr.shape[1:], F32)

    hzs[...] = jnp.zeros(hzs.shape, F32)
    for first in (0, 66):
        sp[first : first + 2, 8:72, :] = jnp.zeros((2, 64, 128), F32)

    def halo(k):
        axis, side = k // 2, k % 2
        d = [0, 0, 0]
        d[axis] = 2 * side - 1
        if axis == 0:
            src = sp.at[pl.ds(2 if side == 0 else 64, 2), pl.ds(8, 64), :]
            dst = hxr.at[1 - side]
        elif axis == 1:
            src, dst = hys.at[side], hyr.at[1 - side]
        else:
            src, dst = hzs, hzr.at[1 - side]
        return d, pltpu.make_async_remote_copy(
            src_ref=src, dst_ref=dst, send_sem=hs.at[k], recv_sem=hr.at[k],
            device_id=at(d), device_id_type=MESH)

    def part_of(k, c):
        axis, side = k // 2, k % 2
        if axis == 0:
            return halo(k)
        d = [0, 0, 0]
        d[axis] = 2 * side - 1
        if axis == 1:
            part = pl.ds(c * planes, planes)
            src, dst = hys.at[side, part], hyr.at[1 - side, part]
        else:
            src, dst = hzs.at[c // 4], hzr.at[1 - side, c // 4]
        return d, pltpu.make_async_remote_copy(
            src_ref=src, dst_ref=dst, send_sem=hs.at[k], recv_sem=hr.at[k],
            device_id=at(d), device_id_type=MESH)

    def send(k, c):
        d, copy = part_of(k, c)
        pl.when(exists(d))(lambda: copy.start())


    def sum_chunk(c, _):
        base = c * planes
        part = pl.ds(base, planes)
        pltpu.make_async_copy(w_hbm.at[part], wb.at[part], img_sem.at[0, c]).wait()
        pltpu.make_async_copy(f_hbm.at[part], fb.at[part], img_sem.at[1, c]).wait()
        h = c // 4
        group = lane64 // 4 - 8 * (c % 4)
        packed = hzs[h]
        for j in range(planes):
            w = wb[base + j]
            f = fb[base + j]
            s = w + f
            diff[base + j] = w - f
            sp[base + j + 2, 8:72, :] = s
            hys[0, base + j] = s[0:2]
            hys[1, base + j] = s[62:64]
            turned = roll(s, 32 * (c % 4) + 4 * j + 2, 1)
            packed = jnp.where(group == j, turned, packed)
        hzs[h] = packed
        return 0

    for c in range(chunks):
        sum_chunk(c, 0)
        if c == 3:
            near_done()
            send(0, 0)
            for k in (2, 3):
                for early in range(3):
                    send(k, early)
        if c >= 3:
            for k in (2, 3):
                send(k, c)
        if c % 4 == 3:
            for k in (4, 5):
                send(k, c)
    send(1, 0)
    small[0].wait()

    def dz_chunk(c, _):
        base = pl.multiple_of(c * 16, 16)
        for half in range(2):
            parts = [jnp.concatenate(split(sp[base + 8 * half + j + 2, 8:72, :]), 1) for j in range(8)]
            out = jnp.dot(jnp.concatenate(parts, 0), dz_w[...], preferred_element_type=F32)
            for j in range(8):
                dzb[base + 8 * half + j] = out[64 * j : 64 * (j + 1)]
        return 0

    lax.fori_loop(0, 4, dz_chunk, 0, unroll=True)

    groups = 16
    slabs = groups + 3
    even4 = 0.5 * (W4 + W4[::-1])
    odd4 = 0.5 * (W4 - W4[::-1])

    def column(axes):
        per = 4

        def one(yt, _):
            r0 = pl.multiple_of(8 * yt, 8)

            def put(a, g, value):
                xs[pl.ds(r0, 8), pl.ds(pl.multiple_of((a * slabs + g) * 128, 128), 128)] = value

            def some(gg, acc):
                acc = [list(row) for row in acc]
                x0 = 4 * per * gg
                if 0 in axes:
                    c = [sp[x0 + i, pl.ds(r0 + 8, 8), :] for i in range(4 * per + 4)]
                for sub in range(per):
                    force = [[] for _ in axes]
                    for k in range(4):
                        i = 4 * sub + k
                        dv = diff[x0 + i, pl.ds(r0, 8), :]
                        for n, a in enumerate(axes):
                            if a == 0:
                                s = (c[i] - c[i + 4]) + 8.0 * (c[i + 3] - c[i + 1])
                            elif a == 1:
                                ym2, ym1, yp1, yp2 = (
                                    sp[x0 + i + 2, pl.ds(r0 + o, 8), :] for o in (6, 7, 9, 10))
                                s = (ym2 - yp2) + 8.0 * (yp1 - ym1)
                            else:
                                s = dzb[x0 + i, pl.ds(r0, 8), :]
                            force[n].append(dv * s)
                    for n, a in enumerate(axes):
                        f = force[n]
                        e0, e1, o0, o1 = f[0] + f[3], f[1] + f[2], f[0] - f[3], f[1] - f[2]
                        for m in range(2):
                            both = float(even4[0, m]) * e0 + float(even4[1, m]) * e1
                            diff4 = float(odd4[0, m]) * o0 + float(odd4[1, m]) * o1
                            acc[n][m] = acc[n][m] + (both + diff4)
                            acc[n][3 - m] = acc[n][3 - m] + (both - diff4)
                        put(a, per * gg + sub, acc[n][0])
                        acc[n] = [acc[n][1], acc[n][2], acc[n][3], zero8]
                return tuple(tuple(row) for row in acc)

            acc = lax.fori_loop(0, groups // per, some, tuple(tuple(zero8 for _ in range(4)) for _ in axes))
            for n, a in enumerate(axes):
                for m in range(3):
                    put(a, groups + m, acc[n][m])
            return 0

        return one

    lax.fori_loop(1, 7, column((0, 1)), 0)
    lax.fori_loop(0, 2, lambda i, _: column((0,))(7 * i, 0), 0)

    for side, d in ((0, -1), (1, 1)):
        for axis, ref in enumerate((fxr, fyr, fzr)):
            @pl.when(jnp.logical_not(has[axis][d]))
            def _(side=side, ref=ref):
                ref[side] = jnp.zeros(ref.shape[1:], F32)
    for dx, dy in sides:
        if dx or dy:
            @pl.when(jnp.logical_not(seen(-dx, -dy)))
            def _(dx=dx, dy=dy):
                crecv[3 * (dx + 1) + dy + 1] = zero8

    for k in range(6):
        arrived(halo, k)

    def place_y(x, _):
        sp[x + 2, 6:8, :] = hyr[0, x]
        sp[x + 2, 72:74, :] = hyr[1, x]
        return 0

    lax.fori_loop(0, 64, place_y, 0, unroll=8)

    m4 = lane64 % 4
    for h in range(2):
        u = jnp.where(m4 < 2, hzr[0, h], hzr[1, h])
        a_part = jnp.where(m4 < 2, -roll(u, -2, 1), roll(u, 2, 1))
        b_part = jnp.where(m4 == 1, 8.0 * roll(u, -1, 1), jnp.where(m4 == 2, -8.0 * roll(u, 1, 1), 0.0))
        cz[h] = a_part + b_part
    plane = sorted(((ox, oy) for ox in range(nx) for oy in range(ny) if ox or oy),
                   key=lambda o: -min(o[1], ny - o[1]) - 0.5 * min(o[0], nx - o[0]))

    def in_plane(ox, oy):
        return (lax.rem(gx + ox, nx), lax.rem(gy + oy, ny), gz)

    def fine_copy(k):
        axis, side = k // 2, k % 2
        d = [0, 0, 0]
        d[axis] = 2 * side - 1
        if axis == 0:
            src, dst = e.at[:, pl.ds(10 * side, 2)], fxr.at[1 - side]
        elif axis == 1:
            src, dst = fys.at[side], fyr.at[1 - side]
        else:
            src, dst = fzs.at[side], fzr.at[1 - side]
        return d, pltpu.make_async_remote_copy(
            src_ref=src, dst_ref=dst, send_sem=fs.at[k], recv_sem=fr.at[k],
            device_id=at(d), device_id_type=MESH)

    small[2].wait()

    def z_fix(c, _):
        base = pl.multiple_of(c * 16, 16)
        layer = cz[c // 2]
        for half in range(2):
            group = lane64 // 4 - 16 * lax.rem(c, 2) - 8 * half
            parts = [jnp.concatenate(split(jnp.where(group == j, layer, 0.0)), 1) for j in range(8)]
            out = jnp.dot(jnp.concatenate(parts, 0), h_w[...], preferred_element_type=F32)
            for j in range(8):
                dzb[base + 8 * half + j] = dzb[base + 8 * half + j] + out[64 * j : 64 * (j + 1)]
        return 0

    lax.fori_loop(0, 4, z_fix, 0, unroll=True)

    outer = (
        (0, diff[0] * (hxr[0, 0] - 8.0 * hxr[0, 1]), diff[1] * hxr[0, 1], 0),
        (groups - 1, diff[62] * -hxr[1, 0], diff[63] * (8.0 * hxr[1, 0] - hxr[1, 1]), 2),
    )
    for g, f0, f1, k in outer:
        for m in range(4):
            part = slice(128 * (g + m), 128 * (g + m + 1))
            xs[:, part] = xs[:, part] + (float(W4[k, m]) * f0 + float(W4[k + 1, m]) * f1)

    lax.fori_loop(1, 7, column((2,)), 0)
    lax.fori_loop(0, 2, lambda i, _: column((1, 2))(7 * i, 0), 0)

    for copy in small[3:]:
        copy.wait()
    total = None
    for a in range(3):
        x = xs[:, a * slabs * 128 : (a + 1) * slabs * 128]
        hi, lo = split(x)
        y = jnp.dot(wy[...], jnp.concatenate([hi, lo], 0), preferred_element_type=F32)
        y = y[:24] + y[24:]
        pieces = [y[:, 128 * i : 128 * (i + 1)] for i in range(slabs)]
        hi, lo = split(jnp.concatenate([p[16:24] for p in pieces], 0))
        z = jnp.dot(jnp.concatenate([hi, lo], 1), wz[1 + a], preferred_element_type=F32)
        z = z[:, :128] + z[:, 128:]
        total = z if total is None else total + z
        for i in range(slabs):
            zs[a, i] = pieces[i][:16]

    lane8 = lanes((8, 128))
    taken = []
    for jj in range(6):
        v = None
        for i in range(slabs):
            tap = i - 8 * jj + 25
            if 0 <= tap < 29:
                term = float(C29[tap]) * total[8 * i : 8 * (i + 1)]
                v = term if v is None else v + term
        taken.append(v)
    for g in range(3):
        v = jnp.where(lane8 < 64, taken[2 * g], taken[2 * g + 1])
        csend[g] = jnp.where(lane8 // 32 % 2 == 0, v, roll(v, -1, 0))
    crecv[4, pl.ds(gz, 1), :] = csend[1, 2:3, :]

    def coarse_copy(dx, dy, o):
        slot = 3 * (dx + 1) + dy + 1
        return pltpu.make_async_remote_copy(
            src_ref=csend.at[dx + 1, pl.ds(2 * (dy + 1), 1), :], dst_ref=crecv.at[slot, pl.ds(gz, 1), :],
            send_sem=cs.at[slot], recv_sem=cr.at[slot], device_id=beside(dx, dy, o), device_id_type=MESH)

    def coarse_line(dx, dy):
        slot = 3 * (dx + 1) + dy + 1
        rows = crecv.at[slot] if dx or dy else crecv.at[slot, pl.ds(0, nz - 1), :]
        return pltpu.make_async_remote_copy(
            src_ref=rows, dst_ref=rows, send_sem=cs.at[slot], recv_sem=cr.at[slot],
            device_id=beside(0, 0, 1), device_id_type=MESH)

    def coarse_all(fn):
        for o in ring_order(nz):
            for dx, dy in sorted(sides, key=lambda d: -abs(d[0]) - abs(d[1])):
                if o or dx or dy:
                    fn(dx, dy, o)

    far_done()
    coarse_all(lambda dx, dy, o: if_seen(dx, dy, lambda: coarse_copy(dx, dy, o).start()))

    small[1].wait()

    row16 = lax.broadcasted_iota(jnp.int32, (16, 128), 0)
    lane16 = lanes((16, 128))
    row_g = row16 - 2 + gy * 8
    lane_g = lane16 - (FB + 2) + gz * 16
    in_grid = (row_g >= 0) & (row_g < ny * 8) & (lane_g >= 0) & (lane_g < nz * 16)

    def lap(centre, low, high):
        total = roll(centre, 1, 0) + roll(centre, -1, 0) + roll(centre, 1, 1) + roll(centre, -1, 1)
        if low is not None:
            total = total + low
        if high is not None:
            total = total + high
        return total - 6.0 * centre

    def fine_bend(a, _):
        for j in range(8):
            block = jnp.concatenate([ctl[a, j], jnp.zeros((8, 112), F32)], 1)
            block = jnp.concatenate([block, zero8], 0)
            fw[j + 2] = roll(roll(block, 2, 0), FB + 2, 1)
        zero16 = jnp.zeros((16, 128), F32)
        for j in (0, 1, 10, 11):
            fw[j] = zero16
        first = []
        for j in range(12):
            if j in (0, 11):
                first.append(None)
                continue
            low = fw[j - 1] if 0 < j else None
            high = fw[j + 1] if j < 11 else None
            value = lap(fw[j], low, high)
            p = gx * 8 + j - 2
            ok = in_grid & (p >= 0) & (p < nx * 8)
            first.append(jnp.where(ok, value, 0.0))
        for j in range(12):
            centre = first[j] if first[j] is not None else zero16
            low = first[j - 1] if j > 0 else None
            high = first[j + 1] if j < 11 else None
            e[a, j] = BEND * lap(centre, low, high)
        return 0

    lax.fori_loop(0, 3, fine_bend, 0)

    for a in range(3):
        hi, lo = split(zs[a].reshape(16 * slabs, 128))
        z = jnp.dot(jnp.concatenate([hi, lo], 1), wz[0], preferred_element_type=F32)
        z = z[:, :128] + z[:, 128:]
        for j in range(12):
            v = e[a, j]
            for k in range(5):
                i = 2 * j - 4 + k
                if 0 <= i < slabs:
                    v = v + float(TWO[k]) * z[16 * i : 16 * (i + 1)]
            e[a, j] = v
    for k in (0, 1):
        start(fine_copy, k)

    kx, ky, kz = cctl.shape[1:]
    shape = (ky, kz)
    crow = lax.broadcasted_iota(jnp.int32, (ky, 128), 0)
    clane = lanes((ky, 128))

    def clap(centre, low, high):
        total = jnp.where(crow > 0, roll(centre, 1, 0), 0.0) + jnp.where(crow < ky - 1, roll(centre, -1, 0), 0.0)
        total = total + roll(centre, 1, 1) + roll(centre, -1, 1)
        if low is not None:
            total = total + low
        if high is not None:
            total = total + high
        return jnp.where(clane < kz, total - 6.0 * centre, 0.0)

    def coarse_bend(a, _):
        field = [jnp.concatenate([cctl[a, j], jnp.zeros((ky, 128 - kz), F32)], 1) for j in range(kx)]
        for _level in range(2):
            field = [clap(field[j], field[j - 1] if j else None, field[j + 1] if j < kx - 1 else None)
                     for j in range(kx)]
        for j in range(kx):
            coarse_out[a, j] = BEND * field[j][:, :kz]
        return 0

    lax.fori_loop(0, 3, coarse_bend, 0)

    for dx, dy in sides:
        if_seen(-dx, -dy, lambda: coarse_line(dx, dy).wait_recv())
    line = crecv[0]
    for i in range(1, 9):
        line = line + crecv[i]
    line = pltpu.roll(line, 0, 1, stride=4, stride_axis=0)
    place = lane8 % 32 + 2 - 4 * lax.broadcasted_iota(jnp.int32, (8, 128), 0)
    for a in range(3):
        piece = jnp.where((place >= 0) & (place < 8), roll(line, -2 - 8 * a, 1), 0.0)
        xg[gx, a, pl.ds(gy, 1), :] = jnp.sum(piece, axis=0, keepdims=True)

    def gather_copy(ox, oy, sx, sy):
        slot = xg.at[sx, :, pl.ds(sy, 1), :]
        return pltpu.make_async_remote_copy(
            src_ref=slot, dst_ref=slot, send_sem=gs, recv_sem=gr,
            device_id=in_plane(ox, oy), device_id_type=MESH)

    def gather_plane():
        return pltpu.make_async_remote_copy(
            src_ref=total_rows, dst_ref=total_rows, send_sem=gs, recv_sem=gr,
            device_id=in_plane(0, 1), device_id_type=MESH)

    for ox, oy in plane:
        gather_copy(ox, oy, gx, gy).start()

    for k in (0, 1):
        sent(fine_copy, k)
        arrived(fine_copy, k)
    for a in range(3):
        for j in range(8):
            v = e[a, j + 2]
            if j < 2:
                v = v + fxr[0, a, j]
            if j >= 6:
                v = v + fxr[1, a, j - 6]
            e[a, j + 2] = v
            fys[0, 8 * a + j] = v[0:2]
            fys[1, 8 * a + j] = v[10:12]
    for k in (2, 3):
        start(fine_copy, k)

    for k in (2, 3):
        arrived(fine_copy, k)
    pack0 = zero8
    pack1 = zero8
    zero4 = jnp.zeros((4, 128), F32)
    for a in range(3):
        for j in range(8):
            s = 8 * a + j
            v = e[a, j + 2]
            edges = jnp.concatenate([fyr[0, s], zero4, fyr[1, s]], 0)
            v = roll(v, -2, 0)[0:8] + edges
            e[a, j + 2, 0:8, :] = v
            turned = roll(v, 2 * s - FB, 1)
            pack0 = jnp.where(lane8 // 2 == s, turned, pack0)
            pack1 = jnp.where(lane8 // 2 == s + 9, turned, pack1)
    fzs[0] = pack0
    fzs[1] = pack1
    for k in (4, 5):
        start(fine_copy, k)

    for k in (4, 5):
        arrived(fine_copy, k)
    p0 = fzr[0]
    p1 = fzr[1]
    for a in range(3):
        for j in range(8):
            s = 8 * a + j
            v = roll(e[a, j + 2, 0:8, :], -(FB + 2), 1)
            v = v + jnp.where(lane8 < 2, roll(p0, -(18 + 2 * s), 1), 0.0)
            v = v + jnp.where((lane8 >= 14) & (lane8 < 16), roll(p1, 14 - 2 * s, 1), 0.0)
            fine_out[a, j] = v[:, :16]

    gather_plane().wait_recv()
    for g in range(nx):
        for a in range(3):
            rows = xg[g, a]
            for p in range(2):
                for q in range(2):
                    mix[a, 2 * g + p, pl.ds(q, ny, stride=2), :] = roll(rows, -(64 * p + 32 * q), 1)
    for a in range(3):
        for j in range(kx):
            coarse_out[a, j] = coarse_out[a, j] + mix[a, j][:, :kz]

    for k in range(6):
        sent(halo, k)
    for k in range(2, 6):
        sent(fine_copy, k)
    for dx, dy in sides:
        if_seen(dx, dy, lambda: coarse_line(dx, dy).wait_send())
    gather_plane().wait_send()


def write_out(fine, coarse, fine_out, coarse_out, sem):
    copies = [pltpu.make_async_copy(coarse, coarse_out, sem.at[0]), pltpu.make_async_copy(fine, fine_out, sem.at[1])]
    for copy in copies:
        copy.start()
    for copy in copies:
        copy.wait()


def per_device(dims, warped_image, fixed_image, fine_control, coarse_control):
    sx, sy, sz = warped_image.shape
    kx, ky, kz = coarse_control.shape[1:]
    nx, ny, nz = dims
    slabs = 19
    vmem = pl.BlockSpec(memory_space=pltpu.VMEM)
    hbm = pl.BlockSpec(memory_space=pltpu.HBM)
    v = lambda *shape: pltpu.VMEM(shape, F32)
    h = lambda *shape: pltpu.VMEM(shape, BF16)
    out = lambda *shape: jax.ShapeDtypeStruct(shape, F32)
    dma = pltpu.SemaphoreType.DMA
    flag = pltpu.SemaphoreType.REGULAR
    far = lambda x: pltpu.with_memory_space_constraint(jnp.asarray(x), pltpu.HBM)
    results = pl.pallas_call(
        lambda *refs: gradient(dims, *refs),
        out_shape=(out(*fine_control.shape), out(*coarse_control.shape)),
        in_specs=[hbm] * 8,
        out_specs=(vmem, vmem),
        scratch_shapes=[
            v(*fine_control.shape), v(*coarse_control.shape), h(2 * sz, sz), h(256, sz), h(48, 2 * sy),
            h(4, 2 * sz, 256), dma((6,)), v(sx, sy, sz), v(sx, sy, sz), v(sx + 4, sy + 16, sz), v(sx, sy, sz),
            v(sx, sy, sz), v(2, sy, 128), v(3, 12, 16, 128),
            v(2, 2, sy, sz), v(2, sx, 2, sz), v(2, sx, 2, sz), v(2, sy, 128), v(2, 2, sy, 128), v(12, 16, 128),
            v(sy, 3 * slabs * 128), v(3, slabs, 16, 128), v(3, 8, 128), v(9, nz, 128),
            v(nx, 3, ny, 128), v(3 * (nx * ny - 1), 128), v(3, kx, ky, 128),
            v(2, 3, 2, 16, 128), v(2, 24, 2, 128), v(2, 24, 2, 128), v(2, 8, 128), v(2, 8, 128),
            dma((2, 8)), dma((6,)), dma((6,)), dma((9,)), dma((9,)), dma, dma, dma((6,)), dma((6,)), flag, flag,
        ],
        compiler_params=pltpu.CompilerParams(collective_id=0, has_side_effects=True, vmem_limit_bytes=48 << 20),
        name="gradient",
    )(far(warped_image), far(fixed_image), far(fine_control), far(coarse_control), far(d_matrix(sz)),
      far(h_matrix(sz)), far(y_matrix(sy)), far(z_matrices(sz)))
    return pl.pallas_call(
        write_out,
        out_shape=(out(*fine_control.shape), out(*coarse_control.shape)),
        in_specs=[vmem] * 2,
        out_specs=(hbm, hbm),
        scratch_shapes=[dma((2,))],
        compiler_params=pltpu.CompilerParams(vmem_limit_bytes=1 << 20),
        name="write_out",
    )(*results)


def solution(mesh):
    dims = tuple(mesh.shape[a] for a in ("gx", "gy", "gz"))
    in_specs = (P("gx", "gy", "gz"), P("gx", "gy", "gz"), P(None, "gx", "gy", "gz"), P())
    out_specs = (P(None, "gx", "gy", "gz"), P())
    return jax.shard_map(
        lambda *args: per_device(dims, *args), mesh=mesh, in_specs=in_specs, out_specs=out_specs, check_vma=False
    )
```
